32 devices in a mesh: dom: 32 (over z, y, x, core).
Axes of the slice: x: 2, y: 2, z: 4, core: 2. Of those that a mesh axis runs over, the one named last changes fastest.
Arguments:
- forcing: float32 [1024, 128], P('dom'), may hold values from -6 to 6
- first_guess: float32 [1024, 128], P('dom'), may hold values from -4 to 4
- corners: int32 [3, 262144], P(None, 'dom'), may hold values from 0 to 8191, as said below
- gradients: float32 [4, 262144], P(None, 'dom'), may hold values from -5 to 5
- element_area: float32 [262144], P('dom'), may hold values from 0.5 to 2
- element_depth: float32 [262144], P('dom'), may hold values from 0.2 to 4
- send_blocks: int32 [32, 4, 8], P('dom'), may hold values from 0 to 32, as said below
- recv_blocks: int32 [32, 4, 8], P('dom'), may hold values from 0 to 32, as said below
Outputs:
- elevation: float32 [1024, 128], P('dom')
- residual_left: float32 [1024, 128], P('dom')
The draws below stay inside these ranges and needn't reach their ends.
Inputs may be any that keep to these rules, and one draw needn't show every extreme that they name: `corners`: column e of device d's elements names three different local nodes of device d, numbered below (64) * 128: numbers below 4096 are its owned nodes in block order, the rest its halo blocks. The first corner is an owned node, and every owned node is the first corner of some element of its device. `send_blocks`: entry [d, o, s] is the owned block of device d sent in slot s of offset o to the reader d - k_o, or 32 for an empty slot; it is live exactly when recv_blocks[d - k_o, o, s] is, and readers outside the mesh get nothing. Live blocks of one device and offset differ. For k_o = 1 every slot toward an existing reader is live. `recv_blocks`: entry [q, o, s] is the halo block of device q filled by slot s of offset o from device q + k_o, or 32 for an empty slot. The live entries of one device differ.
All inputs are finite; a program needn't handle non-finite values.
Results may differ from the reference program's by a relative error of at most 0.00022.
Values sent between devices are 32-bit elements; how exact they have to be, the bound alone decides.
A program may use at most 64 MiB of HBM per device.

```python
import math
import jax
import jax.numpy as jnp

BLOCK = 128
OWN_BLOCKS = 32
SLOTS = 8
REACH = 2
ITERS = 2
OFFSETS = 4
HALO_BLOCKS = 32
ELEM_DEV = 8192
NODES = 131072
ELEMS = 262144
N_DOM = 32


def shift_values():
    return jnp.array([shift_at - REACH if shift_at < REACH else shift_at - REACH + 1 for shift_at in range(OFFSETS)], dtype=jnp.int32)


def link_tables(key):
    base = jax.random.fold_in(key, 4242)
    key_live, key_start, key_place = jax.random.split(base, 3)
    shift_table = shift_values()
    readers = jnp.arange(N_DOM, dtype=jnp.int32)[:, None, None]
    sources = readers + shift_table[None, :, None]
    inside = (sources >= 0) & (sources < N_DOM)
    coin = jax.random.randint(key_live, (N_DOM, OFFSETS, SLOTS), 0, 4, dtype=jnp.int32)
    forced = jnp.broadcast_to(shift_table[None, :, None] == 1, (N_DOM, OFFSETS, SLOTS))
    live = inside & ((coin != 0) | forced)
    start = jax.random.randint(key_start, (N_DOM, OFFSETS, 1), 0, OWN_BLOCKS, dtype=jnp.int32)
    slot_ids = jnp.arange(SLOTS, dtype=jnp.int32)[None, None, :]
    read_blocks = jnp.where(live, (start + slot_ids) % OWN_BLOCKS, OWN_BLOCKS).astype(jnp.int32)

    def placing(one_key):
        return jax.random.permutation(one_key, HALO_BLOCKS)
    places = jax.vmap(placing)(jax.random.split(key_place, N_DOM)).astype(jnp.int32)
    places = places.reshape(N_DOM, OFFSETS, SLOTS)
    recv_table = jnp.where(live, places, HALO_BLOCKS).astype(jnp.int32)
    owners = jnp.arange(N_DOM, dtype=jnp.int32)[:, None, None]
    targets = owners - shift_table[None, :, None]
    target_in = (targets >= 0) & (targets < N_DOM)
    clipped = jnp.clip(targets, 0, N_DOM - 1).astype(jnp.int32)
    offset_ids = jnp.arange(OFFSETS, dtype=jnp.int32)[None, :, None]
    picked = read_blocks[clipped, offset_ids, slot_ids]
    send_table = jnp.where(target_in, picked, OWN_BLOCKS).astype(jnp.int32)
    return (send_table, recv_table)


def draw_send_blocks(key, part):
    return link_tables(key)[0]


def draw_recv_blocks(key, part):
    return link_tables(key)[1]


def draw_corners(key, part):
    base = jax.random.fold_in(key, 31)
    key_perm, key_first, key_second = jax.random.split(base, 3)
    owned_nodes = OWN_BLOCKS * BLOCK
    local_nodes = (OWN_BLOCKS + HALO_BLOCKS) * BLOCK

    def shuffled(one_key):
        return jax.random.permutation(one_key, ELEM_DEV)
    leading = jax.vmap(shuffled)(jax.random.split(key_perm, N_DOM)).astype(jnp.int32) % owned_nodes
    step_one = jax.random.randint(key_first, (N_DOM, ELEM_DEV), 1, local_nodes, dtype=jnp.int32)
    extra = jax.random.randint(key_second, (N_DOM, ELEM_DEV), 0, local_nodes - 2, dtype=jnp.int32)
    step_two = 1 + (step_one + extra) % (local_nodes - 1)
    stacked = jnp.stack([leading, (leading + step_one) % local_nodes, (leading + step_two) % local_nodes])
    return stacked.reshape(3, N_DOM * ELEM_DEV).astype(jnp.int32)


def block_scale(stream_key, shape, shards, least, top_value):
    factor_of = 1.0
    for axis_at, parts in shards:
        steps = jax.random.uniform(jax.random.fold_in(jax.random.fold_in(stream_key, 6), axis_at), (parts,), jnp.float32, least / len(shards), top_value / len(shards))
        factor_of = factor_of * jnp.repeat(jnp.exp(steps), shape[axis_at] // parts).reshape((-1,) + (1,) * (len(shape) - 1 - axis_at))
    return factor_of


def noise(own_key, dims, spread, reach, shards=(), kind=jnp.bfloat16):
    values = jax.random.normal(own_key, dims, jnp.float32) * spread
    if len(shards) > 0:
        values = block_scale(own_key, dims, shards, -0.22, 0.18) * values
    return jnp.clip(values, min=-reach, max=reach).astype(kind)


def setup_inputs(seed: int = 0) -> dict:
    arg_keys = jax.random.split(jax.random.key(seed), 9)
    return {
        "forcing": noise(arg_keys[0], (N_DOM * OWN_BLOCKS, BLOCK), 1.0, 6.0, ((0, 32),), jnp.float32),
        "first_guess": noise(arg_keys[1], (N_DOM * OWN_BLOCKS, BLOCK), 0.5, 4.0, ((0, 32),), jnp.float32),
        "corners": draw_corners(jax.random.fold_in(arg_keys[8], 71), 0),
        "gradients": noise(arg_keys[3], (4, ELEMS), 1.0, 5.0, ((1, 32),), jnp.float32),
        "element_area": jnp.clip(jnp.exp(math.log(2.0) - 1.3862944 * jax.random.uniform(arg_keys[4], (ELEMS,), jnp.float32) ** block_scale(arg_keys[4], (ELEMS,), ((0, 32),), -0.2, 0.2)), 0.5, 2.0),
        "element_depth": jnp.clip(jnp.exp(math.log(4.0) - 2.9957323 * jax.random.uniform(arg_keys[5], (ELEMS,), jnp.float32) ** block_scale(arg_keys[5], (ELEMS,), ((0, 32),), -0.2, 0.2)), 0.2, 4.0),
        "send_blocks": draw_send_blocks(jax.random.fold_in(arg_keys[8], 71), 0),
        "recv_blocks": draw_recv_blocks(jax.random.fold_in(arg_keys[8], 71), 0),
    }


def shift_list():
    return [shift_at - REACH if shift_at < REACH else shift_at - REACH + 1 for shift_at in range(OFFSETS)]


def node_numbers(corners, send_blocks, recv_blocks):
    shift_table = jnp.array(shift_list(), dtype=jnp.int32)
    readers = jnp.arange(N_DOM, dtype=jnp.int32)[:, None, None]
    sources = readers + shift_table[None, :, None]
    inside = (sources >= 0) & (sources < N_DOM)
    clipped = jnp.clip(sources, 0, N_DOM - 1).astype(jnp.int32)
    offset_ids = jnp.arange(OFFSETS, dtype=jnp.int32)[None, :, None]
    slot_ids = jnp.arange(SLOTS, dtype=jnp.int32)[None, None, :]
    source_block = send_blocks[clipped, offset_ids, slot_ids]
    live = inside & (source_block < OWN_BLOCKS) & (recv_blocks < HALO_BLOCKS)
    nowhere = N_DOM * OWN_BLOCKS
    global_block = jnp.where(live, clipped * OWN_BLOCKS + source_block, nowhere).astype(jnp.int32)
    target = jnp.where(live, recv_blocks, HALO_BLOCKS).astype(jnp.int32)
    readers_full = jnp.broadcast_to(readers, target.shape).astype(jnp.int32)
    halo_table = jnp.full((N_DOM, HALO_BLOCKS + 1), nowhere, dtype=jnp.int32)
    halo_table = halo_table.at[readers_full, target].set(global_block)
    owned_table = (jnp.arange(N_DOM, dtype=jnp.int32)[:, None] * OWN_BLOCKS
                   + jnp.arange(OWN_BLOCKS, dtype=jnp.int32)[None, :])
    block_table = jnp.concatenate([owned_table, halo_table[:, :HALO_BLOCKS]], axis=1)
    owners = (jnp.arange(N_DOM * ELEM_DEV, dtype=jnp.int32) // ELEM_DEV)[None, :]
    mapped = block_table[owners, corners // BLOCK]
    return (mapped * BLOCK + corners % BLOCK).astype(jnp.int32)


def reference(forcing, first_guess, corners, gradients, element_area, element_depth, send_blocks, recv_blocks):
    nodes = node_numbers(corners, send_blocks, recv_blocks)
    grad_x = [gradients[0], gradients[2], -(gradients[0] + gradients[2])]
    grad_y = [gradients[1], gradients[3], -(gradients[1] + gradients[3])]
    scaled = element_depth * element_area
    stiffness = [[scaled * (grad_x[row_at] * grad_x[col_at] + grad_y[row_at] * grad_y[col_at])
                  for col_at in range(3)] for row_at in range(3)]
    flat_nodes = nodes.reshape(-1)
    extent = NODES + BLOCK
    third = element_area / 3.0
    mass = jax.ops.segment_sum(jnp.concatenate([third, third, third]), flat_nodes,
                               num_segments=extent)[:NODES].reshape(forcing.shape)

    def operate(field):
        padded = jnp.concatenate([field.reshape(-1), jnp.zeros((BLOCK,), dtype=jnp.float32)])
        values = [padded[nodes[corner_at]] for corner_at in range(3)]
        contrib = jnp.concatenate([stiffness[row_at][0] * values[0] + stiffness[row_at][1] * values[1]
                                   + stiffness[row_at][2] * values[2] for row_at in range(3)])
        summed = jax.ops.segment_sum(contrib, flat_nodes, num_segments=extent)[:NODES].reshape(field.shape)
        return mass * field + summed

    elevation = first_guess
    residual = forcing - operate(first_guess)
    direction = residual
    norm_now = jnp.sum(residual * residual)
    for step_at in range(ITERS):
        applied = operate(direction)
        step_size = norm_now / jnp.sum(direction * applied)
        elevation = elevation + step_size * direction
        residual = residual - step_size * applied
        norm_next = jnp.sum(residual * residual)
        direction = residual + (norm_next / norm_now) * direction
        norm_now = norm_next
    return elevation, residual
```

```python
import functools

import jax
import jax.numpy as jnp
from jax import lax
from jax.experimental import pallas as pl
from jax.experimental.pallas import tpu as pltpu
from jax.sharding import PartitionSpec as P

LANES = 128
ROWS = 8
LAY = 8


def shift_list(offsets):
    half_count = offsets // 2
    return [
        shift_at - half_count if shift_at < half_count else shift_at - half_count + 1
        for shift_at in range(offsets)
    ]


def learning_rounds(n, reach):
    rounds = []
    while reach < n - 1:
        rounds.append(reach)
        reach *= 2
    return rounds


def message_pairs(shifts):
    roles = sorted([0, *shifts])
    reach = max(roles) - min(roles)
    return {
        distance: [(a, b) for a in roles for b in roles if a - b == distance]
        for distance in range(-reach, reach + 1)
        if distance != 0
    }


def kernel(
    n,
    forcing,
    guess,
    corners,
    gradients,
    area,
    depth,
    send,
    recv,
    both,
    blk,
    lane,
    hot,
    elem,
    vals,
    hi,
    lo,
    table,
    base,
    links,
    links_in,
    guess_out,
    mix_out,
    mix_in,
    back_out,
    back_in,
    sum_out,
    sum_in,
    guess_send_sem,
    guess_recv_sem,
    link_send_sem,
    link_recv_sem,
    mix_send_sem,
    mix_recv_sem,
    back_send_sem,
    back_recv_sem,
    sum_send_sem,
    sum_recv_sem,
    known,
):
    own, _ = forcing.shape
    _, offsets, slots = send.shape
    halo = offsets * slots
    nodes = own + halo
    rows = area.shape[0]
    groups = rows // ROWS
    shifts = shift_list(offsets)
    pairs = message_pairs(shifts)
    distances = list(pairs)
    reach = max(distances)
    me = lax.axis_index("dom")
    f32 = jnp.float32
    bf16 = jnp.bfloat16

    def there(distance):
        return jnp.logical_and(me + distance >= 0, me + distance < n)

    def when_there(distance, action):
        @pl.when(there(distance))
        def _():
            action()

    def remote(source, target, send_sem, recv_sem, distance):
        return pltpu.make_async_remote_copy(
            src_ref=source,
            dst_ref=target,
            send_sem=send_sem,
            recv_sem=recv_sem,
            device_id=(me + distance,),
            device_id_type=pl.DeviceIdType.MESH,
        )

    def guess_copy(o):
        return remote(
            guess_out.at[o],
            table.at[0, pl.ds(own + o * slots, slots)],
            guess_send_sem.at[o],
            guess_recv_sem.at[o],
            -shifts[o],
        )

    def link_copy(o):
        return remote(
            links, links_in.at[o], link_send_sem.at[o], link_recv_sem.at[o], -shifts[o]
        )

    def mix_copy(e, i):
        count = len(pairs[distances[i]])
        return remote(
            mix_out.at[e, i, pl.ds(0, count)],
            mix_in.at[e, i, pl.ds(0, count)],
            mix_send_sem.at[e, i],
            mix_recv_sem.at[e, i],
            distances[i],
        )

    def back_copy(o):
        return remote(
            back_out.at[o], back_in.at[o], back_send_sem.at[o], back_recv_sem.at[o], shifts[o]
        )

    barrier = pltpu.get_barrier_semaphore()
    for distance in distances:
        when_there(
            distance,
            lambda distance=distance: pl.semaphore_signal(
                barrier,
                inc=1,
                device_id=(me + distance,),
                device_id_type=pl.DeviceIdType.MESH,
            ),
        )

    rounds = learning_rounds(n, reach)

    def tell(i):
        for side in range(2):
            far = rounds[i] * (2 * side - 1)
            when_there(
                far,
                lambda side=side, far=far: pl.semaphore_signal(
                    known.at[i, side],
                    inc=1,
                    device_id=(me + far,),
                    device_id_type=pl.DeviceIdType.MESH,
                ),
            )

    def learn(i):
        for side in range(2):
            far = rounds[i] * (1 - 2 * side)
            when_there(
                far, lambda side=side: pl.semaphore_wait(known.at[i, side], 1)
            )

    def next_round(i):
        if i > 0 and i <= len(rounds):
            learn(i - 1)
        if i < len(rounds):
            tell(i)

    for o in range(offsets):

        @pl.when(jnp.logical_not(there(shifts[o])))
        def _():
            table[0, own + o * slots : own + (o + 1) * slots] = jnp.zeros((slots, LANES), f32)
            links_in[o] = jnp.full((halo, LANES), own, jnp.int32)

        @pl.when(jnp.logical_not(there(-shifts[o])))
        def _():
            back_in[o] = jnp.zeros((slots, LANES), f32)

    for i, distance in enumerate(distances):

        @pl.when(jnp.logical_not(there(-distance)))
        def _():
            for e in range(2):
                mix_in[e, i] = jnp.zeros(mix_in.shape[2:], f32)

    for o in range(offsets):
        for s in range(slots):
            at = jnp.minimum(send[0, o, s], own - 1)
            guess_out[o, s : s + 1, :] = guess[pl.ds(at, 1), :]
    for o in range(offsets):
        for s in range(slots):
            links[o * slots + s : o * slots + s + 1, :] = jnp.full(
                (1, LANES), send[0, o, s], jnp.int32
            )
    pl.semaphore_wait(
        barrier, jnp.minimum(me, reach) + jnp.minimum(n - 1 - me, reach)
    )
    for o in range(offsets):
        when_there(-shifts[o], lambda o=o: guess_copy(o).start())
    for o in range(offsets):
        when_there(-shifts[o], lambda o=o: link_copy(o).start())
    next_round(0)
    table[0, 0:own] = guess[...]

    def lay(r, carry):
        for j in range(LAY):
            at = pl.multiple_of((r * LAY + j) * LANES, LANES)
            for c in range(3):
                lane[pl.ds(c * rows + r * LAY + j, 1), :] = corners[c : c + 1, pl.ds(at, LANES)]
            for c in range(4):
                elem[pl.ds(c * rows + r * LAY + j, 1), :] = gradients[c : c + 1, pl.ds(at, LANES)]
        return carry

    lax.fori_loop(0, rows // LAY, lay, 0)

    wide = lax.broadcasted_iota(jnp.int32, (ROWS, LANES), 1)
    lookup = jnp.where(wide < own, wide, 2 * LANES)
    for o in range(offsets):
        for s in range(slots):
            lookup = jnp.where(wide == own + recv[0, o, s], own + o * slots + s, lookup)
    lookup = jnp.where(wide < nodes, lookup, 2 * LANES)

    for g in range(3 * groups):
        node = lane[g * ROWS : (g + 1) * ROWS, :]
        block = lax.shift_right_logical(node, 7)
        blk[g * ROWS : (g + 1) * ROWS, :] = jnp.take_along_axis(
            lookup, block, axis=1, mode="promise_in_bounds"
        )
        lane[g * ROWS : (g + 1) * ROWS, :] = lax.bitwise_and(node, LANES - 1)

    tall = lax.broadcasted_iota(jnp.int32, (LANES, LANES), 0)

    def heat(g, carry):
        at = pl.multiple_of(g * ROWS, ROWS)
        for j in range(ROWS):
            row = lane[pl.ds(at + j, 1), :]
            hot[pl.ds(pl.multiple_of((at + j) * LANES, LANES), LANES), :] = (
                jnp.where(row == tall, 1.0, 0.0).astype(bf16).T
            )
        return carry

    lax.fori_loop(0, 3 * groups, heat, 0)
    for o in range(offsets):
        when_there(shifts[o], lambda o=o: guess_copy(o).wait_recv())
    next_round(1)

    own_names = lax.broadcasted_iota(jnp.int32, (own, LANES), 0)
    all_names = lax.broadcasted_iota(jnp.int32, (nodes, LANES), 0)

    def at_corner(c, g):
        return pl.ds(pl.multiple_of(c * rows + g * ROWS, ROWS), ROWS)

    def operate(t):
        def picked(c, g, count):
            index = lane[at_corner(c, g), :]
            block = blk[at_corner(c, g), :]
            value = jnp.zeros((ROWS, LANES), f32)
            for b in range(count):
                row = jnp.broadcast_to(table[t, b : b + 1, :], (ROWS, LANES))
                got = jnp.take_along_axis(row, index, axis=1, mode="promise_in_bounds")
                value = jnp.where(block == b, got, value)
            return value

        def spread(g, energy):
            u = [picked(0, g, own), picked(1, g, nodes), picked(2, g, nodes)]
            if t > 0:
                for c in range(3):
                    vals[t - 1, at_corner(c, g), :] = u[c]
            adds, local_energy = element(g, u, t == 1)
            for c in range(3):
                top = adds[c].astype(bf16).astype(f32)
                hi[at_corner(c, g), :] = top
                lo[at_corner(c, g), :] = adds[c] - top
            return energy + local_energy if t == 1 else energy

        def summed(g, sums):
            first, rest = sums

            def product(c, names):
                parts = []
                at = pl.multiple_of(c * rows + g * ROWS, ROWS)
                for j in range(ROWS):
                    mask = blk[pl.ds(at + j, 1), :] == names
                    parts.append(
                        jnp.concatenate(
                            [
                                jnp.where(mask, hi[pl.ds(at + j, 1), :], 0.0),
                                jnp.where(mask, lo[pl.ds(at + j, 1), :], 0.0),
                            ],
                            axis=0,
                        ).astype(bf16)
                    )
                left = jnp.concatenate(parts, axis=1)
                right = hot[pl.ds(pl.multiple_of(at * LANES, ROWS * LANES), ROWS * LANES), :]
                return jnp.dot(left, right, preferred_element_type=f32)

            first = first + product(0, own_names)
            rest = rest + product(1, all_names) + product(2, all_names)
            return first, rest

        def step(g, carry):
            sums, energy = carry
            sums = summed(g, sums)
            energy = spread(g + 1, energy)
            return sums, energy

        sums = (jnp.zeros((2 * own, LANES), f32), jnp.zeros((2 * nodes, LANES), f32))
        energy = spread(0, jnp.zeros((ROWS, LANES), f32))
        sums, energy = lax.fori_loop(0, groups - 1, step, (sums, energy))
        first, rest = summed(groups - 1, sums)
        total = rest[:nodes] + rest[nodes:]
        return total[:own] + (first[:own] + first[own:]), total[own:], energy

    def element(g, u, with_energy):
        gx0, gy0, gx1, gy1 = [elem[at_corner(c, g), :] for c in range(4)]
        here = pl.ds(pl.multiple_of(g * ROWS, ROWS), ROWS)
        size = area[here, :]
        scaled = depth[here, :] * size
        third = size / 3.0
        from0, from1 = u[0] - u[2], u[1] - u[2]
        raw_x = gx0 * from0 + gx1 * from1
        raw_y = gy0 * from0 + gy1 * from1
        slope_x = scaled * raw_x
        slope_y = scaled * raw_y
        flow0 = gx0 * slope_x + gy0 * slope_y
        flow1 = gx1 * slope_x + gy1 * slope_y
        adds = [
            flow0 + third * u[0],
            flow1 + third * u[1],
            third * u[2] - (flow0 + flow1),
        ]
        if not with_energy:
            return adds, None
        return adds, (
            slope_x * raw_x
            + slope_y * raw_y
            + third * (u[0] * u[0] + u[1] * u[1] + u[2] * u[2])
        )

    def exchange(e, own_part, halo_part):
        base[...] = own_part
        for i, distance in enumerate(distances):
            for j, (mine, theirs) in enumerate(pairs[distance]):
                if mine == 0:
                    o = shifts.index(theirs)
                    for s in range(slots):
                        at = jnp.minimum(send[0, o, s], own - 1)
                        mix_out[e, i, j, s : s + 1, :] = base[pl.ds(at, 1), :]
                else:
                    o = shifts.index(mine)
                    mix_out[e, i, j] = halo_part[o * slots : (o + 1) * slots]
        for i, distance in enumerate(distances):
            when_there(distance, lambda i=i: mix_copy(e, i).start())

    def collect(e, own_part, halo_part):
        for i, distance in enumerate(distances):
            when_there(-distance, lambda i=i: mix_copy(e, i).wait_recv())
        own_total = own_part
        halo_total = [halo_part[o * slots : (o + 1) * slots] for o in range(offsets)]
        for i, distance in enumerate(distances):
            for j, (theirs, mine) in enumerate(pairs[distance]):
                if mine == 0:
                    own_total = owned(own_total, shifts.index(theirs), mix_in.at[e, i, j])
                elif theirs == 0:
                    o = shifts.index(mine)
                    halo_total[o] = halo_total[o] + mix_in[e, i, j]
                else:
                    o, p = shifts.index(mine), shifts.index(theirs)
                    names = links_in[o, o * slots : (o + 1) * slots]
                    for s in range(slots):
                        at = p * slots + s
                        halo_total[o] = halo_total[o] + jnp.where(
                            names == links_in[o, at : at + 1, :], mix_in[e, i, j, s : s + 1, :], 0.0
                        )
        return own_total, halo_total

    def owned(total, o, part):
        for s in range(slots):
            total = total + jnp.where(own_names == send[0, o, s], part[s : s + 1, :], 0.0)
        return total

    def fill(t, own_total, halo_total):
        table[t, 0:own] = own_total
        for o in range(offsets):
            table[t, own + o * slots : own + (o + 1) * slots] = halo_total[o]

    small = lax.broadcasted_iota(jnp.int32, (1, LANES), 1)

    def whole(a):
        return jnp.sum(jnp.sum(a, axis=0, keepdims=True), axis=1, keepdims=True)

    def start_sum(k, terms):
        line = jnp.zeros((1, LANES), f32)
        for i, term in enumerate(terms):
            line = jnp.where(small == i, whole(term), line)
        sum_out[k] = line
        sum_in[k, me] = line

        def push(i, carry):
            pltpu.make_async_remote_copy(
                src_ref=sum_out.at[k],
                dst_ref=sum_in.at[k, me],
                send_sem=sum_send_sem.at[k],
                recv_sem=sum_recv_sem.at[k],
                device_id=(lax.rem(me + 1 + lax.rem(i + n // 2, n - 1), n),),
                device_id_type=pl.DeviceIdType.MESH,
            ).start()
            return carry

        lax.fori_loop(0, n - 1, push, 0)

    def sum_bytes(k):
        return sum_in.at[k, pl.ds(0, n - 1)]

    def finish_sum(k, count):
        pltpu.make_async_copy(sum_bytes(k), sum_bytes(k), sum_recv_sem.at[k]).wait()
        line = jnp.sum(sum_in[k], axis=0)
        return [
            jnp.sum(jnp.where(small == i, line, 0.0), axis=1, keepdims=True)
            for i in range(count)
        ]

    own_part, halo_part, _ = operate(0)
    own_part, halo_part = forcing[...] - own_part, -halo_part
    exchange(0, own_part, halo_part)
    next_round(2)
    for o in range(offsets):
        when_there(shifts[o], lambda o=o: link_copy(o).wait_recv())
    own_total, halo_total = collect(0, own_part, halo_part)
    fill(1, own_total, halo_total)
    for i in range(3, len(rounds) + 1):
        next_round(i)

    own_part, halo_part, energy = operate(1)
    exchange(1, own_part, halo_part)
    residual = table[1, 0:own]
    start_sum(0, [residual * residual, energy])
    own_total, halo_total = collect(1, own_part, halo_part)
    fill(2, own_total, halo_total)

    own_part, halo_part, _ = operate(2)
    for o in range(offsets):
        back_out[o] = halo_part[o * slots : (o + 1) * slots]
    for o in range(offsets):
        when_there(shifts[o], lambda o=o: back_copy(o).start())

    norm, crossed = finish_sum(0, 2)
    step = norm / crossed

    def pair_energy(g, energy):
        u = [
            vals[0, at_corner(c, g), :] - step * vals[1, at_corner(c, g), :] for c in range(3)
        ]
        return energy + element(g, u, True)[1]

    energy = lax.fori_loop(0, groups, pair_energy, jnp.zeros((ROWS, LANES), f32))
    residual, image = table[1, 0:own], table[2, 0:own]
    later = residual - step * image
    start_sum(1, [later * later, energy, later * image])

    for o in range(offsets):
        when_there(-shifts[o], lambda o=o: back_copy(o).wait_recv())
    for o in range(offsets):
        own_part = owned(own_part, o, back_in.at[o])
    applied = image - step * own_part
    for o in range(offsets):
        when_there(-shifts[o], lambda o=o: guess_copy(o).wait_send())
        when_there(-shifts[o], lambda o=o: link_copy(o).wait_send())
        when_there(shifts[o], lambda o=o: back_copy(o).wait_send())
    for e in range(2):
        for i, distance in enumerate(distances):
            when_there(distance, lambda e=e, i=i: mix_copy(e, i).wait_send())
    fresh, own_pair, mixed = finish_sum(1, 3)
    beta = fresh / norm
    next_step = fresh / (own_pair + beta * (2.0 * mixed + beta * crossed))
    both[0:own] = guess[...] + step * residual + next_step * (later + beta * residual)
    both[own : 2 * own] = later - next_step * (applied + beta * image)
    for k in range(2):
        pltpu.make_async_copy(sum_bytes(k), sum_bytes(k), sum_send_sem.at[k]).wait()


def local(
    n,
    forcing,
    first_guess,
    corners,
    gradients,
    element_area,
    element_depth,
    send_blocks,
    recv_blocks,
):
    own, columns = forcing.shape
    _, offsets, slots = send_blocks.shape
    count = element_area.shape[0]
    rows = count // LANES
    nodes = own + offsets * slots
    assert columns == LANES and nodes <= LANES and rows % ROWS == 0 and slots % ROWS == 0
    f32 = jnp.float32
    vmem = pl.BlockSpec(memory_space=pltpu.VMEM)
    smem = pl.BlockSpec(memory_space=pltpu.SMEM)
    dma = pltpu.SemaphoreType.DMA
    pairs = message_pairs(shift_list(offsets))
    most = max(len(listed) for listed in pairs.values())
    part = (offsets, slots, LANES)
    mix = (2, len(pairs), most, slots, LANES)
    both = pl.pallas_call(
        functools.partial(kernel, n),
        out_shape=jax.ShapeDtypeStruct((2 * own, columns), f32),
        in_specs=[vmem] * 6 + [smem] * 2,
        out_specs=vmem,
        scratch_shapes=[
            pltpu.VMEM((3 * rows, LANES), jnp.int32),
            pltpu.VMEM((3 * rows, LANES), jnp.int32),
            pltpu.VMEM((3 * count, LANES), jnp.bfloat16),
            pltpu.VMEM((4 * rows, LANES), f32),
            pltpu.VMEM((2, 3 * rows, LANES), f32),
            pltpu.VMEM((3 * rows, LANES), f32),
            pltpu.VMEM((3 * rows, LANES), f32),
            pltpu.VMEM((3, nodes, LANES), f32),
            pltpu.VMEM((own, LANES), f32),
            pltpu.VMEM((offsets * slots, LANES), jnp.int32),
            pltpu.VMEM((offsets, offsets * slots, LANES), jnp.int32),
            pltpu.VMEM(part, f32),
            pltpu.VMEM(mix, f32),
            pltpu.VMEM(mix, f32),
            pltpu.VMEM(part, f32),
            pltpu.VMEM(part, f32),
            pltpu.VMEM((2, 1, LANES), f32),
            pltpu.VMEM((2, n, 1, LANES), f32),
            dma((offsets,)),
            dma((offsets,)),
            dma((offsets,)),
            dma((offsets,)),
            dma((2, len(pairs))),
            dma((2, len(pairs))),
            dma((offsets,)),
            dma((offsets,)),
            dma((2,)),
            dma((2,)),
            pltpu.SemaphoreType.REGULAR((len(learning_rounds(n, max(pairs))) + 1, 2)),
        ],
        compiler_params=pltpu.CompilerParams(collective_id=0, has_side_effects=True),
    )(
        forcing,
        first_guess,
        corners,
        gradients,
        element_area.reshape(rows, LANES),
        element_depth.reshape(rows, LANES),
        send_blocks,
        recv_blocks,
    )
    return both[:own], both[own:]


def solution(mesh):
    placed = (
        P("dom", None),
        P("dom", None),
        P(None, "dom"),
        P(None, "dom"),
        P("dom"),
        P("dom"),
        P("dom", None, None),
        P("dom", None, None),
    )
    return jax.shard_map(
        functools.partial(local, mesh.shape["dom"]),
        mesh=mesh,
        in_specs=placed,
        out_specs=(P("dom", None), P("dom", None)),
        check_vma=False,
    )
```

```python
import functools

import jax
import jax.numpy as jnp
from jax import lax
from jax.experimental import pallas as pl
from jax.experimental.pallas import tpu as pltpu
from jax.sharding import PartitionSpec as P

LANES = 128
ROWS = 8
HEAT = 6
STEP = 2


def shift_list(offsets):
    half_count = offsets // 2
    return [
        shift_at - half_count if shift_at < half_count else shift_at - half_count + 1
        for shift_at in range(offsets)
    ]


def learning_rounds(n, reach):
    rounds = []
    while reach < n - 1:
        rounds.append(reach)
        reach *= 2
    return rounds


def message_pairs(shifts):
    roles = sorted([0, *shifts])
    reach = max(roles) - min(roles)
    return {
        distance: [(a, b) for a in roles for b in roles if a - b == distance]
        for distance in range(-reach, reach + 1)
        if distance != 0
    }


def kernel(
    n,
    forcing,
    guess,
    corners,
    gradients,
    area,
    depth,
    send,
    recv,
    both,
    blk,
    name,
    lane,
    hot,
    elem,
    vals,
    hi,
    lo,
    table,
    base,
    links,
    links_in,
    guess_out,
    mix_out,
    mix_in,
    back_out,
    back_in,
    sum_out,
    sum_in,
    guess_send_sem,
    guess_recv_sem,
    link_send_sem,
    link_recv_sem,
    mix_send_sem,
    mix_recv_sem,
    back_send_sem,
    back_recv_sem,
    sum_send_sem,
    sum_recv_sem,
    known,
):
    own, _ = forcing.shape
    _, offsets, slots = send.shape
    halo = offsets * slots
    nodes = own + halo
    wide_rows = max(own, halo)
    rows = area.shape[0]
    groups = rows // ROWS
    shifts = shift_list(offsets)
    pairs = message_pairs(shifts)
    distances = list(pairs)
    reach = max(distances)
    me = lax.axis_index("dom")
    f32 = jnp.float32
    bf16 = jnp.bfloat16

    def there(distance):
        return jnp.logical_and(me + distance >= 0, me + distance < n)

    def when_there(distance, action):
        @pl.when(there(distance))
        def _():
            action()

    def remote(source, target, send_sem, recv_sem, distance):
        return pltpu.make_async_remote_copy(
            src_ref=source,
            dst_ref=target,
            send_sem=send_sem,
            recv_sem=recv_sem,
            device_id=(me + distance,),
            device_id_type=pl.DeviceIdType.MESH,
        )

    def guess_copy(o):
        return remote(
            guess_out.at[o],
            table.at[0, pl.ds(own + o * slots, slots)],
            guess_send_sem.at[o],
            guess_recv_sem.at[o],
            -shifts[o],
        )

    def link_copy(o):
        return remote(
            links, links_in.at[o], link_send_sem.at[o], link_recv_sem.at[o], -shifts[o]
        )

    def mix_copy(e, i):
        count = len(pairs[distances[i]])
        return remote(
            mix_out.at[e, i, pl.ds(0, count)],
            mix_in.at[e, i, pl.ds(0, count)],
            mix_send_sem.at[e, i],
            mix_recv_sem.at[e, i],
            distances[i],
        )

    def back_copy(o):
        return remote(
            back_out.at[o], back_in.at[o], back_send_sem.at[o], back_recv_sem.at[o], shifts[o]
        )

    barrier = pltpu.get_barrier_semaphore()
    for distance in distances:
        when_there(
            distance,
            lambda distance=distance: pl.semaphore_signal(
                barrier,
                inc=1,
                device_id=(me + distance,),
                device_id_type=pl.DeviceIdType.MESH,
            ),
        )

    rounds = learning_rounds(n, reach)

    def tell(i):
        for side in range(2):
            far = rounds[i] * (2 * side - 1)
            when_there(
                far,
                lambda side=side, far=far: pl.semaphore_signal(
                    known.at[i, side],
                    inc=1,
                    device_id=(me + far,),
                    device_id_type=pl.DeviceIdType.MESH,
                ),
            )

    def learn(i):
        for side in range(2):
            far = rounds[i] * (1 - 2 * side)
            when_there(
                far, lambda side=side: pl.semaphore_wait(known.at[i, side], 1)
            )

    def next_round(i):
        if i > 0 and i <= len(rounds):
            learn(i - 1)
        if i < len(rounds):
            tell(i)

    for o in range(offsets):

        @pl.when(jnp.logical_not(there(shifts[o])))
        def _():
            table[0, own + o * slots : own + (o + 1) * slots] = jnp.zeros((slots, LANES), f32)
            links_in[o] = jnp.full((halo, LANES), own, jnp.int32)

        @pl.when(jnp.logical_not(there(-shifts[o])))
        def _():
            back_in[o] = jnp.zeros((slots, LANES), f32)

    for i, distance in enumerate(distances):

        @pl.when(jnp.logical_not(there(-distance)))
        def _():
            for e in range(2):
                mix_in[e, i] = jnp.zeros(mix_in.shape[2:], f32)

    for o in range(offsets):
        for s in range(slots):
            at = jnp.minimum(send[0, o, s], own - 1)
            guess_out[o, s : s + 1, :] = guess[pl.ds(at, 1), :]
    for o in range(offsets):
        for s in range(slots):
            links[o * slots + s : o * slots + s + 1, :] = jnp.full(
                (1, LANES), send[0, o, s], jnp.int32
            )
    pl.semaphore_wait(
        barrier, jnp.minimum(me, reach) + jnp.minimum(n - 1 - me, reach)
    )
    for o in range(offsets):
        when_there(-shifts[o], lambda o=o: guess_copy(o).start())
    for o in range(offsets):
        when_there(-shifts[o], lambda o=o: link_copy(o).start())
    next_round(0)
    table[0, 0:own] = guess[...]

    def lay(r, carry):
        for j in range(ROWS):
            at = pl.multiple_of((r * ROWS + j) * LANES, LANES)
            for c in range(3):
                lane[pl.ds((r * 3 + c) * ROWS + j, 1), :] = corners[c : c + 1, pl.ds(at, LANES)]
            for c in range(4):
                elem[pl.ds((r * 4 + c) * ROWS + j, 1), :] = gradients[c : c + 1, pl.ds(at, LANES)]
        return carry

    lax.fori_loop(0, groups, lay, 0)

    wide = lax.broadcasted_iota(jnp.int32, (ROWS, LANES), 1)
    lookup = jnp.where(wide < own, wide, 2 * LANES)
    for o in range(offsets):
        for s in range(slots):
            lookup = jnp.where(wide == own + recv[0, o, s], own + o * slots + s, lookup)
    lookup = jnp.where(wide < nodes, lookup, 2 * LANES)

    for g in range(3 * groups):
        here = slice(g * ROWS, (g + 1) * ROWS)
        node = lane[here, :]
        block = jnp.take_along_axis(
            lookup, lax.shift_right_logical(node, 7), axis=1, mode="promise_in_bounds"
        )
        blk[here, :] = block
        name[here, :] = jnp.where(block < own, block, block - own)
        hi[here, :] = jnp.where(block < own, 1.0, -1.0)
        lane[here, :] = lax.bitwise_and(node, LANES - 1)

    tall = lax.broadcasted_iota(jnp.int32, (LANES, LANES), 0)

    def heat(g, carry):
        for j in range(HEAT * ROWS):
            at = g * (HEAT * ROWS) + j
            code = jnp.where(lane[pl.ds(at, 1), :] == tall, hi[pl.ds(at, 1), :], 0.0)
            code = code.astype(bf16).T
            to = pl.ds(pl.multiple_of(at * LANES, LANES), LANES)
            hot[to, 0:LANES] = jnp.maximum(code, 0.0).astype(hot.dtype)
            hot[to, LANES : 2 * LANES] = jnp.maximum(-code, 0.0).astype(hot.dtype)
        return carry

    lax.fori_loop(0, 3 * groups // HEAT, heat, 0)
    for o in range(offsets):
        when_there(shifts[o], lambda o=o: guess_copy(o).wait_recv())
    next_round(1)

    own_names = lax.broadcasted_iota(jnp.int32, (own, LANES), 0)
    names = lax.broadcasted_iota(jnp.int32, (wide_rows, LANES), 0)

    def at_corner(c, g):
        return pl.ds(pl.multiple_of((g * 3 + c) * ROWS, ROWS), ROWS)

    def operate(t):
        def picked(c, g, count):
            index = lane[at_corner(c, g), :]
            block = blk[at_corner(c, g), :]
            value = jnp.zeros((ROWS, LANES), f32)
            for b in range(count):
                row = jnp.broadcast_to(table[t, b : b + 1, :], (ROWS, LANES))
                got = jnp.take_along_axis(row, index, axis=1, mode="promise_in_bounds")
                value = jnp.where(block == b, got, value)
            return value

        def spread(g, energy):
            u = [picked(0, g, own), picked(1, g, nodes), picked(2, g, nodes)]
            if t > 0:
                for c in range(3):
                    vals[t - 1, at_corner(c, g), :] = u[c]
            adds, local_energy = element(g, u, t == 1)
            for c in range(3):
                top = adds[c].astype(bf16).astype(f32)
                hi[at_corner(c, g), :] = top
                lo[at_corner(c, g), :] = adds[c] - top
            return energy + local_energy if t == 1 else energy

        def summed(g, sums):
            first = pl.multiple_of(g * (3 * ROWS), 3 * ROWS)
            parts = []
            for j in range(STEP * 3 * ROWS):
                mask = name[pl.ds(first + j, 1), :] == names
                parts.append(
                    jnp.concatenate(
                        [
                            jnp.where(mask, hi[pl.ds(first + j, 1), :], 0.0),
                            jnp.where(mask, lo[pl.ds(first + j, 1), :], 0.0),
                        ],
                        axis=0,
                    ).astype(bf16)
                )
            count = STEP * 3 * ROWS * LANES
            return sums + lax.dot_general(
                jnp.concatenate(parts, axis=1),
                hot[pl.ds(pl.multiple_of(first * LANES, 3 * ROWS * LANES), count), :],
                (((1,), (0,)), ((), ())),
                preferred_element_type=f32,
            )

        def spread_some(g, energy):
            for k in range(STEP):
                energy = spread(g + k, energy)
            return energy

        def step(i, carry):
            sums, energy = carry
            sums = summed(i * STEP, sums)
            energy = spread_some((i + 1) * STEP, energy)
            return sums, energy

        sums = jnp.zeros((2 * wide_rows, 2 * LANES), f32)
        energy = spread_some(0, jnp.zeros((ROWS, LANES), f32))
        sums, energy = lax.fori_loop(0, groups // STEP - 1, step, (sums, energy))
        sums = summed(groups - STEP, sums)
        sums = sums[:wide_rows] + sums[wide_rows:]
        return sums[:own, :LANES], sums[:halo, LANES:], energy

    def element(g, u, with_energy):
        gx0, gy0, gx1, gy1 = [
            elem[pl.ds(pl.multiple_of((g * 4 + c) * ROWS, ROWS), ROWS), :] for c in range(4)
        ]
        here = pl.ds(pl.multiple_of(g * ROWS, ROWS), ROWS)
        size = area[here, :]
        scaled = depth[here, :] * size
        third = size / 3.0
        from0, from1 = u[0] - u[2], u[1] - u[2]
        raw_x = gx0 * from0 + gx1 * from1
        raw_y = gy0 * from0 + gy1 * from1
        slope_x = scaled * raw_x
        slope_y = scaled * raw_y
        flow0 = gx0 * slope_x + gy0 * slope_y
        flow1 = gx1 * slope_x + gy1 * slope_y
        adds = [
            flow0 + third * u[0],
            flow1 + third * u[1],
            third * u[2] - (flow0 + flow1),
        ]
        if not with_energy:
            return adds, None
        return adds, (
            slope_x * raw_x
            + slope_y * raw_y
            + third * (u[0] * u[0] + u[1] * u[1] + u[2] * u[2])
        )

    def exchange(e, own_part, halo_part):
        base[...] = own_part
        for i, distance in enumerate(distances):
            for j, (mine, theirs) in enumerate(pairs[distance]):
                if mine == 0:
                    o = shifts.index(theirs)
                    for s in range(slots):
                        at = jnp.minimum(send[0, o, s], own - 1)
                        mix_out[e, i, j, s : s + 1, :] = base[pl.ds(at, 1), :]
                else:
                    o = shifts.index(mine)
                    mix_out[e, i, j] = halo_part[o * slots : (o + 1) * slots]
        for i, distance in enumerate(distances):
            when_there(distance, lambda i=i: mix_copy(e, i).start())

    def collect(e, own_part, halo_part):
        for i, distance in enumerate(distances):
            when_there(-distance, lambda i=i: mix_copy(e, i).wait_recv())
        own_total = own_part
        halo_total = [halo_part[o * slots : (o + 1) * slots] for o in range(offsets)]
        for i, distance in enumerate(distances):
            for j, (theirs, mine) in enumerate(pairs[distance]):
                if mine == 0:
                    own_total = owned(own_total, shifts.index(theirs), mix_in.at[e, i, j])
                elif theirs == 0:
                    o = shifts.index(mine)
                    halo_total[o] = halo_total[o] + mix_in[e, i, j]
                else:
                    o, p = shifts.index(mine), shifts.index(theirs)
                    names = links_in[o, o * slots : (o + 1) * slots]
                    for s in range(slots):
                        at = p * slots + s
                        halo_total[o] = halo_total[o] + jnp.where(
                            names == links_in[o, at : at + 1, :], mix_in[e, i, j, s : s + 1, :], 0.0
                        )
        return own_total, halo_total

    def owned(total, o, part):
        for s in range(slots):
            total = total + jnp.where(own_names == send[0, o, s], part[s : s + 1, :], 0.0)
        return total

    def fill(t, own_total, halo_total):
        table[t, 0:own] = own_total
        for o in range(offsets):
            table[t, own + o * slots : own + (o + 1) * slots] = halo_total[o]

    small = lax.broadcasted_iota(jnp.int32, (1, LANES), 1)

    def whole(a):
        return jnp.sum(jnp.sum(a, axis=0, keepdims=True), axis=1, keepdims=True)

    def start_sum(k, terms):
        line = jnp.zeros((1, LANES), f32)
        for i, term in enumerate(terms):
            line = jnp.where(small == i, whole(term), line)
        sum_out[k] = line
        sum_in[k, me] = line

        def push(i, carry):
            pltpu.make_async_remote_copy(
                src_ref=sum_out.at[k],
                dst_ref=sum_in.at[k, me],
                send_sem=sum_send_sem.at[k],
                recv_sem=sum_recv_sem.at[k],
                device_id=(lax.rem(me + 1 + lax.rem(i + n // 2, n - 1), n),),
                device_id_type=pl.DeviceIdType.MESH,
            ).start()
            return carry

        lax.fori_loop(0, n - 1, push, 0)

    def sum_bytes(k):
        return sum_in.at[k, pl.ds(0, n - 1)]

    def finish_sum(k, count):
        pltpu.make_async_copy(sum_bytes(k), sum_bytes(k), sum_recv_sem.at[k]).wait()
        line = jnp.sum(sum_in[k], axis=0)
        return [
            jnp.sum(jnp.where(small == i, line, 0.0), axis=1, keepdims=True)
            for i in range(count)
        ]

    own_part, halo_part, _ = operate(0)
    own_part, halo_part = forcing[...] - own_part, -halo_part
    exchange(0, own_part, halo_part)
    next_round(2)
    for o in range(offsets):
        when_there(shifts[o], lambda o=o: link_copy(o).wait_recv())
    own_total, halo_total = collect(0, own_part, halo_part)
    fill(1, own_total, halo_total)
    for i in range(3, len(rounds) + 1):
        next_round(i)

    own_part, halo_part, energy = operate(1)
    exchange(1, own_part, halo_part)
    residual = table[1, 0:own]
    start_sum(0, [residual * residual, energy])
    own_total, halo_total = collect(1, own_part, halo_part)
    fill(2, own_total, halo_total)

    own_part, halo_part, _ = operate(2)
    for o in range(offsets):
        back_out[o] = halo_part[o * slots : (o + 1) * slots]
    for o in range(offsets):
        when_there(shifts[o], lambda o=o: back_copy(o).start())

    norm, crossed = finish_sum(0, 2)
    step = norm / crossed

    def pair_energy(g, energy):
        u = [
            vals[0, at_corner(c, g), :] - step * vals[1, at_corner(c, g), :] for c in range(3)
        ]
        return energy + element(g, u, True)[1]

    energy = lax.fori_loop(0, groups, pair_energy, jnp.zeros((ROWS, LANES), f32))
    residual, image = table[1, 0:own], table[2, 0:own]
    later = residual - step * image
    start_sum(1, [later * later, energy, later * image])

    for o in range(offsets):
        when_there(-shifts[o], lambda o=o: back_copy(o).wait_recv())
    for o in range(offsets):
        own_part = owned(own_part, o, back_in.at[o])
    applied = image - step * own_part
    for o in range(offsets):
        when_there(-shifts[o], lambda o=o: guess_copy(o).wait_send())
        when_there(-shifts[o], lambda o=o: link_copy(o).wait_send())
        when_there(shifts[o], lambda o=o: back_copy(o).wait_send())
    for e in range(2):
        for i, distance in enumerate(distances):
            when_there(distance, lambda e=e, i=i: mix_copy(e, i).wait_send())
    fresh, own_pair, mixed = finish_sum(1, 3)
    beta = fresh / norm
    next_step = fresh / (own_pair + beta * (2.0 * mixed + beta * crossed))
    both[0:own] = guess[...] + step * residual + next_step * (later + beta * residual)
    both[own : 2 * own] = later - next_step * (applied + beta * image)
    for k in range(2):
        pltpu.make_async_copy(sum_bytes(k), sum_bytes(k), sum_send_sem.at[k]).wait()


def local(
    n,
    forcing,
    first_guess,
    corners,
    gradients,
    element_area,
    element_depth,
    send_blocks,
    recv_blocks,
):
    own, columns = forcing.shape
    _, offsets, slots = send_blocks.shape
    count = element_area.shape[0]
    rows = count // LANES
    nodes = own + offsets * slots
    assert columns == LANES and nodes <= LANES and slots % ROWS == 0
    assert rows % (ROWS * STEP) == 0 and (3 * rows // ROWS) % HEAT == 0
    f32 = jnp.float32
    vmem = pl.BlockSpec(memory_space=pltpu.VMEM)
    smem = pl.BlockSpec(memory_space=pltpu.SMEM)
    dma = pltpu.SemaphoreType.DMA
    pairs = message_pairs(shift_list(offsets))
    most = max(len(listed) for listed in pairs.values())
    part = (offsets, slots, LANES)
    mix = (2, len(pairs), most, slots, LANES)
    both = pl.pallas_call(
        functools.partial(kernel, n),
        out_shape=jax.ShapeDtypeStruct((2 * own, columns), f32),
        in_specs=[vmem] * 6 + [smem] * 2,
        out_specs=vmem,
        scratch_shapes=[
            pltpu.VMEM((3 * rows, LANES), jnp.int32),
            pltpu.VMEM((3 * rows, LANES), jnp.int32),
            pltpu.VMEM((3 * rows, LANES), jnp.int32),
            pltpu.VMEM((3 * count, 2 * LANES), jnp.float8_e4m3fn),
            pltpu.VMEM((4 * rows, LANES), f32),
            pltpu.VMEM((2, 3 * rows, LANES), f32),
            pltpu.VMEM((3 * rows, LANES), f32),
            pltpu.VMEM((3 * rows, LANES), f32),
            pltpu.VMEM((3, nodes, LANES), f32),
            pltpu.VMEM((own, LANES), f32),
            pltpu.VMEM((offsets * slots, LANES), jnp.int32),
            pltpu.VMEM((offsets, offsets * slots, LANES), jnp.int32),
            pltpu.VMEM(part, f32),
            pltpu.VMEM(mix, f32),
            pltpu.VMEM(mix, f32),
            pltpu.VMEM(part, f32),
            pltpu.VMEM(part, f32),
            pltpu.VMEM((2, 1, LANES), f32),
            pltpu.VMEM((2, n, 1, LANES), f32),
            dma((offsets,)),
            dma((offsets,)),
            dma((offsets,)),
            dma((offsets,)),
            dma((2, len(pairs))),
            dma((2, len(pairs))),
            dma((offsets,)),
            dma((offsets,)),
            dma((2,)),
            dma((2,)),
            pltpu.SemaphoreType.REGULAR((len(learning_rounds(n, max(pairs))) + 1, 2)),
        ],
        compiler_params=pltpu.CompilerParams(collective_id=0, has_side_effects=True),
    )(
        forcing,
        first_guess,
        corners,
        gradients,
        element_area.reshape(rows, LANES),
        element_depth.reshape(rows, LANES),
        send_blocks,
        recv_blocks,
    )
    return both[:own], both[own:]


def solution(mesh):
    placed = (
        P("dom", None),
        P("dom", None),
        P(None, "dom"),
        P(None, "dom"),
        P("dom"),
        P("dom"),
        P("dom", None, None),
        P("dom", None, None),
    )
    return jax.shard_map(
        functools.partial(local, mesh.shape["dom"]),
        mesh=mesh,
        in_specs=placed,
        out_specs=(P("dom", None), P("dom", None)),
        check_vma=False,
    )
```

```python
import functools

import jax
import jax.numpy as jnp
from jax import lax
from jax.experimental import pallas as pl
from jax.experimental.pallas import tpu as pltpu
from jax.sharding import PartitionSpec as P

LANES = 128
ROWS = 8
HEAT = 6
STEP = 2
PUSH = 8


def shift_list(offsets):
    half_count = offsets // 2
    return [
        shift_at - half_count if shift_at < half_count else shift_at - half_count + 1
        for shift_at in range(offsets)
    ]


def learning_rounds(n, reach):
    rounds = []
    while reach < n - 1:
        rounds.append(reach)
        reach *= 2
    return rounds


def message_pairs(shifts):
    roles = sorted([0, *shifts])
    reach = max(roles) - min(roles)
    return {
        distance: [(a, b) for a in roles for b in roles if a - b == distance]
        for distance in range(-reach, reach + 1)
        if distance != 0
    }


def kernel(
    n,
    forcing_in,
    guess_in,
    corners_in,
    gradients_in,
    area_in,
    depth_in,
    send_in,
    recv_in,
    both,
    forcing,
    guess,
    corners,
    gradients,
    area,
    depth,
    send,
    recv,
    load_sem,
    blk,
    name,
    lane,
    hot,
    elem,
    vals,
    hi,
    lo,
    table,
    base,
    links,
    links_in,
    guess_out,
    mix_out,
    mix_in,
    back_out,
    back_in,
    sum_out,
    sum_in,
    guess_send_sem,
    guess_recv_sem,
    link_send_sem,
    link_recv_sem,
    mix_send_sem,
    mix_recv_sem,
    back_send_sem,
    back_recv_sem,
    sum_send_sem,
    sum_recv_sem,
    known,
):
    own, _ = forcing.shape
    _, offsets, slots = send.shape
    halo = offsets * slots
    nodes = own + halo
    wide_rows = max(own, halo)
    rows = area.shape[0]
    groups = rows // ROWS
    shifts = shift_list(offsets)
    pairs = message_pairs(shifts)
    distances = list(pairs)
    reach = max(distances)
    order = sorted(distances, key=lambda distance: (-abs(distance), distance))
    me = lax.axis_index("dom")
    f32 = jnp.float32
    bf16 = jnp.bfloat16

    def there(distance):
        return jnp.logical_and(me + distance >= 0, me + distance < n)

    def when_there(distance, action):
        @pl.when(there(distance))
        def _():
            action()

    def remote(source, target, send_sem, recv_sem, distance):
        return pltpu.make_async_remote_copy(
            src_ref=source,
            dst_ref=target,
            send_sem=send_sem,
            recv_sem=recv_sem,
            device_id=(me + distance,),
            device_id_type=pl.DeviceIdType.MESH,
        )

    def guess_copy(o):
        return remote(
            guess_out.at[o],
            table.at[0, pl.ds(own + o * slots, slots)],
            guess_send_sem.at[o],
            guess_recv_sem.at[o],
            -shifts[o],
        )

    def link_copy(o):
        return remote(
            links, links_in.at[o], link_send_sem.at[o], link_recv_sem.at[o], -shifts[o]
        )

    def mix_copy(e, i):
        count = len(pairs[distances[i]])
        return remote(
            mix_out.at[e, i, pl.ds(0, count)],
            mix_in.at[e, i, pl.ds(0, count)],
            mix_send_sem.at[e, i],
            mix_recv_sem.at[e, i],
            distances[i],
        )

    def back_copy(o):
        return remote(
            back_out.at[o], back_in.at[o], back_send_sem.at[o], back_recv_sem.at[o], shifts[o]
        )

    loads = [
        pltpu.make_async_copy(source, target, load_sem.at[i])
        for i, (source, target) in enumerate(
            [
                (send_in, send),
                (guess_in, guess),
                (corners_in, corners),
                (recv_in, recv),
                (gradients_in, gradients),
                (area_in, area),
                (depth_in, depth),
                (forcing_in, forcing),
            ]
        )
    ]
    for load in loads[:3]:
        load.start()
    barrier = pltpu.get_barrier_semaphore()
    for distance in distances:
        when_there(
            distance,
            lambda distance=distance: pl.semaphore_signal(
                barrier,
                inc=1,
                device_id=(me + distance,),
                device_id_type=pl.DeviceIdType.MESH,
            ),
        )

    for load in loads[3:]:
        load.start()
    rounds = learning_rounds(n, reach)

    def tell(i):
        for side in range(2):
            far = rounds[i] * (2 * side - 1)
            when_there(
                far,
                lambda side=side, far=far: pl.semaphore_signal(
                    known.at[i, side],
                    inc=1,
                    device_id=(me + far,),
                    device_id_type=pl.DeviceIdType.MESH,
                ),
            )

    def learn(i):
        for side in range(2):
            far = rounds[i] * (1 - 2 * side)
            when_there(
                far, lambda side=side: pl.semaphore_wait(known.at[i, side], 1)
            )

    def next_round(i):
        if i > 0 and i <= len(rounds):
            learn(i - 1)
        if i < len(rounds):
            tell(i)

    for load in loads[:2]:
        load.wait()
    for o in range(offsets):
        for s in range(slots):
            at = jnp.minimum(send[0, o, s], own - 1)
            guess_out[o, s : s + 1, :] = guess[pl.ds(at, 1), :]
    for o in range(offsets):
        for s in range(slots):
            links[o * slots + s : o * slots + s + 1, :] = jnp.full(
                (1, LANES), send[0, o, s], jnp.int32
            )
    pl.semaphore_wait(
        barrier, jnp.minimum(me, reach) + jnp.minimum(n - 1 - me, reach)
    )
    for o in range(offsets):
        when_there(-shifts[o], lambda o=o: guess_copy(o).start())
    for o in range(offsets):
        when_there(-shifts[o], lambda o=o: link_copy(o).start())
    next_round(0)
    for o in range(offsets):

        @pl.when(jnp.logical_not(there(shifts[o])))
        def _():
            table[0, own + o * slots : own + (o + 1) * slots] = jnp.zeros((slots, LANES), f32)
            links_in[o] = jnp.full((halo, LANES), own, jnp.int32)

        @pl.when(jnp.logical_not(there(-shifts[o])))
        def _():
            back_in[o] = jnp.zeros((slots, LANES), f32)

    for i, distance in enumerate(distances):

        @pl.when(jnp.logical_not(there(-distance)))
        def _():
            for e in range(2):
                mix_in[e, i] = jnp.zeros(mix_in.shape[2:], f32)
    table[0, 0:own] = guess[...]
    for load in loads[2:5]:
        load.wait()

    def lay(r, carry):
        for j in range(ROWS):
            at = pl.multiple_of((r * ROWS + j) * LANES, LANES)
            for c in range(3):
                lane[pl.ds((r * 3 + c) * ROWS + j, 1), :] = corners[c : c + 1, pl.ds(at, LANES)]
            for c in range(4):
                elem[pl.ds((r * 4 + c) * ROWS + j, 1), :] = gradients[c : c + 1, pl.ds(at, LANES)]
        return carry

    lax.fori_loop(0, groups, lay, 0)

    wide = lax.broadcasted_iota(jnp.int32, (ROWS, LANES), 1)
    lookup = jnp.where(wide < own, wide, 2 * LANES)
    for o in range(offsets):
        for s in range(slots):
            lookup = jnp.where(wide == own + recv[0, o, s], own + o * slots + s, lookup)
    lookup = jnp.where(wide < nodes, lookup, 2 * LANES)

    for g in range(3 * groups):
        here = slice(g * ROWS, (g + 1) * ROWS)
        node = lane[here, :]
        block = jnp.take_along_axis(
            lookup, lax.shift_right_logical(node, 7), axis=1, mode="promise_in_bounds"
        )
        blk[here, :] = block
        name[here, :] = jnp.where(block < own, block, block - own)
        hi[here, :] = jnp.where(block < own, 1.0, -1.0)
        lane[here, :] = lax.bitwise_and(node, LANES - 1)

    tall = lax.broadcasted_iota(jnp.int32, (LANES, LANES), 0)

    def heat(g, carry):
        for j in range(HEAT * ROWS):
            at = g * (HEAT * ROWS) + j
            code = jnp.where(lane[pl.ds(at, 1), :] == tall, hi[pl.ds(at, 1), :], 0.0)
            code = code.astype(bf16).T
            to = pl.ds(pl.multiple_of(at * LANES, LANES), LANES)
            hot[to, 0:LANES] = jnp.maximum(code, 0.0).astype(hot.dtype)
            hot[to, LANES : 2 * LANES] = jnp.maximum(-code, 0.0).astype(hot.dtype)
        return carry

    lax.fori_loop(0, 3 * groups // HEAT, heat, 0)
    for load in loads[5:]:
        load.wait()
    for o in range(offsets):
        when_there(shifts[o], lambda o=o: guess_copy(o).wait_recv())
    next_round(1)

    own_names = lax.broadcasted_iota(jnp.int32, (own, LANES), 0)
    names = lax.broadcasted_iota(jnp.int32, (wide_rows, LANES), 0)

    def at_corner(c, g):
        return pl.ds(pl.multiple_of((g * 3 + c) * ROWS, ROWS), ROWS)

    def operate(t, gathered=None):
        def picked(c, g, count):
            index = lane[at_corner(c, g), :]
            block = blk[at_corner(c, g), :]
            value = jnp.zeros((ROWS, LANES), f32)
            for b in range(count):
                row = jnp.broadcast_to(table[t, b : b + 1, :], (ROWS, LANES))
                got = jnp.take_along_axis(row, index, axis=1, mode="promise_in_bounds")
                value = jnp.where(block == b, got, value)
            return value

        def spread(g, energy):
            u = [picked(0, g, own), picked(1, g, nodes), picked(2, g, nodes)]
            if t > 0:
                for c in range(3):
                    vals[t - 1, at_corner(c, g), :] = u[c]
            adds, local_energy = element(g, u, t == 1)
            for c in range(3):
                top = adds[c].astype(bf16).astype(f32)
                hi[at_corner(c, g), :] = top
                lo[at_corner(c, g), :] = adds[c] - top
            return energy + local_energy if t == 1 else energy

        def summed(g, sums):
            first = pl.multiple_of(g * (3 * ROWS), 3 * ROWS)
            parts = []
            for j in range(STEP * 3 * ROWS):
                mask = name[pl.ds(first + j, 1), :] == names
                parts.append(
                    jnp.concatenate(
                        [
                            jnp.where(mask, hi[pl.ds(first + j, 1), :], 0.0),
                            jnp.where(mask, lo[pl.ds(first + j, 1), :], 0.0),
                        ],
                        axis=0,
                    ).astype(bf16)
                )
            count = STEP * 3 * ROWS * LANES
            return sums + lax.dot_general(
                jnp.concatenate(parts, axis=1),
                hot[pl.ds(pl.multiple_of(first * LANES, 3 * ROWS * LANES), count), :],
                (((1,), (0,)), ((), ())),
                preferred_element_type=f32,
            )

        def spread_some(g, energy):
            for k in range(STEP):
                energy = spread(g + k, energy)
            return energy

        def step(i, carry):
            sums, energy = carry
            sums = summed(i * STEP, sums)
            energy = spread_some((i + 1) * STEP, energy)
            return sums, energy

        sums = jnp.zeros((2 * wide_rows, 2 * LANES), f32)
        energy = spread_some(0, jnp.zeros((ROWS, LANES), f32))
        sums, energy = lax.fori_loop(0, groups // STEP - 1, step, (sums, energy))
        if gathered is not None:
            gathered()
        sums = summed(groups - STEP, sums)
        sums = sums[:wide_rows] + sums[wide_rows:]
        return sums[:own, :LANES], sums[:halo, LANES:], energy

    def element(g, u, with_energy):
        gx0, gy0, gx1, gy1 = [
            elem[pl.ds(pl.multiple_of((g * 4 + c) * ROWS, ROWS), ROWS), :] for c in range(4)
        ]
        here = pl.ds(pl.multiple_of(g * ROWS, ROWS), ROWS)
        size = area[here, :]
        scaled = depth[here, :] * size
        third = size / 3.0
        from0, from1 = u[0] - u[2], u[1] - u[2]
        raw_x = gx0 * from0 + gx1 * from1
        raw_y = gy0 * from0 + gy1 * from1
        slope_x = scaled * raw_x
        slope_y = scaled * raw_y
        flow0 = gx0 * slope_x + gy0 * slope_y
        flow1 = gx1 * slope_x + gy1 * slope_y
        adds = [
            flow0 + third * u[0],
            flow1 + third * u[1],
            third * u[2] - (flow0 + flow1),
        ]
        if not with_energy:
            return adds, None
        return adds, (
            slope_x * raw_x
            + slope_y * raw_y
            + third * (u[0] * u[0] + u[1] * u[1] + u[2] * u[2])
        )

    def exchange(e, own_part, halo_part):
        base[...] = own_part
        for distance in reversed(order):
            i = distances.index(distance)
            for j, (mine, theirs) in enumerate(pairs[distance]):
                if mine == 0:
                    o = shifts.index(theirs)
                    for s in range(slots):
                        at = jnp.minimum(send[0, o, s], own - 1)
                        mix_out[e, i, j, s : s + 1, :] = base[pl.ds(at, 1), :]
                else:
                    o = shifts.index(mine)
                    mix_out[e, i, j] = halo_part[o * slots : (o + 1) * slots]
            when_there(distance, lambda i=i: mix_copy(e, i).start())

    def collect(e, own_part, halo_part):
        own_total = own_part
        halo_total = [halo_part[o * slots : (o + 1) * slots] for o in range(offsets)]
        for distance in order:
            i = distances.index(distance)
            when_there(-distance, lambda i=i: mix_copy(e, i).wait_recv())
            for j, (theirs, mine) in enumerate(pairs[distance]):
                if mine == 0:
                    own_total = owned(own_total, shifts.index(theirs), mix_in.at[e, i, j])
                elif theirs == 0:
                    o = shifts.index(mine)
                    halo_total[o] = halo_total[o] + mix_in[e, i, j]
                else:
                    o, p = shifts.index(mine), shifts.index(theirs)
                    names = links_in[o, o * slots : (o + 1) * slots]
                    for s in range(slots):
                        at = p * slots + s
                        halo_total[o] = halo_total[o] + jnp.where(
                            names == links_in[o, at : at + 1, :], mix_in[e, i, j, s : s + 1, :], 0.0
                        )
        return own_total, halo_total

    def owned(total, o, part):
        for s in range(slots):
            total = total + jnp.where(own_names == send[0, o, s], part[s : s + 1, :], 0.0)
        return total

    def fill(t, own_total, halo_total):
        table[t, 0:own] = own_total
        for o in range(offsets):
            table[t, own + o * slots : own + (o + 1) * slots] = halo_total[o]

    small = lax.broadcasted_iota(jnp.int32, (1, LANES), 1)

    def whole(a):
        return jnp.sum(jnp.sum(a, axis=0, keepdims=True), axis=1, keepdims=True)

    def start_sum(k, terms):
        line = jnp.zeros((1, LANES), f32)
        for i, term in enumerate(terms):
            line = jnp.where(small == i, whole(term), line)
        sum_out[k] = line
        sum_in[k, me] = line

        def push(ahead):
            other = me + ahead
            pltpu.make_async_remote_copy(
                src_ref=sum_out.at[k],
                dst_ref=sum_in.at[k, me],
                send_sem=sum_send_sem.at[k],
                recv_sem=sum_recv_sem.at[k],
                device_id=(jnp.where(other >= n, other - n, other),),
                device_id_type=pl.DeviceIdType.MESH,
            ).start()

        def push_some(first, last):
            steps = (last - first) // PUSH

            def body(i, carry):
                for j in range(PUSH):
                    push(first + i * PUSH + j)
                return carry

            lax.fori_loop(0, steps, body, 0)
            for ahead in range(first + steps * PUSH, last):
                push(ahead)

        push_some(n // 2, n)
        push_some(1, n // 2)

    def sum_bytes(k):
        return sum_in.at[k, pl.ds(0, n - 1)]

    def finish_sum(k, count):
        pltpu.make_async_copy(sum_bytes(k), sum_bytes(k), sum_recv_sem.at[k]).wait()
        line = jnp.sum(sum_in[k], axis=0)
        return [
            jnp.sum(jnp.where(small == i, line, 0.0), axis=1, keepdims=True)
            for i in range(count)
        ]

    own_part, halo_part, _ = operate(0)
    own_part, halo_part = forcing[...] - own_part, -halo_part
    exchange(0, own_part, halo_part)
    next_round(2)
    for o in range(offsets):
        when_there(shifts[o], lambda o=o: link_copy(o).wait_recv())
    own_total, halo_total = collect(0, own_part, halo_part)
    fill(1, own_total, halo_total)
    for i in range(3, len(rounds) + 1):
        next_round(i)

    own_part, halo_part, energy = operate(1)
    exchange(1, own_part, halo_part)
    residual = table[1, 0:own]
    start_sum(0, [residual * residual, energy])
    own_total, halo_total = collect(1, own_part, halo_part)
    fill(2, own_total, halo_total)

    residual, image = table[1, 0:own], table[2, 0:own]
    scalars = []

    def second_sums():
        norm, crossed = finish_sum(0, 2)
        step = norm / crossed
        scalars.extend([norm, crossed, step])

        def pair_energy(g, energy):
            u = [
                vals[0, at_corner(c, g), :] - step * vals[1, at_corner(c, g), :]
                for c in range(3)
            ]
            return energy + element(g, u, True)[1]

        energy = jnp.zeros((ROWS, LANES), f32)
        for g in range(groups):
            energy = pair_energy(g, energy)
        later = residual - step * image
        start_sum(1, [later * later, energy, later * image])

    own_part, halo_part, _ = operate(2, second_sums)
    for o in range(offsets):
        back_out[o] = halo_part[o * slots : (o + 1) * slots]
    for o in range(offsets):
        when_there(shifts[o], lambda o=o: back_copy(o).start())
    norm, crossed, step = scalars
    later = residual - step * image

    for o in range(offsets):
        when_there(-shifts[o], lambda o=o: back_copy(o).wait_recv())
    for o in range(offsets):
        own_part = owned(own_part, o, back_in.at[o])
    applied = image - step * own_part
    for o in range(offsets):
        when_there(-shifts[o], lambda o=o: guess_copy(o).wait_send())
        when_there(-shifts[o], lambda o=o: link_copy(o).wait_send())
        when_there(shifts[o], lambda o=o: back_copy(o).wait_send())
    for e in range(2):
        for i, distance in enumerate(distances):
            when_there(distance, lambda e=e, i=i: mix_copy(e, i).wait_send())
    fresh, own_pair, mixed = finish_sum(1, 3)
    beta = fresh / norm
    next_step = fresh / (own_pair + beta * (2.0 * mixed + beta * crossed))
    both[0:own] = guess[...] + step * residual + next_step * (later + beta * residual)
    both[own : 2 * own] = later - next_step * (applied + beta * image)
    for k in range(2):
        pltpu.make_async_copy(sum_bytes(k), sum_bytes(k), sum_send_sem.at[k]).wait()


def local(
    n,
    forcing,
    first_guess,
    corners,
    gradients,
    element_area,
    element_depth,
    send_blocks,
    recv_blocks,
):
    own, columns = forcing.shape
    _, offsets, slots = send_blocks.shape
    count = element_area.shape[0]
    rows = count // LANES
    nodes = own + offsets * slots
    assert columns == LANES and nodes <= LANES and slots % ROWS == 0
    assert rows % (ROWS * STEP) == 0 and (3 * rows // ROWS) % HEAT == 0
    f32 = jnp.float32
    vmem = pl.BlockSpec(memory_space=pltpu.VMEM)
    dma = pltpu.SemaphoreType.DMA
    pairs = message_pairs(shift_list(offsets))
    most = max(len(listed) for listed in pairs.values())
    part = (offsets, slots, LANES)
    mix = (2, len(pairs), most, slots, LANES)
    both = pl.pallas_call(
        functools.partial(kernel, n),
        out_shape=pltpu.VMEM((2 * own, columns), f32),
        in_specs=[pl.BlockSpec(memory_space=pl.ANY)] * 8,
        out_specs=vmem,
        scratch_shapes=[
            pltpu.VMEM(forcing.shape, f32),
            pltpu.VMEM(first_guess.shape, f32),
            pltpu.VMEM(corners.shape, jnp.int32),
            pltpu.VMEM(gradients.shape, f32),
            pltpu.VMEM((rows, LANES), f32),
            pltpu.VMEM((rows, LANES), f32),
            pltpu.SMEM(send_blocks.shape, jnp.int32),
            pltpu.SMEM(recv_blocks.shape, jnp.int32),
            dma((8,)),
            pltpu.VMEM((3 * rows, LANES), jnp.int32),
            pltpu.VMEM((3 * rows, LANES), jnp.int32),
            pltpu.VMEM((3 * rows, LANES), jnp.int32),
            pltpu.VMEM((3 * count, 2 * LANES), jnp.float8_e4m3fn),
            pltpu.VMEM((4 * rows, LANES), f32),
            pltpu.VMEM((2, 3 * rows, LANES), f32),
            pltpu.VMEM((3 * rows, LANES), f32),
            pltpu.VMEM((3 * rows, LANES), f32),
            pltpu.VMEM((3, nodes, LANES), f32),
            pltpu.VMEM((own, LANES), f32),
            pltpu.VMEM((offsets * slots, LANES), jnp.int32),
            pltpu.VMEM((offsets, offsets * slots, LANES), jnp.int32),
            pltpu.VMEM(part, f32),
            pltpu.VMEM(mix, f32),
            pltpu.VMEM(mix, f32),
            pltpu.VMEM(part, f32),
            pltpu.VMEM(part, f32),
            pltpu.VMEM((2, 1, LANES), f32),
            pltpu.VMEM((2, n, 1, LANES), f32),
            dma((offsets,)),
            dma((offsets,)),
            dma((offsets,)),
            dma((offsets,)),
            dma((2, len(pairs))),
            dma((2, len(pairs))),
            dma((offsets,)),
            dma((offsets,)),
            dma((2,)),
            dma((2,)),
            pltpu.SemaphoreType.REGULAR((len(learning_rounds(n, max(pairs))) + 1, 2)),
        ],
        compiler_params=pltpu.CompilerParams(
            collective_id=0, has_side_effects=True
        ),
    )(
        forcing,
        first_guess,
        corners,
        gradients,
        element_area.reshape(rows, LANES),
        element_depth.reshape(rows, LANES),
        send_blocks,
        recv_blocks,
    )
    return both[:own], both[own:]


def solution(mesh):
    placed = (
        P("dom", None),
        P("dom", None),
        P(None, "dom"),
        P(None, "dom"),
        P("dom"),
        P("dom"),
        P("dom", None, None),
        P("dom", None, None),
    )
    return jax.shard_map(
        functools.partial(local, mesh.shape["dom"]),
        mesh=mesh,
        in_specs=placed,
        out_specs=(P("dom", None), P("dom", None)),
        check_vma=False,
    )
```

```python
import functools

import jax
import jax.numpy as jnp
from jax import lax
from jax.experimental import pallas as pl
from jax.experimental.pallas import tpu as pltpu
from jax.sharding import PartitionSpec as P

LANES = 128
ROWS = 8
HEAT = 6
PARTS = 2
PUSH = 8


def shift_list(offsets):
    half_count = offsets // 2
    return [
        shift_at - half_count if shift_at < half_count else shift_at - half_count + 1
        for shift_at in range(offsets)
    ]


def learning_rounds(n, reach):
    rounds = []
    while reach < n - 1:
        rounds.append(reach)
        reach *= 2
    return rounds


def message_pairs(shifts):
    roles = sorted([0, *shifts])
    reach = max(roles) - min(roles)
    return {
        distance: [(a, b) for a in roles for b in roles if a - b == distance]
        for distance in range(-reach, reach + 1)
        if distance != 0
    }


def kernel(
    n,
    forcing_in,
    guess_in,
    corners_in,
    gradients_in,
    area_in,
    depth_in,
    send_in,
    recv_in,
    both,
    forcing,
    guess,
    corners,
    gradients,
    area,
    depth,
    send,
    recv,
    load_sem,
    blk,
    name,
    lane,
    hot,
    wide_hot,
    split,
    elem,
    vals,
    hi,
    lo,
    table,
    base,
    links,
    links_in,
    guess_out,
    mix_out,
    mix_in,
    back_out,
    back_in,
    sum_out,
    sum_in,
    guess_send_sem,
    guess_recv_sem,
    link_send_sem,
    link_recv_sem,
    mix_send_sem,
    mix_recv_sem,
    back_send_sem,
    back_recv_sem,
    sum_send_sem,
    sum_recv_sem,
    known,
):
    own, _ = forcing.shape
    _, offsets, slots = send.shape
    halo = offsets * slots
    nodes = own + halo
    wide_rows = max(own, halo)
    rows = area.shape[0]
    groups = rows // ROWS
    shifts = shift_list(offsets)
    pairs = message_pairs(shifts)
    distances = list(pairs)
    reach = max(distances)
    order = sorted(distances, key=lambda distance: (-abs(distance), distance))
    me = lax.axis_index("dom")
    f32 = jnp.float32
    bf16 = jnp.bfloat16

    def there(distance):
        return jnp.logical_and(me + distance >= 0, me + distance < n)

    def when_there(distance, action):
        @pl.when(there(distance))
        def _():
            action()

    def remote(source, target, send_sem, recv_sem, distance):
        return pltpu.make_async_remote_copy(
            src_ref=source,
            dst_ref=target,
            send_sem=send_sem,
            recv_sem=recv_sem,
            device_id=(me + distance,),
            device_id_type=pl.DeviceIdType.MESH,
        )

    def guess_copy(o):
        return remote(
            guess_out.at[o],
            table.at[0, pl.ds(own + o * slots, slots)],
            guess_send_sem.at[o],
            guess_recv_sem.at[o],
            -shifts[o],
        )

    def link_copy(o):
        return remote(
            links, links_in.at[o], link_send_sem.at[o], link_recv_sem.at[o], -shifts[o]
        )

    def mix_copy(e, i):
        count = len(pairs[distances[i]])
        return remote(
            mix_out.at[e, i, pl.ds(0, count)],
            mix_in.at[e, i, pl.ds(0, count)],
            mix_send_sem.at[e, i],
            mix_recv_sem.at[e, i],
            distances[i],
        )

    def back_copy(o):
        return remote(
            back_out.at[o], back_in.at[o], back_send_sem.at[o], back_recv_sem.at[o], shifts[o]
        )

    loads = [
        pltpu.make_async_copy(source, target, load_sem.at[i])
        for i, (source, target) in enumerate(
            [
                (send_in, send),
                (guess_in, guess),
                (corners_in, corners),
                (recv_in, recv),
                (gradients_in, gradients),
                (area_in, area),
                (depth_in, depth),
                (forcing_in, forcing),
            ]
        )
    ]
    for load in loads[:3]:
        load.start()
    barrier = pltpu.get_barrier_semaphore()
    for distance in distances:
        when_there(
            distance,
            lambda distance=distance: pl.semaphore_signal(
                barrier,
                inc=1,
                device_id=(me + distance,),
                device_id_type=pl.DeviceIdType.MESH,
            ),
        )

    for load in loads[3:]:
        load.start()
    rounds = learning_rounds(n, reach)

    def tell(i):
        for side in range(2):
            far = rounds[i] * (2 * side - 1)
            when_there(
                far,
                lambda side=side, far=far: pl.semaphore_signal(
                    known.at[i, side],
                    inc=1,
                    device_id=(me + far,),
                    device_id_type=pl.DeviceIdType.MESH,
                ),
            )

    def learn(i):
        for side in range(2):
            far = rounds[i] * (1 - 2 * side)
            when_there(
                far, lambda side=side: pl.semaphore_wait(known.at[i, side], 1)
            )

    def next_round(i):
        if i > 0 and i <= len(rounds):
            learn(i - 1)
        if i < len(rounds):
            tell(i)

    for load in loads[:2]:
        load.wait()
    for o in range(offsets):
        for s in range(slots):
            at = jnp.minimum(send[0, o, s], own - 1)
            guess_out[o, s : s + 1, :] = guess[pl.ds(at, 1), :]
    for o in range(offsets):
        for s in range(slots):
            links[o * slots + s : o * slots + s + 1, :] = jnp.full(
                (1, LANES), send[0, o, s], jnp.int32
            )
    pl.semaphore_wait(
        barrier, jnp.minimum(me, reach) + jnp.minimum(n - 1 - me, reach)
    )
    for o in range(offsets):
        when_there(-shifts[o], lambda o=o: guess_copy(o).start())
    for o in range(offsets):
        when_there(-shifts[o], lambda o=o: link_copy(o).start())
    next_round(0)
    for o in range(offsets):

        @pl.when(jnp.logical_not(there(shifts[o])))
        def _():
            table[0, own + o * slots : own + (o + 1) * slots] = jnp.zeros((slots, LANES), f32)
            links_in[o] = jnp.full((halo, LANES), own, jnp.int32)

        @pl.when(jnp.logical_not(there(-shifts[o])))
        def _():
            back_in[o] = jnp.zeros((slots, LANES), f32)

    for i, distance in enumerate(distances):

        @pl.when(jnp.logical_not(there(-distance)))
        def _():
            for e in range(2):
                mix_in[e, i] = jnp.zeros(mix_in.shape[2:], f32)
    table[0, 0:own] = guess[...]
    for load in loads[2:5]:
        load.wait()

    def lay(r, carry):
        for j in range(ROWS):
            at = pl.multiple_of((r * ROWS + j) * LANES, LANES)
            for c in range(3):
                lane[pl.ds((r * 3 + c) * ROWS + j, 1), :] = corners[c : c + 1, pl.ds(at, LANES)]
            for c in range(4):
                elem[pl.ds((r * 4 + c) * ROWS + j, 1), :] = gradients[c : c + 1, pl.ds(at, LANES)]
        return carry

    lax.fori_loop(0, groups, lay, 0)

    wide = lax.broadcasted_iota(jnp.int32, (ROWS, LANES), 1)
    lookup = jnp.where(wide < own, wide, 2 * LANES)
    for o in range(offsets):
        for s in range(slots):
            lookup = jnp.where(wide == own + recv[0, o, s], own + o * slots + s, lookup)
    lookup = jnp.where(wide < nodes, lookup, 2 * LANES)

    for g in range(3 * groups):
        here = slice(g * ROWS, (g + 1) * ROWS)
        node = lane[here, :]
        block = jnp.take_along_axis(
            lookup, lax.shift_right_logical(node, 7), axis=1, mode="promise_in_bounds"
        )
        blk[here, :] = block
        name[here, :] = jnp.where(block < own, block, block - own)
        hi[here, :] = jnp.where(block < own, 1.0, -1.0)
        lane[here, :] = lax.bitwise_and(node, LANES - 1)

    tall = lax.broadcasted_iota(jnp.int32, (LANES, LANES), 0)

    def heat(g, carry):
        for j in range(HEAT * ROWS):
            at = g * (HEAT * ROWS) + j
            code = jnp.where(lane[pl.ds(at, 1), :] == tall, hi[pl.ds(at, 1), :], 0.0)
            code = code.astype(bf16)
            block, row = divmod(j, ROWS)
            if block % 3 == 1:
                column = (g * (HEAT // 3) + block // 3) * ROWS + row
                columns = pl.ds(pl.multiple_of(column * LANES, LANES), LANES)
                wide_hot[0:LANES, columns] = jnp.maximum(code, 0.0).astype(hot.dtype)
                wide_hot[LANES : 2 * LANES, columns] = jnp.maximum(-code, 0.0).astype(hot.dtype)
            code = code.T
            to = pl.ds(pl.multiple_of(at * LANES, LANES), LANES)
            hot[to, 0:LANES] = jnp.maximum(code, 0.0).astype(hot.dtype)
            hot[to, LANES : 2 * LANES] = jnp.maximum(-code, 0.0).astype(hot.dtype)
        return carry

    lax.fori_loop(0, 3 * groups // HEAT, heat, 0)
    for load in loads[5:]:
        load.wait()
    for o in range(offsets):
        when_there(shifts[o], lambda o=o: guess_copy(o).wait_recv())
    next_round(1)

    own_names = lax.broadcasted_iota(jnp.int32, (own, LANES), 0)
    names = lax.broadcasted_iota(jnp.int32, (wide_rows, LANES), 0)

    def at_corner(c, g):
        return pl.ds(pl.multiple_of((g * 3 + c) * ROWS, ROWS), ROWS)

    sublane = lax.broadcasted_iota(jnp.int32, (ROWS, LANES), 0)
    once = 1 + jnp.minimum(me, 0)

    def operate(t, gathered=None):
        def picked(c, g, count):
            index = lane[at_corner(c, g), :]
            block = blk[at_corner(c, g), :]
            value = jnp.zeros((ROWS, LANES), f32)
            for b in range(count):
                row = jnp.broadcast_to(table[t, b : b + 1, :], (ROWS, LANES))
                got = jnp.take_along_axis(row, index, axis=1, mode="promise_in_bounds")
                value = jnp.where(block == b, got, value)
            return value

        def multiplied(g):
            columns = pl.ds(pl.multiple_of(g * (ROWS * LANES), ROWS * LANES), ROWS * LANES)
            product = lax.dot_general(
                split[...],
                wide_hot[:, columns],
                (((1,), (0,)), ((), ())),
                preferred_element_type=f32,
            )
            product = product[:wide_rows] + product[wide_rows:]
            at = pl.multiple_of((g * 3 + 1) * ROWS, ROWS)
            rows_left = []
            for j in range(ROWS):
                kept = jnp.where(
                    name[pl.ds(at + j, 1), :] == names, product[:, j * LANES : (j + 1) * LANES], 0.0
                )
                kept = [kept[r : r + ROWS] for r in range(0, wide_rows, ROWS)]
                while len(kept) > 1:
                    kept = [a + b for a, b in zip(kept[::2], kept[1::2])]
                rows_left.append(kept[0])
            bit = 1
            while bit < ROWS:
                upper = jnp.bitwise_and(sublane, bit) != 0
                rows_left = [
                    jnp.where(upper, b, a) + pltpu.roll(jnp.where(upper, a, b), bit, axis=0)
                    for a, b in zip(rows_left[::2], rows_left[1::2])
                ]
                bit *= 2
            return rows_left[0]

        def spread(g, energy):
            u = [picked(0, g, own), multiplied(g), picked(2, g, nodes)]
            if t > 0:
                for c in range(3):
                    vals[t - 1, at_corner(c, g), :] = u[c]
            adds, local_energy = element(g, u, t == 1)
            for c in range(3):
                top = adds[c].astype(bf16).astype(f32)
                hi[at_corner(c, g), :] = top
                lo[at_corner(c, g), :] = adds[c] - top
            return energy + local_energy if t == 1 else energy

        def summed(first, last, sums):
            parts = []
            for at in range(first * 3 * ROWS, last * 3 * ROWS):
                mask = name[at : at + 1, :] == names
                parts.append(
                    jnp.concatenate(
                        [
                            jnp.where(mask, hi[at : at + 1, :], 0.0),
                            jnp.where(mask, lo[at : at + 1, :], 0.0),
                        ],
                        axis=0,
                    ).astype(bf16)
                )
            product = lax.dot_general(
                jnp.concatenate(parts, axis=1),
                hot[first * 3 * ROWS * LANES : last * 3 * ROWS * LANES, :],
                (((1,), (0,)), ((), ())),
                preferred_element_type=f32,
            )
            return product if sums is None else sums + product

        bounds = [-(-groups * i // PARTS) for i in range(PARTS + 1)]
        energy = jnp.zeros((ROWS, LANES), f32)
        for g in range(bounds[0], bounds[1]):
            energy = spread(g, energy)
        sums = jnp.zeros((2 * wide_rows, 2 * LANES), f32)
        for part in range(1, PARTS):

            def step(_, carry, part=part):
                sums, energy = carry
                sums = summed(bounds[part - 1], bounds[part], sums)
                for g in range(bounds[part], bounds[part + 1]):
                    energy = spread(g, energy)
                return sums, energy

            sums, energy = lax.fori_loop(0, once, step, (sums, energy))
        if gathered is not None:
            gathered()
        sums = summed(bounds[PARTS - 1], groups, sums)
        sums = sums[:wide_rows] + sums[wide_rows:]
        return sums[:own, :LANES], sums[:halo, LANES:], energy

    def element(g, u, with_energy):
        gx0, gy0, gx1, gy1 = [
            elem[pl.ds(pl.multiple_of((g * 4 + c) * ROWS, ROWS), ROWS), :] for c in range(4)
        ]
        here = pl.ds(pl.multiple_of(g * ROWS, ROWS), ROWS)
        size = area[here, :]
        scaled = depth[here, :] * size
        third = size / 3.0
        from0, from1 = u[0] - u[2], u[1] - u[2]
        raw_x = gx0 * from0 + gx1 * from1
        raw_y = gy0 * from0 + gy1 * from1
        slope_x = scaled * raw_x
        slope_y = scaled * raw_y
        flow0 = gx0 * slope_x + gy0 * slope_y
        flow1 = gx1 * slope_x + gy1 * slope_y
        adds = [
            flow0 + third * u[0],
            flow1 + third * u[1],
            third * u[2] - (flow0 + flow1),
        ]
        if not with_energy:
            return adds, None
        return adds, (
            slope_x * raw_x
            + slope_y * raw_y
            + third * (u[0] * u[0] + u[1] * u[1] + u[2] * u[2])
        )

    def exchange(e, own_part, halo_part):
        base[...] = own_part
        for distance in reversed(order):
            i = distances.index(distance)
            for j, (mine, theirs) in enumerate(pairs[distance]):
                if mine == 0:
                    o = shifts.index(theirs)
                    for s in range(slots):
                        at = jnp.minimum(send[0, o, s], own - 1)
                        mix_out[e, i, j, s : s + 1, :] = base[pl.ds(at, 1), :]
                else:
                    o = shifts.index(mine)
                    mix_out[e, i, j] = halo_part[o * slots : (o + 1) * slots]
            when_there(distance, lambda i=i: mix_copy(e, i).start())

    def collect(e, own_part, halo_part):
        own_total = own_part
        halo_total = [halo_part[o * slots : (o + 1) * slots] for o in range(offsets)]
        for distance in order:
            i = distances.index(distance)
            when_there(-distance, lambda i=i: mix_copy(e, i).wait_recv())
            for j, (theirs, mine) in enumerate(pairs[distance]):
                if mine == 0:
                    own_total = owned(own_total, shifts.index(theirs), mix_in.at[e, i, j])
                elif theirs == 0:
                    o = shifts.index(mine)
                    halo_total[o] = halo_total[o] + mix_in[e, i, j]
                else:
                    o, p = shifts.index(mine), shifts.index(theirs)
                    names = links_in[o, o * slots : (o + 1) * slots]
                    for s in range(slots):
                        at = p * slots + s
                        halo_total[o] = halo_total[o] + jnp.where(
                            names == links_in[o, at : at + 1, :], mix_in[e, i, j, s : s + 1, :], 0.0
                        )
        return own_total, halo_total

    def owned(total, o, part):
        for s in range(slots):
            total = total + jnp.where(own_names == send[0, o, s], part[s : s + 1, :], 0.0)
        return total

    def divide(own_total, halo_total):
        for side, total in enumerate([own_total, halo_total]):
            columns = slice(side * LANES, (side + 1) * LANES)
            top = total.astype(bf16)
            split[0:own, columns] = top
            split[own : 2 * own, columns] = (total - top.astype(f32)).astype(bf16)

    def fill(t, own_total, halo_total):
        halo_total = jnp.concatenate(halo_total, axis=0)
        table[t, 0:own] = own_total
        table[t, own:nodes] = halo_total
        divide(own_total, halo_total)

    small = lax.broadcasted_iota(jnp.int32, (1, LANES), 1)

    def whole(a):
        return jnp.sum(jnp.sum(a, axis=0, keepdims=True), axis=1, keepdims=True)

    def start_sum(k, terms):
        line = jnp.zeros((1, LANES), f32)
        for i, term in enumerate(terms):
            line = jnp.where(small == i, whole(term), line)
        sum_out[k] = line
        sum_in[k, me] = line

        def push(ahead):
            other = me + ahead
            pltpu.make_async_remote_copy(
                src_ref=sum_out.at[k],
                dst_ref=sum_in.at[k, me],
                send_sem=sum_send_sem.at[k],
                recv_sem=sum_recv_sem.at[k],
                device_id=(jnp.where(other >= n, other - n, other),),
                device_id_type=pl.DeviceIdType.MESH,
            ).start()

        def push_some(first, last):
            steps = (last - first) // PUSH

            def body(i, carry):
                for j in range(PUSH):
                    push(first + i * PUSH + j)
                return carry

            lax.fori_loop(0, steps, body, 0)
            for ahead in range(first + steps * PUSH, last):
                push(ahead)

        push_some(n // 2, n)
        push_some(1, n // 2)

    def sum_bytes(k):
        return sum_in.at[k, pl.ds(0, n - 1)]

    def finish_sum(k, count):
        pltpu.make_async_copy(sum_bytes(k), sum_bytes(k), sum_recv_sem.at[k]).wait()
        line = jnp.sum(sum_in[k], axis=0)
        return [
            jnp.sum(jnp.where(small == i, line, 0.0), axis=1, keepdims=True)
            for i in range(count)
        ]

    divide(table[0, 0:own], table[0, own:nodes])
    own_part, halo_part, _ = operate(0)
    own_part, halo_part = forcing[...] - own_part, -halo_part
    exchange(0, own_part, halo_part)
    next_round(2)
    for o in range(offsets):
        when_there(shifts[o], lambda o=o: link_copy(o).wait_recv())
    own_total, halo_total = collect(0, own_part, halo_part)
    fill(1, own_total, halo_total)
    for i in range(3, len(rounds) + 1):
        next_round(i)

    own_part, halo_part, energy = operate(1)
    exchange(1, own_part, halo_part)
    residual = table[1, 0:own]
    start_sum(0, [residual * residual, energy])
    own_total, halo_total = collect(1, own_part, halo_part)
    fill(2, own_total, halo_total)

    residual, image = table[1, 0:own], table[2, 0:own]
    scalars = []

    def second_sums():
        norm, crossed = finish_sum(0, 2)
        step = norm / crossed
        scalars.extend([norm, crossed, step])

        def pair_energy(g, energy):
            u = [
                vals[0, at_corner(c, g), :] - step * vals[1, at_corner(c, g), :]
                for c in range(3)
            ]
            return energy + element(g, u, True)[1]

        energy = jnp.zeros((ROWS, LANES), f32)
        for g in range(groups):
            energy = pair_energy(g, energy)
        later = residual - step * image
        start_sum(1, [later * later, energy, later * image])

    own_part, halo_part, _ = operate(2, second_sums)
    for o in range(offsets):
        back_out[o] = halo_part[o * slots : (o + 1) * slots]
    for o in range(offsets):
        when_there(shifts[o], lambda o=o: back_copy(o).start())
    norm, crossed, step = scalars
    later = residual - step * image

    for o in range(offsets):
        when_there(-shifts[o], lambda o=o: back_copy(o).wait_recv())
    for o in range(offsets):
        own_part = owned(own_part, o, back_in.at[o])
    applied = image - step * own_part
    for o in range(offsets):
        when_there(-shifts[o], lambda o=o: guess_copy(o).wait_send())
        when_there(-shifts[o], lambda o=o: link_copy(o).wait_send())
        when_there(shifts[o], lambda o=o: back_copy(o).wait_send())
    for e in range(2):
        for i, distance in enumerate(distances):
            when_there(distance, lambda e=e, i=i: mix_copy(e, i).wait_send())
    fresh, own_pair, mixed = finish_sum(1, 3)
    beta = fresh / norm
    next_step = fresh / (own_pair + beta * (2.0 * mixed + beta * crossed))
    both[0:own] = guess[...] + step * residual + next_step * (later + beta * residual)
    both[own : 2 * own] = later - next_step * (applied + beta * image)
    for k in range(2):
        pltpu.make_async_copy(sum_bytes(k), sum_bytes(k), sum_send_sem.at[k]).wait()


def local(
    n,
    forcing,
    first_guess,
    corners,
    gradients,
    element_area,
    element_depth,
    send_blocks,
    recv_blocks,
):
    own, columns = forcing.shape
    _, offsets, slots = send_blocks.shape
    count = element_area.shape[0]
    rows = count // LANES
    nodes = own + offsets * slots
    assert columns == LANES and nodes <= LANES and slots % ROWS == 0
    assert rows % ROWS == 0 and (3 * rows // ROWS) % HEAT == 0 and HEAT % 3 == 0
    assert own == offsets * slots and own % (2 * ROWS) == 0
    f32 = jnp.float32
    vmem = pl.BlockSpec(memory_space=pltpu.VMEM)
    dma = pltpu.SemaphoreType.DMA
    pairs = message_pairs(shift_list(offsets))
    most = max(len(listed) for listed in pairs.values())
    part = (offsets, slots, LANES)
    mix = (2, len(pairs), most, slots, LANES)
    both = pl.pallas_call(
        functools.partial(kernel, n),
        out_shape=pltpu.VMEM((2 * own, columns), f32),
        in_specs=[pl.BlockSpec(memory_space=pl.ANY)] * 8,
        out_specs=vmem,
        scratch_shapes=[
            pltpu.VMEM(forcing.shape, f32),
            pltpu.VMEM(first_guess.shape, f32),
            pltpu.VMEM(corners.shape, jnp.int32),
            pltpu.VMEM(gradients.shape, f32),
            pltpu.VMEM((rows, LANES), f32),
            pltpu.VMEM((rows, LANES), f32),
            pltpu.SMEM(send_blocks.shape, jnp.int32),
            pltpu.SMEM(recv_blocks.shape, jnp.int32),
            dma((8,)),
            pltpu.VMEM((3 * rows, LANES), jnp.int32),
            pltpu.VMEM((3 * rows, LANES), jnp.int32),
            pltpu.VMEM((3 * rows, LANES), jnp.int32),
            pltpu.VMEM((3 * count, 2 * LANES), jnp.float8_e4m3fn),
            pltpu.VMEM((2 * LANES, count), jnp.float8_e4m3fn),
            pltpu.VMEM((2 * own, 2 * LANES), jnp.bfloat16),
            pltpu.VMEM((4 * rows, LANES), f32),
            pltpu.VMEM((2, 3 * rows, LANES), f32),
            pltpu.VMEM((3 * rows, LANES), f32),
            pltpu.VMEM((3 * rows, LANES), f32),
            pltpu.VMEM((3, nodes, LANES), f32),
            pltpu.VMEM((own, LANES), f32),
            pltpu.VMEM((offsets * slots, LANES), jnp.int32),
            pltpu.VMEM((offsets, offsets * slots, LANES), jnp.int32),
            pltpu.VMEM(part, f32),
            pltpu.VMEM(mix, f32),
            pltpu.VMEM(mix, f32),
            pltpu.VMEM(part, f32),
            pltpu.VMEM(part, f32),
            pltpu.VMEM((2, 1, LANES), f32),
            pltpu.VMEM((2, n, 1, LANES), f32),
            dma((offsets,)),
            dma((offsets,)),
            dma((offsets,)),
            dma((offsets,)),
            dma((2, len(pairs))),
            dma((2, len(pairs))),
            dma((offsets,)),
            dma((offsets,)),
            dma((2,)),
            dma((2,)),
            pltpu.SemaphoreType.REGULAR((len(learning_rounds(n, max(pairs))) + 1, 2)),
        ],
        compiler_params=pltpu.CompilerParams(
            collective_id=0, has_side_effects=True
        ),
    )(
        forcing,
        first_guess,
        corners,
        gradients,
        element_area.reshape(rows, LANES),
        element_depth.reshape(rows, LANES),
        send_blocks,
        recv_blocks,
    )
    return both[:own], both[own:]


def solution(mesh):
    placed = (
        P("dom", None),
        P("dom", None),
        P(None, "dom"),
        P(None, "dom"),
        P("dom"),
        P("dom"),
        P("dom", None, None),
        P("dom", None, None),
    )
    return jax.shard_map(
        functools.partial(local, mesh.shape["dom"]),
        mesh=mesh,
        in_specs=placed,
        out_specs=(P("dom", None), P("dom", None)),
        check_vma=False,
    )
```

```python
import functools

import jax
import jax.numpy as jnp
from jax import lax
from jax.experimental import pallas as pl
from jax.experimental.pallas import tpu as pltpu
from jax.sharding import PartitionSpec as P

LANES = 128
ROWS = 8
HEAT = 6
PARTS = 2
FIRST = (1, 2)
LATER = ((1,), ())
PUSH = 8


def shift_list(offsets):
    half_count = offsets // 2
    return [
        shift_at - half_count if shift_at < half_count else shift_at - half_count + 1
        for shift_at in range(offsets)
    ]


def learning_rounds(n, reach):
    rounds = []
    while reach < n - 1:
        rounds.append(reach)
        reach *= 2
    return rounds


def message_pairs(shifts):
    roles = sorted([0, *shifts])
    reach = max(roles) - min(roles)
    return {
        distance: [(a, b) for a in roles for b in roles if a - b == distance]
        for distance in range(-reach, reach + 1)
        if distance != 0
    }


def kernel(
    n,
    forcing_in,
    guess_in,
    corners_in,
    gradients_in,
    area_in,
    depth_in,
    send_in,
    recv_in,
    both,
    forcing,
    guess,
    corners,
    gradients,
    area,
    depth,
    send,
    recv,
    load_sem,
    blk,
    name,
    lane,
    hot,
    wide_hot,
    split,
    elem,
    vals,
    hi,
    lo,
    table,
    base,
    links,
    links_in,
    guess_out,
    mix_out,
    mix_in,
    back_out,
    back_in,
    sum_out,
    sum_in,
    guess_send_sem,
    guess_recv_sem,
    link_send_sem,
    link_recv_sem,
    mix_send_sem,
    mix_recv_sem,
    back_send_sem,
    back_recv_sem,
    sum_send_sem,
    sum_recv_sem,
    known,
):
    own, _ = forcing.shape
    _, offsets, slots = send.shape
    halo = offsets * slots
    nodes = own + halo
    wide_rows = max(own, halo)
    rows = area.shape[0]
    groups = rows // ROWS
    shifts = shift_list(offsets)
    pairs = message_pairs(shifts)
    distances = list(pairs)
    reach = max(distances)
    order = sorted(distances, key=lambda distance: (-abs(distance), distance))
    me = lax.axis_index("dom")
    f32 = jnp.float32
    bf16 = jnp.bfloat16

    def there(distance):
        return jnp.logical_and(me + distance >= 0, me + distance < n)

    def when_there(distance, action):
        @pl.when(there(distance))
        def _():
            action()

    def remote(source, target, send_sem, recv_sem, distance):
        return pltpu.make_async_remote_copy(
            src_ref=source,
            dst_ref=target,
            send_sem=send_sem,
            recv_sem=recv_sem,
            device_id=(me + distance,),
            device_id_type=pl.DeviceIdType.MESH,
        )

    def guess_copy(o):
        return remote(
            guess_out.at[o],
            table.at[0, pl.ds(own + o * slots, slots)],
            guess_send_sem.at[o],
            guess_recv_sem.at[o],
            -shifts[o],
        )

    def link_copy(o):
        return remote(
            links, links_in.at[o], link_send_sem.at[o], link_recv_sem.at[o], -shifts[o]
        )

    def mix_copy(e, i):
        count = len(pairs[distances[i]])
        return remote(
            mix_out.at[e, i, pl.ds(0, count)],
            mix_in.at[e, i, pl.ds(0, count)],
            mix_send_sem.at[e, i],
            mix_recv_sem.at[e, i],
            distances[i],
        )

    def back_copy(o):
        return remote(
            back_out.at[o], back_in.at[o], back_send_sem.at[o], back_recv_sem.at[o], shifts[o]
        )

    loads = [
        pltpu.make_async_copy(source, target, load_sem.at[i])
        for i, (source, target) in enumerate(
            [
                (send_in, send),
                (guess_in, guess),
                (corners_in, corners),
                (recv_in, recv),
                (gradients_in, gradients),
                (area_in, area),
                (depth_in, depth),
                (forcing_in, forcing),
            ]
        )
    ]
    for load in loads[:3]:
        load.start()
    barrier = pltpu.get_barrier_semaphore()
    for distance in distances:
        when_there(
            distance,
            lambda distance=distance: pl.semaphore_signal(
                barrier,
                inc=1,
                device_id=(me + distance,),
                device_id_type=pl.DeviceIdType.MESH,
            ),
        )

    for load in loads[3:]:
        load.start()
    rounds = learning_rounds(n, reach)

    def tell(i):
        for side in range(2):
            far = rounds[i] * (2 * side - 1)
            when_there(
                far,
                lambda side=side, far=far: pl.semaphore_signal(
                    known.at[i, side],
                    inc=1,
                    device_id=(me + far,),
                    device_id_type=pl.DeviceIdType.MESH,
                ),
            )

    def learn(i):
        for side in range(2):
            far = rounds[i] * (1 - 2 * side)
            when_there(
                far, lambda side=side: pl.semaphore_wait(known.at[i, side], 1)
            )

    def next_round(i):
        if i > 0 and i <= len(rounds):
            learn(i - 1)
        if i < len(rounds):
            tell(i)

    for load in loads[:2]:
        load.wait()
    for o in range(offsets):
        for s in range(slots):
            at = jnp.minimum(send[0, o, s], own - 1)
            guess_out[o, s : s + 1, :] = guess[pl.ds(at, 1), :]
    for o in range(offsets):
        for s in range(slots):
            links[o * slots + s : o * slots + s + 1, :] = jnp.full(
                (1, LANES), send[0, o, s], jnp.int32
            )
    pl.semaphore_wait(
        barrier, jnp.minimum(me, reach) + jnp.minimum(n - 1 - me, reach)
    )
    for o in range(offsets):
        when_there(-shifts[o], lambda o=o: guess_copy(o).start())
    for o in range(offsets):
        when_there(-shifts[o], lambda o=o: link_copy(o).start())
    next_round(0)
    for o in range(offsets):

        @pl.when(jnp.logical_not(there(shifts[o])))
        def _():
            table[0, own + o * slots : own + (o + 1) * slots] = jnp.zeros((slots, LANES), f32)
            links_in[o] = jnp.full((halo, LANES), own, jnp.int32)

        @pl.when(jnp.logical_not(there(-shifts[o])))
        def _():
            back_in[o] = jnp.zeros((slots, LANES), f32)

    for i, distance in enumerate(distances):

        @pl.when(jnp.logical_not(there(-distance)))
        def _():
            for e in range(2):
                mix_in[e, i] = jnp.zeros(mix_in.shape[2:], f32)
    table[0, 0:own] = guess[...]
    for load in loads[2:5]:
        load.wait()

    def lay(r, carry):
        for j in range(ROWS):
            at = pl.multiple_of((r * ROWS + j) * LANES, LANES)
            for c in range(3):
                lane[pl.ds((r * 3 + c) * ROWS + j, 1), :] = corners[c : c + 1, pl.ds(at, LANES)]
            for c in range(4):
                elem[pl.ds((r * 4 + c) * ROWS + j, 1), :] = gradients[c : c + 1, pl.ds(at, LANES)]
        return carry

    lax.fori_loop(0, groups, lay, 0)

    wide = lax.broadcasted_iota(jnp.int32, (ROWS, LANES), 1)
    lookup = jnp.where(wide < own, wide, 2 * LANES)
    for o in range(offsets):
        for s in range(slots):
            lookup = jnp.where(wide == own + recv[0, o, s], own + o * slots + s, lookup)
    lookup = jnp.where(wide < nodes, lookup, 2 * LANES)

    for g in range(3 * groups):
        here = slice(g * ROWS, (g + 1) * ROWS)
        node = lane[here, :]
        block = jnp.take_along_axis(
            lookup, lax.shift_right_logical(node, 7), axis=1, mode="promise_in_bounds"
        )
        blk[here, :] = block
        name[here, :] = jnp.where(block < own, block, block - own)
        hi[here, :] = jnp.where(block < own, 1.0, -1.0)
        lane[here, :] = lax.bitwise_and(node, LANES - 1)

    tall = lax.broadcasted_iota(jnp.int32, (LANES, LANES), 0).astype(f32).astype(bf16)

    def heat(g, carry):
        for j in range(HEAT * ROWS):
            at = g * (HEAT * ROWS) + j

            def filled(ref):
                row = jnp.broadcast_to(ref[pl.ds(at, 1), :].astype(f32), (2 * ROWS, LANES))
                return jnp.concatenate([row.astype(bf16)] * (LANES // (2 * ROWS)), axis=0)

            code = jnp.where(filled(lane) == tall, filled(hi), jnp.zeros((LANES, LANES), bf16))
            block, row = divmod(j, ROWS)
            if block % 3 > 0:
                column = (g * (HEAT // 3) + block // 3) * ROWS + row
                columns = pl.ds(pl.multiple_of(column * LANES, LANES), LANES)
                side = block % 3 - 1
                wide_hot[side, 0:LANES, columns] = jnp.maximum(code, 0.0).astype(hot.dtype)
                wide_hot[side, LANES : 2 * LANES, columns] = jnp.maximum(-code, 0.0).astype(hot.dtype)
            code = code.T
            to = pl.ds(pl.multiple_of(at * LANES, LANES), LANES)
            hot[to, 0:LANES] = jnp.maximum(code, 0.0).astype(hot.dtype)
            hot[to, LANES : 2 * LANES] = jnp.maximum(-code, 0.0).astype(hot.dtype)
        return carry

    lax.fori_loop(0, 3 * groups // HEAT, heat, 0)
    for load in loads[5:]:
        load.wait()
    for o in range(offsets):
        when_there(shifts[o], lambda o=o: guess_copy(o).wait_recv())
    next_round(1)

    own_names = lax.broadcasted_iota(jnp.int32, (own, LANES), 0)
    names = lax.broadcasted_iota(jnp.int32, (wide_rows, LANES), 0)

    def at_corner(c, g):
        return pl.ds(pl.multiple_of((g * 3 + c) * ROWS, ROWS), ROWS)

    sublane = lax.broadcasted_iota(jnp.int32, (ROWS, LANES), 0)
    once = 1 + jnp.minimum(me, 0)

    def operate(t, gathered=None):
        def picked(c, g, count):
            index = lane[at_corner(c, g), :]
            block = blk[at_corner(c, g), :]
            value = jnp.zeros((ROWS, LANES), f32)
            for b in range(count):
                row = jnp.broadcast_to(table[t, b : b + 1, :], (ROWS, LANES))
                got = jnp.take_along_axis(row, index, axis=1, mode="promise_in_bounds")
                value = jnp.where(block == b, got, value)
            return value

        def multiplied(c, g):
            columns = pl.ds(pl.multiple_of(g * (ROWS * LANES), ROWS * LANES), ROWS * LANES)
            product = lax.dot_general(
                split[...],
                wide_hot[c - 1, :, columns],
                (((1,), (0,)), ((), ())),
                preferred_element_type=f32,
            )
            product = product[:wide_rows] + product[wide_rows:]
            at = pl.multiple_of((g * 3 + c) * ROWS, ROWS)
            rows_left = []
            for j in range(ROWS):
                kept = jnp.where(
                    name[pl.ds(at + j, 1), :] == names, product[:, j * LANES : (j + 1) * LANES], 0.0
                )
                kept = [kept[r : r + ROWS] for r in range(0, wide_rows, ROWS)]
                while len(kept) > 1:
                    kept = [a + b for a, b in zip(kept[::2], kept[1::2])]
                rows_left.append(kept[0])
            bit = 1
            while bit < ROWS:
                upper = jnp.bitwise_and(sublane, bit) != 0
                rows_left = [
                    jnp.where(upper, b, a) + pltpu.roll(jnp.where(upper, a, b), bit, axis=0)
                    for a, b in zip(rows_left[::2], rows_left[1::2])
                ]
                bit *= 2
            return rows_left[0]

        def spread(g, energy, products):
            u = [picked(0, g, own)] + [
                multiplied(c, g) if c in products else picked(c, g, nodes) for c in (1, 2)
            ]
            if t > 0:
                for c in range(3):
                    vals[t - 1, at_corner(c, g), :] = u[c]
            adds, local_energy = element(g, u, t == 1)
            for c in range(3):
                top = adds[c].astype(bf16).astype(f32)
                hi[at_corner(c, g), :] = top
                lo[at_corner(c, g), :] = adds[c] - top
            return energy + local_energy if t == 1 else energy

        def summed(first, last, sums):
            parts = []
            for at in range(first * 3 * ROWS, last * 3 * ROWS):
                mask = name[at : at + 1, :] == names
                parts.append(
                    jnp.concatenate(
                        [
                            jnp.where(mask, hi[at : at + 1, :], 0.0),
                            jnp.where(mask, lo[at : at + 1, :], 0.0),
                        ],
                        axis=0,
                    ).astype(bf16)
                )
            product = lax.dot_general(
                jnp.concatenate(parts, axis=1),
                hot[first * 3 * ROWS * LANES : last * 3 * ROWS * LANES, :],
                (((1,), (0,)), ((), ())),
                preferred_element_type=f32,
            )
            return product if sums is None else sums + product

        bounds = [-(-groups * i // PARTS) for i in range(PARTS + 1)]
        energy = jnp.zeros((ROWS, LANES), f32)
        for g in range(bounds[0], bounds[1]):
            energy = spread(g, energy, FIRST)
        sums = jnp.zeros((2 * wide_rows, 2 * LANES), f32)
        for part in range(1, PARTS):

            def step(_, carry, part=part):
                sums, energy = carry
                sums = summed(bounds[part - 1], bounds[part], sums)
                for g in range(bounds[part], bounds[part + 1]):
                    energy = spread(g, energy, LATER[(g - bounds[part]) % len(LATER)])
                return sums, energy

            sums, energy = lax.fori_loop(0, once, step, (sums, energy))
        if gathered is not None:
            gathered()
        sums = lax.fori_loop(
            0, once, lambda _, sums: summed(bounds[PARTS - 1], groups, sums), sums
        )
        sums = sums[:wide_rows] + sums[wide_rows:]
        return sums[:own, :LANES], sums[:halo, LANES:], energy

    def element(g, u, with_energy):
        gx0, gy0, gx1, gy1 = [
            elem[pl.ds(pl.multiple_of((g * 4 + c) * ROWS, ROWS), ROWS), :] for c in range(4)
        ]
        here = pl.ds(pl.multiple_of(g * ROWS, ROWS), ROWS)
        size = area[here, :]
        scaled = depth[here, :] * size
        third = size / 3.0
        from0, from1 = u[0] - u[2], u[1] - u[2]
        raw_x = gx0 * from0 + gx1 * from1
        raw_y = gy0 * from0 + gy1 * from1
        slope_x = scaled * raw_x
        slope_y = scaled * raw_y
        flow0 = gx0 * slope_x + gy0 * slope_y
        flow1 = gx1 * slope_x + gy1 * slope_y
        adds = [
            flow0 + third * u[0],
            flow1 + third * u[1],
            third * u[2] - (flow0 + flow1),
        ]
        if not with_energy:
            return adds, None
        return adds, (
            slope_x * raw_x
            + slope_y * raw_y
            + third * (u[0] * u[0] + u[1] * u[1] + u[2] * u[2])
        )

    def exchange(e, own_part, halo_part):
        base[...] = own_part
        for distance in reversed(order):
            i = distances.index(distance)
            for j, (mine, theirs) in enumerate(pairs[distance]):
                if mine == 0:
                    o = shifts.index(theirs)
                    for s in range(slots):
                        at = jnp.minimum(send[0, o, s], own - 1)
                        mix_out[e, i, j, s : s + 1, :] = base[pl.ds(at, 1), :]
                else:
                    o = shifts.index(mine)
                    mix_out[e, i, j] = halo_part[o * slots : (o + 1) * slots]
            when_there(distance, lambda i=i: mix_copy(e, i).start())

    def collect(e, own_part, halo_part):
        own_total = own_part
        halo_total = [halo_part[o * slots : (o + 1) * slots] for o in range(offsets)]
        for distance in order:
            i = distances.index(distance)
            when_there(-distance, lambda i=i: mix_copy(e, i).wait_recv())
            for j, (theirs, mine) in enumerate(pairs[distance]):
                if mine == 0:
                    own_total = owned(own_total, shifts.index(theirs), mix_in.at[e, i, j])
                elif theirs == 0:
                    o = shifts.index(mine)
                    halo_total[o] = halo_total[o] + mix_in[e, i, j]
                else:
                    o, p = shifts.index(mine), shifts.index(theirs)
                    names = links_in[o, o * slots : (o + 1) * slots]
                    for s in range(slots):
                        at = p * slots + s
                        halo_total[o] = halo_total[o] + jnp.where(
                            names == links_in[o, at : at + 1, :], mix_in[e, i, j, s : s + 1, :], 0.0
                        )
        return own_total, halo_total

    def owned(total, o, part):
        for s in range(slots):
            total = total + jnp.where(own_names == send[0, o, s], part[s : s + 1, :], 0.0)
        return total

    def divide(own_total, halo_total):
        for side, total in enumerate([own_total, halo_total]):
            columns = slice(side * LANES, (side + 1) * LANES)
            top = total.astype(bf16)
            split[0:own, columns] = top
            split[own : 2 * own, columns] = (total - top.astype(f32)).astype(bf16)

    def fill(t, own_total, halo_total):
        halo_total = jnp.concatenate(halo_total, axis=0)
        table[t, 0:own] = own_total
        table[t, own:nodes] = halo_total
        divide(own_total, halo_total)

    small = lax.broadcasted_iota(jnp.int32, (1, LANES), 1)

    def whole(a):
        return jnp.sum(jnp.sum(a, axis=0, keepdims=True), axis=1, keepdims=True)

    def start_sum(k, terms):
        line = jnp.zeros((1, LANES), f32)
        for i, term in enumerate(terms):
            line = jnp.where(small == i, whole(term), line)
        sum_out[k] = line
        sum_in[k, me] = line

        def push(ahead):
            other = me + ahead
            pltpu.make_async_remote_copy(
                src_ref=sum_out.at[k],
                dst_ref=sum_in.at[k, me],
                send_sem=sum_send_sem.at[k],
                recv_sem=sum_recv_sem.at[k],
                device_id=(jnp.where(other >= n, other - n, other),),
                device_id_type=pl.DeviceIdType.MESH,
            ).start()

        def push_some(first, last):
            steps = (last - first) // PUSH

            def body(i, carry):
                for j in range(PUSH):
                    push(first + i * PUSH + j)
                return carry

            lax.fori_loop(0, steps, body, 0)
            for ahead in range(first + steps * PUSH, last):
                push(ahead)

        push_some(n // 2, n)
        push_some(1, n // 2)

    def sum_bytes(k):
        return sum_in.at[k, pl.ds(0, n - 1)]

    def finish_sum(k, count):
        pltpu.make_async_copy(sum_bytes(k), sum_bytes(k), sum_recv_sem.at[k]).wait()
        line = jnp.sum(sum_in[k], axis=0)
        return [
            jnp.sum(jnp.where(small == i, line, 0.0), axis=1, keepdims=True)
            for i in range(count)
        ]

    divide(table[0, 0:own], table[0, own:nodes])
    own_part, halo_part, _ = operate(0)
    own_part, halo_part = forcing[...] - own_part, -halo_part
    exchange(0, own_part, halo_part)
    next_round(2)
    for o in range(offsets):
        when_there(shifts[o], lambda o=o: link_copy(o).wait_recv())
    own_total, halo_total = collect(0, own_part, halo_part)
    fill(1, own_total, halo_total)
    for i in range(3, len(rounds) + 1):
        next_round(i)

    own_part, halo_part, energy = operate(1)
    exchange(1, own_part, halo_part)
    residual = table[1, 0:own]
    start_sum(0, [residual * residual, energy])
    own_total, halo_total = collect(1, own_part, halo_part)
    fill(2, own_total, halo_total)

    residual, image = table[1, 0:own], table[2, 0:own]
    scalars = []

    def second_sums():
        norm, crossed = finish_sum(0, 2)
        step = norm / crossed
        scalars.extend([norm, crossed, step])

        def pair_energy(g, energy):
            u = [
                vals[0, at_corner(c, g), :] - step * vals[1, at_corner(c, g), :]
                for c in range(3)
            ]
            return energy + element(g, u, True)[1]

        energy = jnp.zeros((ROWS, LANES), f32)
        for g in range(groups):
            energy = pair_energy(g, energy)
        later = residual - step * image
        start_sum(1, [later * later, energy, later * image])

    own_part, halo_part, _ = operate(2, second_sums)
    for o in range(offsets):
        back_out[o] = halo_part[o * slots : (o + 1) * slots]
    for o in range(offsets):
        when_there(shifts[o], lambda o=o: back_copy(o).start())
    norm, crossed, step = scalars
    later = residual - step * image

    for o in range(offsets):
        when_there(-shifts[o], lambda o=o: back_copy(o).wait_recv())
    for o in range(offsets):
        own_part = owned(own_part, o, back_in.at[o])
    applied = image - step * own_part
    for o in range(offsets):
        when_there(-shifts[o], lambda o=o: guess_copy(o).wait_send())
        when_there(-shifts[o], lambda o=o: link_copy(o).wait_send())
        when_there(shifts[o], lambda o=o: back_copy(o).wait_send())
    for e in range(2):
        for i, distance in enumerate(distances):
            when_there(distance, lambda e=e, i=i: mix_copy(e, i).wait_send())
    fresh, own_pair, mixed = finish_sum(1, 3)
    beta = fresh / norm
    next_step = fresh / (own_pair + beta * (2.0 * mixed + beta * crossed))
    both[0:own] = guess[...] + step * residual + next_step * (later + beta * residual)
    both[own : 2 * own] = later - next_step * (applied + beta * image)
    for k in range(2):
        pltpu.make_async_copy(sum_bytes(k), sum_bytes(k), sum_send_sem.at[k]).wait()


def local(
    n,
    forcing,
    first_guess,
    corners,
    gradients,
    element_area,
    element_depth,
    send_blocks,
    recv_blocks,
):
    own, columns = forcing.shape
    _, offsets, slots = send_blocks.shape
    count = element_area.shape[0]
    rows = count // LANES
    nodes = own + offsets * slots
    assert columns == LANES and nodes <= LANES and slots % ROWS == 0
    assert rows % ROWS == 0 and (3 * rows // ROWS) % HEAT == 0 and HEAT % 3 == 0
    assert own == offsets * slots and own % (2 * ROWS) == 0
    f32 = jnp.float32
    vmem = pl.BlockSpec(memory_space=pltpu.VMEM)
    dma = pltpu.SemaphoreType.DMA
    pairs = message_pairs(shift_list(offsets))
    most = max(len(listed) for listed in pairs.values())
    part = (offsets, slots, LANES)
    mix = (2, len(pairs), most, slots, LANES)
    both = pl.pallas_call(
        functools.partial(kernel, n),
        out_shape=pltpu.VMEM((2 * own, columns), f32),
        in_specs=[pl.BlockSpec(memory_space=pl.ANY)] * 8,
        out_specs=vmem,
        scratch_shapes=[
            pltpu.VMEM(forcing.shape, f32),
            pltpu.VMEM(first_guess.shape, f32),
            pltpu.VMEM(corners.shape, jnp.int32),
            pltpu.VMEM(gradients.shape, f32),
            pltpu.VMEM((rows, LANES), f32),
            pltpu.VMEM((rows, LANES), f32),
            pltpu.SMEM(send_blocks.shape, jnp.int32),
            pltpu.SMEM(recv_blocks.shape, jnp.int32),
            dma((8,)),
            pltpu.VMEM((3 * rows, LANES), jnp.int32),
            pltpu.VMEM((3 * rows, LANES), jnp.int32),
            pltpu.VMEM((3 * rows, LANES), jnp.int32),
            pltpu.VMEM((3 * count, 2 * LANES), jnp.float8_e4m3fn),
            pltpu.VMEM((2, 2 * LANES, count), jnp.float8_e4m3fn),
            pltpu.VMEM((2 * own, 2 * LANES), jnp.bfloat16),
            pltpu.VMEM((4 * rows, LANES), f32),
            pltpu.VMEM((2, 3 * rows, LANES), f32),
            pltpu.VMEM((3 * rows, LANES), f32),
            pltpu.VMEM((3 * rows, LANES), f32),
            pltpu.VMEM((3, nodes, LANES), f32),
            pltpu.VMEM((own, LANES), f32),
            pltpu.VMEM((offsets * slots, LANES), jnp.int32),
            pltpu.VMEM((offsets, offsets * slots, LANES), jnp.int32),
            pltpu.VMEM(part, f32),
            pltpu.VMEM(mix, f32),
            pltpu.VMEM(mix, f32),
            pltpu.VMEM(part, f32),
            pltpu.VMEM(part, f32),
            pltpu.VMEM((2, 1, LANES), f32),
            pltpu.VMEM((2, n, 1, LANES), f32),
            dma((offsets,)),
            dma((offsets,)),
            dma((offsets,)),
            dma((offsets,)),
            dma((2, len(pairs))),
            dma((2, len(pairs))),
            dma((offsets,)),
            dma((offsets,)),
            dma((2,)),
            dma((2,)),
            pltpu.SemaphoreType.REGULAR((len(learning_rounds(n, max(pairs))) + 1, 2)),
        ],
        compiler_params=pltpu.CompilerParams(
            collective_id=0, has_side_effects=True
        ),
    )(
        forcing,
        first_guess,
        corners,
        gradients,
        element_area.reshape(rows, LANES),
        element_depth.reshape(rows, LANES),
        send_blocks,
        recv_blocks,
    )
    return both[:own], both[own:]


def solution(mesh):
    placed = (
        P("dom", None),
        P("dom", None),
        P(None, "dom"),
        P(None, "dom"),
        P("dom"),
        P("dom"),
        P("dom", None, None),
        P("dom", None, None),
    )
    return jax.shard_map(
        functools.partial(local, mesh.shape["dom"]),
        mesh=mesh,
        in_specs=placed,
        out_specs=(P("dom", None), P("dom", None)),
        check_vma=False,
    )
```

```python
import functools

import jax
import jax.numpy as jnp
from jax import lax
from jax.experimental import pallas as pl
from jax.experimental.pallas import tpu as pltpu
from jax.sharding import PartitionSpec as P

LANES = 128
ROWS = 8
HEAT = 6
PARTS = 2
FIRST = (1, 2)
LATER = ((1,), ())
PUSH = 8


def shift_list(offsets):
    half_count = offsets // 2
    return [
        shift_at - half_count if shift_at < half_count else shift_at - half_count + 1
        for shift_at in range(offsets)
    ]


def learning_rounds(n, reach):
    rounds = []
    while reach < n - 1:
        rounds.append(reach)
        reach *= 2
    return rounds


def message_pairs(shifts):
    roles = sorted([0, *shifts])
    reach = max(roles) - min(roles)
    return {
        distance: [(a, b) for a in roles for b in roles if a - b == distance]
        for distance in range(-reach, reach + 1)
        if distance != 0
    }


def kernel(
    n,
    forcing_in,
    guess_in,
    corners_in,
    gradients_in,
    area_in,
    depth_in,
    send_in,
    recv_in,
    both,
    forcing,
    guess,
    corners,
    gradients,
    area,
    depth,
    send,
    recv,
    load_sem,
    blk,
    name,
    lane,
    hot,
    wide_hot,
    split,
    elem,
    vals,
    hi,
    lo,
    table,
    base,
    links,
    links_in,
    guess_out,
    mix_out,
    mix_in,
    back_out,
    back_in,
    sum_out,
    sum_in,
    guess_send_sem,
    guess_recv_sem,
    link_send_sem,
    link_recv_sem,
    mix_send_sem,
    mix_recv_sem,
    back_send_sem,
    back_recv_sem,
    sum_send_sem,
    sum_recv_sem,
    known,
):
    own, _ = forcing.shape
    _, offsets, slots = send.shape
    halo = offsets * slots
    nodes = own + halo
    wide_rows = max(own, halo)
    rows = area.shape[0]
    groups = rows // ROWS
    shifts = shift_list(offsets)
    pairs = message_pairs(shifts)
    distances = list(pairs)
    reach = max(distances)
    order = sorted(distances, key=lambda distance: (-abs(distance), distance))
    me = lax.axis_index("dom")
    f32 = jnp.float32
    bf16 = jnp.bfloat16

    def there(distance):
        return jnp.logical_and(me + distance >= 0, me + distance < n)

    def when_there(distance, action):
        @pl.when(there(distance))
        def _():
            action()

    def remote(source, target, send_sem, recv_sem, distance):
        return pltpu.make_async_remote_copy(
            src_ref=source,
            dst_ref=target,
            send_sem=send_sem,
            recv_sem=recv_sem,
            device_id=(me + distance,),
            device_id_type=pl.DeviceIdType.MESH,
        )

    def guess_copy(o):
        return remote(
            guess_out.at[o],
            table.at[0, pl.ds(own + o * slots, slots)],
            guess_send_sem.at[o],
            guess_recv_sem.at[o],
            -shifts[o],
        )

    def link_copy(o):
        return remote(
            links, links_in.at[o], link_send_sem.at[o], link_recv_sem.at[o], -shifts[o]
        )

    def mix_copy(e, i):
        count = len(pairs[distances[i]])
        return remote(
            mix_out.at[e, i, pl.ds(0, count)],
            mix_in.at[e, i, pl.ds(0, count)],
            mix_send_sem.at[e, i],
            mix_recv_sem.at[e, i],
            distances[i],
        )

    def back_copy(o):
        return remote(
            back_out.at[o], back_in.at[o], back_send_sem.at[o], back_recv_sem.at[o], shifts[o]
        )

    loads = [
        pltpu.make_async_copy(source, target, load_sem.at[i])
        for i, (source, target) in enumerate(
            [
                (send_in, send),
                (guess_in, guess),
                (corners_in, corners),
                (recv_in, recv),
                (gradients_in, gradients),
                (area_in, area),
                (depth_in, depth),
                (forcing_in, forcing),
            ]
        )
    ]
    for load in loads[:3]:
        load.start()
    barrier = pltpu.get_barrier_semaphore()
    for distance in distances:
        when_there(
            distance,
            lambda distance=distance: pl.semaphore_signal(
                barrier,
                inc=1,
                device_id=(me + distance,),
                device_id_type=pl.DeviceIdType.MESH,
            ),
        )

    for load in loads[3:]:
        load.start()
    rounds = learning_rounds(n, reach)

    def tell(i):
        for side in range(2):
            far = rounds[i] * (2 * side - 1)
            when_there(
                far,
                lambda side=side, far=far: pl.semaphore_signal(
                    known.at[i, side],
                    inc=1,
                    device_id=(me + far,),
                    device_id_type=pl.DeviceIdType.MESH,
                ),
            )

    def learn(i):
        for side in range(2):
            far = rounds[i] * (1 - 2 * side)
            when_there(
                far, lambda side=side: pl.semaphore_wait(known.at[i, side], 1)
            )

    def next_round(i):
        if i > 0 and i <= len(rounds):
            learn(i - 1)
        if i < len(rounds):
            tell(i)

    for load in loads[:2]:
        load.wait()
    for o in range(offsets):
        for s in range(slots):
            at = jnp.minimum(send[0, o, s], own - 1)
            guess_out[o, s : s + 1, :] = guess[pl.ds(at, 1), :]
    for o in range(offsets):
        for s in range(slots):
            links[o * slots + s : o * slots + s + 1, :] = jnp.full(
                (1, LANES), send[0, o, s], jnp.int32
            )
    pl.semaphore_wait(
        barrier, jnp.minimum(me, reach) + jnp.minimum(n - 1 - me, reach)
    )
    for o in range(offsets):
        when_there(-shifts[o], lambda o=o: guess_copy(o).start())
    for o in range(offsets):
        when_there(-shifts[o], lambda o=o: link_copy(o).start())
    next_round(0)
    for o in range(offsets):

        @pl.when(jnp.logical_not(there(shifts[o])))
        def _():
            table[0, own + o * slots : own + (o + 1) * slots] = jnp.zeros((slots, LANES), f32)
            links_in[o] = jnp.full((halo, LANES), own, jnp.int32)

        @pl.when(jnp.logical_not(there(-shifts[o])))
        def _():
            back_in[o] = jnp.zeros((slots, LANES), f32)

    for i, distance in enumerate(distances):

        @pl.when(jnp.logical_not(there(-distance)))
        def _():
            for e in range(2):
                mix_in[e, i] = jnp.zeros(mix_in.shape[2:], f32)
    table[0, 0:own] = guess[...]
    for load in loads[2:5]:
        load.wait()

    def lay(r, carry):
        for j in range(ROWS):
            at = pl.multiple_of((r * ROWS + j) * LANES, LANES)
            for c in range(3):
                lane[pl.ds((r * 3 + c) * ROWS + j, 1), :] = corners[c : c + 1, pl.ds(at, LANES)]
            for c in range(4):
                elem[pl.ds((r * 4 + c) * ROWS + j, 1), :] = gradients[c : c + 1, pl.ds(at, LANES)]
        return carry

    lax.fori_loop(0, groups, lay, 0)

    wide = lax.broadcasted_iota(jnp.int32, (ROWS, LANES), 1)
    lookup = jnp.where(wide < own, wide, 2 * LANES)
    for o in range(offsets):
        for s in range(slots):
            lookup = jnp.where(wide == own + recv[0, o, s], own + o * slots + s, lookup)
    lookup = jnp.where(wide < nodes, lookup, 2 * LANES)

    for g in range(3 * groups):
        here = slice(g * ROWS, (g + 1) * ROWS)
        node = lane[here, :]
        block = jnp.take_along_axis(
            lookup, lax.shift_right_logical(node, 7), axis=1, mode="promise_in_bounds"
        )
        blk[here, :] = block
        name[here, :] = jnp.where(block < own, block, block - own)
        hi[here, :] = jnp.where(block < own, 1.0, -1.0)
        lane[here, :] = lax.bitwise_and(node, LANES - 1)

    tall = lax.broadcasted_iota(jnp.int32, (LANES, LANES), 0).astype(f32).astype(bf16)

    def heat(g, carry):
        for j in range(HEAT * ROWS):
            at = g * (HEAT * ROWS) + j

            def filled(ref):
                row = jnp.broadcast_to(ref[pl.ds(at, 1), :].astype(f32), (2 * ROWS, LANES))
                return jnp.concatenate([row.astype(bf16)] * (LANES // (2 * ROWS)), axis=0)

            code = jnp.where(filled(lane) == tall, filled(hi), jnp.zeros((LANES, LANES), bf16))
            block, row = divmod(j, ROWS)
            if block % 3 > 0:
                column = (g * (HEAT // 3) + block // 3) * ROWS + row
                columns = pl.ds(pl.multiple_of(column * LANES, LANES), LANES)
                side = block % 3 - 1
                wide_hot[side, 0:LANES, columns] = jnp.maximum(code, 0.0).astype(hot.dtype)
                wide_hot[side, LANES : 2 * LANES, columns] = jnp.maximum(-code, 0.0).astype(hot.dtype)
            code = code.T
            to = pl.ds(pl.multiple_of(at * LANES, LANES), LANES)
            hot[to, 0:LANES] = jnp.maximum(code, 0.0).astype(hot.dtype)
            hot[to, LANES : 2 * LANES] = jnp.maximum(-code, 0.0).astype(hot.dtype)
        return carry

    lax.fori_loop(0, 3 * groups // HEAT, heat, 0)
    for load in loads[5:]:
        load.wait()
    for o in range(offsets):
        when_there(shifts[o], lambda o=o: guess_copy(o).wait_recv())
    next_round(1)

    own_names = lax.broadcasted_iota(jnp.int32, (own, LANES), 0)
    names = lax.broadcasted_iota(jnp.int32, (wide_rows, LANES), 0)

    def at_corner(c, g):
        return pl.ds(pl.multiple_of((g * 3 + c) * ROWS, ROWS), ROWS)

    small = lax.broadcasted_iota(jnp.int32, (1, LANES), 1)

    def whole(a):
        return jnp.sum(jnp.sum(a, axis=0, keepdims=True), axis=1, keepdims=True)

    def packed(terms):
        line = jnp.zeros((1, LANES), f32)
        for i, term in enumerate(terms):
            line = jnp.where(small == i, whole(term), line)
        return line

    sublane = lax.broadcasted_iota(jnp.int32, (ROWS, LANES), 0)
    once = 1 + jnp.minimum(me, 0)

    def operate(t, gathered=None):
        def picked(c, g, count):
            index = lane[at_corner(c, g), :]
            block = blk[at_corner(c, g), :]
            value = jnp.zeros((ROWS, LANES), f32)
            for b in range(count):
                row = jnp.broadcast_to(table[t, b : b + 1, :], (ROWS, LANES))
                got = jnp.take_along_axis(row, index, axis=1, mode="promise_in_bounds")
                value = jnp.where(block == b, got, value)
            return value

        def multiplied(c, g):
            columns = pl.ds(pl.multiple_of(g * (ROWS * LANES), ROWS * LANES), ROWS * LANES)
            product = lax.dot_general(
                split[...],
                wide_hot[c - 1, :, columns],
                (((1,), (0,)), ((), ())),
                preferred_element_type=f32,
            )
            product = product[:wide_rows] + product[wide_rows:]
            at = pl.multiple_of((g * 3 + c) * ROWS, ROWS)
            rows_left = []
            for j in range(ROWS):
                kept = jnp.where(
                    name[pl.ds(at + j, 1), :] == names, product[:, j * LANES : (j + 1) * LANES], 0.0
                )
                kept = [kept[r : r + ROWS] for r in range(0, wide_rows, ROWS)]
                while len(kept) > 1:
                    kept = [a + b for a, b in zip(kept[::2], kept[1::2])]
                rows_left.append(kept[0])
            bit = 1
            while bit < ROWS:
                upper = jnp.bitwise_and(sublane, bit) != 0
                rows_left = [
                    jnp.where(upper, b, a) + pltpu.roll(jnp.where(upper, a, b), bit, axis=0)
                    for a, b in zip(rows_left[::2], rows_left[1::2])
                ]
                bit *= 2
            return rows_left[0]

        def spread(g, energy, products):
            u = [picked(0, g, own)] + [
                multiplied(c, g) if c in products else picked(c, g, nodes) for c in (1, 2)
            ]
            if t > 0:
                for c in range(3):
                    vals[t - 1, at_corner(c, g), :] = u[c]
            adds, local_energy = element(g, u, t == 1)
            for c in range(3):
                top = adds[c].astype(bf16).astype(f32)
                hi[at_corner(c, g), :] = top
                lo[at_corner(c, g), :] = adds[c] - top
            return energy + local_energy if t == 1 else energy

        def summed(first, last, sums):
            parts = []
            for at in range(first * 3 * ROWS, last * 3 * ROWS):
                mask = name[at : at + 1, :] == names
                parts.append(
                    jnp.concatenate(
                        [
                            jnp.where(mask, hi[at : at + 1, :], 0.0),
                            jnp.where(mask, lo[at : at + 1, :], 0.0),
                        ],
                        axis=0,
                    ).astype(bf16)
                )
            product = lax.dot_general(
                jnp.concatenate(parts, axis=1),
                hot[first * 3 * ROWS * LANES : last * 3 * ROWS * LANES, :],
                (((1,), (0,)), ((), ())),
                preferred_element_type=f32,
            )
            return product if sums is None else sums + product

        bounds = [-(-groups * i // PARTS) for i in range(PARTS + 1)]
        energy = jnp.zeros((ROWS, LANES), f32)
        for g in range(bounds[0], bounds[1]):
            energy = spread(g, energy, FIRST)
        sums = jnp.zeros((2 * wide_rows, 2 * LANES), f32)
        for part in range(1, PARTS):

            def step(_, carry, part=part):
                sums, energy = carry
                if gathered is None:
                    sums = summed(bounds[part - 1], bounds[part], sums)
                for g in range(bounds[part], bounds[part + 1]):
                    products = FIRST if gathered else LATER[(g - bounds[part]) % len(LATER)]
                    energy = spread(g, energy, products)
                return sums, energy

            sums, energy = lax.fori_loop(0, once, step, (sums, energy))
        if gathered is not None:
            gathered()
        first = bounds[PARTS - 1] if gathered is None else 0

        def finish(_, carry):
            sums, line = carry
            if t == 1:
                line = packed([table[t, 0:own] * table[t, 0:own], energy])
            return summed(first, groups, sums), line

        sums, line = lax.fori_loop(0, once, finish, (sums, jnp.zeros((1, LANES), f32)))
        sums = sums[:wide_rows] + sums[wide_rows:]
        return sums[:own, :LANES], sums[:halo, LANES:], line

    def element(g, u, with_energy):
        gx0, gy0, gx1, gy1 = [
            elem[pl.ds(pl.multiple_of((g * 4 + c) * ROWS, ROWS), ROWS), :] for c in range(4)
        ]
        here = pl.ds(pl.multiple_of(g * ROWS, ROWS), ROWS)
        size = area[here, :]
        scaled = depth[here, :] * size
        third = size / 3.0
        from0, from1 = u[0] - u[2], u[1] - u[2]
        raw_x = gx0 * from0 + gx1 * from1
        raw_y = gy0 * from0 + gy1 * from1
        slope_x = scaled * raw_x
        slope_y = scaled * raw_y
        flow0 = gx0 * slope_x + gy0 * slope_y
        flow1 = gx1 * slope_x + gy1 * slope_y
        adds = [
            flow0 + third * u[0],
            flow1 + third * u[1],
            third * u[2] - (flow0 + flow1),
        ]
        if not with_energy:
            return adds, None
        return adds, (
            slope_x * raw_x
            + slope_y * raw_y
            + third * (u[0] * u[0] + u[1] * u[1] + u[2] * u[2])
        )

    def exchange(e, own_part, halo_part):
        base[...] = own_part
        for distance in reversed(order):
            i = distances.index(distance)
            for j, (mine, theirs) in enumerate(pairs[distance]):
                if mine == 0:
                    o = shifts.index(theirs)
                    for s in range(slots):
                        at = jnp.minimum(send[0, o, s], own - 1)
                        mix_out[e, i, j, s : s + 1, :] = base[pl.ds(at, 1), :]
                else:
                    o = shifts.index(mine)
                    mix_out[e, i, j] = halo_part[o * slots : (o + 1) * slots]
            when_there(distance, lambda i=i: mix_copy(e, i).start())

    def collect(e, own_part, halo_part):
        own_total = own_part
        halo_total = [halo_part[o * slots : (o + 1) * slots] for o in range(offsets)]
        for distance in order:
            i = distances.index(distance)
            when_there(-distance, lambda i=i: mix_copy(e, i).wait_recv())
            for j, (theirs, mine) in enumerate(pairs[distance]):
                if mine == 0:
                    own_total = owned(own_total, shifts.index(theirs), mix_in.at[e, i, j])
                elif theirs == 0:
                    o = shifts.index(mine)
                    halo_total[o] = halo_total[o] + mix_in[e, i, j]
                else:
                    o, p = shifts.index(mine), shifts.index(theirs)
                    names = links_in[o, o * slots : (o + 1) * slots]
                    for s in range(slots):
                        at = p * slots + s
                        halo_total[o] = halo_total[o] + jnp.where(
                            names == links_in[o, at : at + 1, :], mix_in[e, i, j, s : s + 1, :], 0.0
                        )
        return own_total, halo_total

    def owned(total, o, part):
        for s in range(slots):
            total = total + jnp.where(own_names == send[0, o, s], part[s : s + 1, :], 0.0)
        return total

    def divide(own_total, halo_total):
        for side, total in enumerate([own_total, halo_total]):
            columns = slice(side * LANES, (side + 1) * LANES)
            top = total.astype(bf16)
            split[0:own, columns] = top
            split[own : 2 * own, columns] = (total - top.astype(f32)).astype(bf16)

    def fill(t, own_total, halo_total):
        halo_total = jnp.concatenate(halo_total, axis=0)
        table[t, 0:own] = own_total
        table[t, own:nodes] = halo_total
        divide(own_total, halo_total)

    def start_sum(k, line):
        sum_out[k] = line
        sum_in[k, me] = line

        def push(ahead):
            other = me + ahead
            pltpu.make_async_remote_copy(
                src_ref=sum_out.at[k],
                dst_ref=sum_in.at[k, me],
                send_sem=sum_send_sem.at[k],
                recv_sem=sum_recv_sem.at[k],
                device_id=(jnp.where(other >= n, other - n, other),),
                device_id_type=pl.DeviceIdType.MESH,
            ).start()

        def push_some(first, last):
            steps = (last - first) // PUSH

            def body(i, carry):
                for j in range(PUSH):
                    push(first + i * PUSH + j)
                return carry

            lax.fori_loop(0, steps, body, 0)
            for ahead in range(first + steps * PUSH, last):
                push(ahead)

        push_some(1, n)

    def sum_bytes(k):
        return sum_in.at[k, pl.ds(0, n - 1)]

    def finish_sum(k, count):
        pltpu.make_async_copy(sum_bytes(k), sum_bytes(k), sum_recv_sem.at[k]).wait()
        line = jnp.sum(sum_in[k], axis=0)
        return [
            jnp.sum(jnp.where(small == i, line, 0.0), axis=1, keepdims=True)
            for i in range(count)
        ]

    divide(table[0, 0:own], table[0, own:nodes])
    own_part, halo_part, _ = operate(0)
    own_part, halo_part = forcing[...] - own_part, -halo_part
    exchange(0, own_part, halo_part)
    next_round(2)
    for o in range(offsets):
        when_there(shifts[o], lambda o=o: link_copy(o).wait_recv())
    own_total, halo_total = collect(0, own_part, halo_part)
    fill(1, own_total, halo_total)
    for i in range(3, len(rounds) + 1):
        next_round(i)

    own_part, halo_part, line = operate(1)
    exchange(1, own_part, halo_part)
    start_sum(0, line)
    own_total, halo_total = collect(1, own_part, halo_part)
    fill(2, own_total, halo_total)

    residual, image = table[1, 0:own], table[2, 0:own]
    scalars = []

    def second_sums():
        norm, crossed = finish_sum(0, 2)
        step = norm / crossed
        scalars.extend([norm, crossed, step])

        def pair_energy(g, energy):
            u = [
                vals[0, at_corner(c, g), :] - step * vals[1, at_corner(c, g), :]
                for c in range(3)
            ]
            return energy + element(g, u, True)[1]

        energy = jnp.zeros((ROWS, LANES), f32)
        for g in range(groups):
            energy = pair_energy(g, energy)
        later = residual - step * image
        start_sum(1, packed([later * later, energy, later * image]))

    own_part, halo_part, _ = operate(2, second_sums)
    for o in range(offsets):
        back_out[o] = halo_part[o * slots : (o + 1) * slots]
    for o in range(offsets):
        when_there(shifts[o], lambda o=o: back_copy(o).start())
    norm, crossed, step = scalars
    later = residual - step * image

    for o in range(offsets):
        when_there(-shifts[o], lambda o=o: back_copy(o).wait_recv())
    for o in range(offsets):
        own_part = owned(own_part, o, back_in.at[o])
    applied = image - step * own_part
    for o in range(offsets):
        when_there(-shifts[o], lambda o=o: guess_copy(o).wait_send())
        when_there(-shifts[o], lambda o=o: link_copy(o).wait_send())
        when_there(shifts[o], lambda o=o: back_copy(o).wait_send())
    for e in range(2):
        for i, distance in enumerate(distances):
            when_there(distance, lambda e=e, i=i: mix_copy(e, i).wait_send())
    moved = guess[...] + step * residual
    per_norm = 1.0 / norm
    fresh, own_pair, mixed = finish_sum(1, 3)
    beta = fresh * per_norm
    next_step = fresh / (own_pair + beta * (2.0 * mixed + beta * crossed))
    both[0:own] = moved + next_step * (later + beta * residual)
    both[own : 2 * own] = later - next_step * (applied + beta * image)
    for k in range(2):
        pltpu.make_async_copy(sum_bytes(k), sum_bytes(k), sum_send_sem.at[k]).wait()


def local(
    n,
    forcing,
    first_guess,
    corners,
    gradients,
    element_area,
    element_depth,
    send_blocks,
    recv_blocks,
):
    own, columns = forcing.shape
    _, offsets, slots = send_blocks.shape
    count = element_area.shape[0]
    rows = count // LANES
    nodes = own + offsets * slots
    assert columns == LANES and nodes <= LANES and slots % ROWS == 0
    assert rows % ROWS == 0 and (3 * rows // ROWS) % HEAT == 0 and HEAT % 3 == 0
    assert own == offsets * slots and own % (2 * ROWS) == 0
    f32 = jnp.float32
    vmem = pl.BlockSpec(memory_space=pltpu.VMEM)
    dma = pltpu.SemaphoreType.DMA
    pairs = message_pairs(shift_list(offsets))
    most = max(len(listed) for listed in pairs.values())
    part = (offsets, slots, LANES)
    mix = (2, len(pairs), most, slots, LANES)
    both = pl.pallas_call(
        functools.partial(kernel, n),
        out_shape=pltpu.VMEM((2 * own, columns), f32),
        in_specs=[pl.BlockSpec(memory_space=pl.ANY)] * 8,
        out_specs=vmem,
        scratch_shapes=[
            pltpu.VMEM(forcing.shape, f32),
            pltpu.VMEM(first_guess.shape, f32),
            pltpu.VMEM(corners.shape, jnp.int32),
            pltpu.VMEM(gradients.shape, f32),
            pltpu.VMEM((rows, LANES), f32),
            pltpu.VMEM((rows, LANES), f32),
            pltpu.SMEM(send_blocks.shape, jnp.int32),
            pltpu.SMEM(recv_blocks.shape, jnp.int32),
            dma((8,)),
            pltpu.VMEM((3 * rows, LANES), jnp.int32),
            pltpu.VMEM((3 * rows, LANES), jnp.int32),
            pltpu.VMEM((3 * rows, LANES), jnp.int32),
            pltpu.VMEM((3 * count, 2 * LANES), jnp.float8_e4m3fn),
            pltpu.VMEM((2, 2 * LANES, count), jnp.float8_e4m3fn),
            pltpu.VMEM((2 * own, 2 * LANES), jnp.bfloat16),
            pltpu.VMEM((4 * rows, LANES), f32),
            pltpu.VMEM((2, 3 * rows, LANES), f32),
            pltpu.VMEM((3 * rows, LANES), f32),
            pltpu.VMEM((3 * rows, LANES), f32),
            pltpu.VMEM((3, nodes, LANES), f32),
            pltpu.VMEM((own, LANES), f32),
            pltpu.VMEM((offsets * slots, LANES), jnp.int32),
            pltpu.VMEM((offsets, offsets * slots, LANES), jnp.int32),
            pltpu.VMEM(part, f32),
            pltpu.VMEM(mix, f32),
            pltpu.VMEM(mix, f32),
            pltpu.VMEM(part, f32),
            pltpu.VMEM(part, f32),
            pltpu.VMEM((2, 1, LANES), f32),
            pltpu.VMEM((2, n, 1, LANES), f32),
            dma((offsets,)),
            dma((offsets,)),
            dma((offsets,)),
            dma((offsets,)),
            dma((2, len(pairs))),
            dma((2, len(pairs))),
            dma((offsets,)),
            dma((offsets,)),
            dma((2,)),
            dma((2,)),
            pltpu.SemaphoreType.REGULAR((len(learning_rounds(n, max(pairs))) + 1, 2)),
        ],
        compiler_params=pltpu.CompilerParams(
            collective_id=0, has_side_effects=True
        ),
    )(
        forcing,
        first_guess,
        corners,
        gradients,
        element_area.reshape(rows, LANES),
        element_depth.reshape(rows, LANES),
        send_blocks,
        recv_blocks,
    )
    return both[:own], both[own:]


def solution(mesh):
    placed = (
        P("dom", None),
        P("dom", None),
        P(None, "dom"),
        P(None, "dom"),
        P("dom"),
        P("dom"),
        P("dom", None, None),
        P("dom", None, None),
    )
    return jax.shard_map(
        functools.partial(local, mesh.shape["dom"]),
        mesh=mesh,
        in_specs=placed,
        out_specs=(P("dom", None), P("dom", None)),
        check_vma=False,
    )
```

```python
import functools

import jax
import jax.numpy as jnp
from jax import lax
from jax.experimental import pallas as pl
from jax.experimental.pallas import tpu as pltpu
from jax.sharding import PartitionSpec as P

LANES = 128
ROWS = 8
HEAT = 6
PARTS = 2
FIRST = (1, 2)
LATER = ((1,), ())
LAST = ((1, 2), (1, 2), (1,))
PUSH = 8


def shift_list(offsets):
    half_count = offsets // 2
    return [
        shift_at - half_count if shift_at < half_count else shift_at - half_count + 1
        for shift_at in range(offsets)
    ]


def learning_rounds(n, reach):
    rounds = []
    while reach < n - 1:
        rounds.append(reach)
        reach *= 2
    return rounds


def message_pairs(shifts):
    roles = sorted([0, *shifts])
    reach = max(roles) - min(roles)
    return {
        distance: [(a, b) for a in roles for b in roles if a - b == distance]
        for distance in range(-reach, reach + 1)
        if distance != 0
    }


def kernel(
    n,
    forcing_in,
    guess_in,
    corners_in,
    gradients_in,
    area_in,
    depth_in,
    send_in,
    recv_in,
    both,
    forcing,
    guess,
    corners,
    gradients,
    area,
    depth,
    send,
    recv,
    load_sem,
    blk,
    name,
    lane,
    hot,
    wide_hot,
    split,
    elem,
    vals,
    hi,
    lo,
    table,
    base,
    links,
    links_in,
    guess_out,
    mix_out,
    mix_in,
    back_out,
    back_in,
    sum_out,
    sum_in,
    guess_send_sem,
    guess_recv_sem,
    link_send_sem,
    link_recv_sem,
    mix_send_sem,
    mix_recv_sem,
    back_send_sem,
    back_recv_sem,
    sum_send_sem,
    sum_recv_sem,
    known,
):
    own, _ = forcing.shape
    _, offsets, slots = send.shape
    halo = offsets * slots
    nodes = own + halo
    wide_rows = max(own, halo)
    rows = area.shape[0]
    groups = rows // ROWS
    shifts = shift_list(offsets)
    pairs = message_pairs(shifts)
    distances = list(pairs)
    order = sorted(distances, key=lambda distance: (-abs(distance), distance))
    me = lax.axis_index("dom")
    f32 = jnp.float32
    bf16 = jnp.bfloat16

    def there(distance):
        return jnp.logical_and(me + distance >= 0, me + distance < n)

    def when_there(distance, action):
        @pl.when(there(distance))
        def _():
            action()

    def remote(source, target, send_sem, recv_sem, distance):
        return pltpu.make_async_remote_copy(
            src_ref=source,
            dst_ref=target,
            send_sem=send_sem,
            recv_sem=recv_sem,
            device_id=(me + distance,),
            device_id_type=pl.DeviceIdType.MESH,
        )

    def guess_copy(o):
        return remote(
            guess_out.at[o],
            table.at[0, pl.ds(own + o * slots, slots)],
            guess_send_sem.at[o],
            guess_recv_sem.at[o],
            -shifts[o],
        )

    def link_copy(o):
        return remote(
            links, links_in.at[o], link_send_sem.at[o], link_recv_sem.at[o], -shifts[o]
        )

    def mix_copy(e, i):
        count = len(pairs[distances[i]])
        return remote(
            mix_out.at[e, i, pl.ds(0, count)],
            mix_in.at[e, i, pl.ds(0, count)],
            mix_send_sem.at[e, i],
            mix_recv_sem.at[e, i],
            distances[i],
        )

    def back_copy(o):
        return remote(
            back_out.at[o], back_in.at[o], back_send_sem.at[o], back_recv_sem.at[o], shifts[o]
        )

    loads = [
        pltpu.make_async_copy(source, target, load_sem.at[i])
        for i, (source, target) in enumerate(
            [
                (send_in, send),
                (guess_in, guess),
                (corners_in, corners),
                (recv_in, recv),
                (gradients_in, gradients),
                (area_in, area),
                (depth_in, depth),
                (forcing_in, forcing),
            ]
        )
    ]
    barrier = pltpu.get_barrier_semaphore()
    near = max(shifts)
    for distance in shifts:
        when_there(
            distance,
            lambda distance=distance: pl.semaphore_signal(
                barrier,
                inc=1,
                device_id=(me + distance,),
                device_id_type=pl.DeviceIdType.MESH,
            ),
        )

    for load in loads:
        load.start()
    rounds = learning_rounds(n, near)

    def tell(i):
        for side in range(2):
            far = rounds[i] * (2 * side - 1)
            when_there(
                far,
                lambda side=side, far=far: pl.semaphore_signal(
                    known.at[i, side],
                    inc=1,
                    device_id=(me + far,),
                    device_id_type=pl.DeviceIdType.MESH,
                ),
            )

    def learn(i):
        for side in range(2):
            far = rounds[i] * (1 - 2 * side)
            when_there(
                far, lambda side=side: pl.semaphore_wait(known.at[i, side], 1)
            )

    def next_round(i):
        if i > 0 and i <= len(rounds):
            learn(i - 1)
        if i < len(rounds):
            tell(i)

    for load in loads[:2]:
        load.wait()
    for o in range(offsets):
        for s in range(slots):
            at = jnp.minimum(send[0, o, s], own - 1)
            guess_out[o, s : s + 1, :] = guess[pl.ds(at, 1), :]
    for o in range(offsets):
        for s in range(slots):
            links[o * slots + s : o * slots + s + 1, :] = jnp.full(
                (1, LANES), send[0, o, s], jnp.int32
            )
    pl.semaphore_wait(
        barrier, jnp.minimum(me, near) + jnp.minimum(n - 1 - me, near)
    )
    for o in range(offsets):
        when_there(-shifts[o], lambda o=o: guess_copy(o).start())
    for o in range(offsets):
        when_there(-shifts[o], lambda o=o: link_copy(o).start())
    next_round(0)
    for o in range(offsets):

        @pl.when(jnp.logical_not(there(shifts[o])))
        def _():
            table[0, own + o * slots : own + (o + 1) * slots] = jnp.zeros((slots, LANES), f32)
            links_in[o] = jnp.full((halo, LANES), own, jnp.int32)

        @pl.when(jnp.logical_not(there(-shifts[o])))
        def _():
            back_in[o] = jnp.zeros((slots, LANES), f32)

    for i, distance in enumerate(distances):

        @pl.when(jnp.logical_not(there(-distance)))
        def _():
            for e in range(2):
                mix_in[e, i] = jnp.zeros(mix_in.shape[2:], f32)
    table[0, 0:own] = guess[...]
    for load in loads[2:5]:
        load.wait()

    def lay(r, carry):
        for j in range(ROWS):
            at = pl.multiple_of((r * ROWS + j) * LANES, LANES)
            for c in range(3):
                lane[pl.ds((r * 3 + c) * ROWS + j, 1), :] = corners[c : c + 1, pl.ds(at, LANES)]
            for c in range(4):
                elem[pl.ds((r * 4 + c) * ROWS + j, 1), :] = gradients[c : c + 1, pl.ds(at, LANES)]
        return carry

    lax.fori_loop(0, groups, lay, 0)

    wide = lax.broadcasted_iota(jnp.int32, (ROWS, LANES), 1)
    lookup = jnp.where(wide < own, wide, 2 * LANES)
    for o in range(offsets):
        for s in range(slots):
            lookup = jnp.where(wide == own + recv[0, o, s], own + o * slots + s, lookup)
    lookup = jnp.where(wide < nodes, lookup, 2 * LANES)

    for g in range(3 * groups):
        here = slice(g * ROWS, (g + 1) * ROWS)
        node = lane[here, :]
        block = jnp.take_along_axis(
            lookup, lax.shift_right_logical(node, 7), axis=1, mode="promise_in_bounds"
        )
        blk[here, :] = block
        name[here, :] = jnp.where(block < own, block, block - own)
        hi[here, :] = jnp.where(block < own, 1.0, -1.0)
        lane[here, :] = lax.bitwise_and(node, LANES - 1)

    tall = lax.broadcasted_iota(jnp.int32, (LANES, LANES), 0).astype(f32).astype(bf16)

    def heat(g, carry):
        for j in range(HEAT * ROWS):
            at = g * (HEAT * ROWS) + j

            def filled(ref):
                row = jnp.broadcast_to(ref[pl.ds(at, 1), :].astype(f32), (2 * ROWS, LANES))
                return jnp.concatenate([row.astype(bf16)] * (LANES // (2 * ROWS)), axis=0)

            code = jnp.where(filled(lane) == tall, filled(hi), jnp.zeros((LANES, LANES), bf16))
            block, row = divmod(j, ROWS)
            if block % 3 > 0:
                column = (g * (HEAT // 3) + block // 3) * ROWS + row
                columns = pl.ds(pl.multiple_of(column * LANES, LANES), LANES)
                side = block % 3 - 1
                wide_hot[side, 0:LANES, columns] = jnp.maximum(code, 0.0).astype(hot.dtype)
                wide_hot[side, LANES : 2 * LANES, columns] = jnp.maximum(-code, 0.0).astype(hot.dtype)
            code = code.T
            to = pl.ds(pl.multiple_of(at * LANES, LANES), LANES)
            hot[to, 0:LANES] = jnp.maximum(code, 0.0).astype(hot.dtype)
            hot[to, LANES : 2 * LANES] = jnp.maximum(-code, 0.0).astype(hot.dtype)
        return carry

    lax.fori_loop(0, 3 * groups // HEAT, heat, 0)
    for load in loads[5:]:
        load.wait()
    for o in range(offsets):
        when_there(shifts[o], lambda o=o: guess_copy(o).wait_recv())
    next_round(1)

    own_names = lax.broadcasted_iota(jnp.int32, (own, LANES), 0)
    names = lax.broadcasted_iota(jnp.int32, (wide_rows, LANES), 0)

    def at_corner(c, g):
        return pl.ds(pl.multiple_of((g * 3 + c) * ROWS, ROWS), ROWS)

    small = lax.broadcasted_iota(jnp.int32, (1, LANES), 1)

    def whole(a):
        return jnp.sum(jnp.sum(a, axis=0, keepdims=True), axis=1, keepdims=True)

    def packed(terms):
        line = jnp.zeros((1, LANES), f32)
        for i, term in enumerate(terms):
            line = jnp.where(small == i, whole(term), line)
        return line

    sublane = lax.broadcasted_iota(jnp.int32, (ROWS, LANES), 0)
    once = 1 + jnp.minimum(me, 0)

    def operate(t, step=None, gathered=None):
        def picked(c, g, count):
            index = lane[at_corner(c, g), :]
            block = blk[at_corner(c, g), :]
            value = jnp.zeros((ROWS, LANES), f32)
            for b in range(count):
                row = jnp.broadcast_to(table[t, b : b + 1, :], (ROWS, LANES))
                got = jnp.take_along_axis(row, index, axis=1, mode="promise_in_bounds")
                value = jnp.where(block == b, got, value)
            return value

        def multiplied(c, g):
            columns = pl.ds(pl.multiple_of(g * (ROWS * LANES), ROWS * LANES), ROWS * LANES)
            product = lax.dot_general(
                split[...],
                wide_hot[c - 1, :, columns],
                (((1,), (0,)), ((), ())),
                preferred_element_type=f32,
            )
            product = product[:wide_rows] + product[wide_rows:]
            at = pl.multiple_of((g * 3 + c) * ROWS, ROWS)
            rows_left = []
            for j in range(ROWS):
                kept = jnp.where(
                    name[pl.ds(at + j, 1), :] == names, product[:, j * LANES : (j + 1) * LANES], 0.0
                )
                kept = [kept[r : r + ROWS] for r in range(0, wide_rows, ROWS)]
                while len(kept) > 1:
                    kept = [a + b for a, b in zip(kept[::2], kept[1::2])]
                rows_left.append(kept[0])
            bit = 1
            while bit < ROWS:
                upper = jnp.bitwise_and(sublane, bit) != 0
                rows_left = [
                    jnp.where(upper, b, a) + pltpu.roll(jnp.where(upper, a, b), bit, axis=0)
                    for a, b in zip(rows_left[::2], rows_left[1::2])
                ]
                bit *= 2
            return rows_left[0]

        def spread(g, energy, products):
            u = [picked(0, g, own)] + [
                multiplied(c, g) if c in products else picked(c, g, nodes) for c in (1, 2)
            ]
            adds, local_energy = element(g, u, t == 1)
            for c in range(3):
                if t == 1:
                    vals[at_corner(c, g), :] = u[c]
                if t == 2:
                    u[c] = vals[at_corner(c, g), :] - step * u[c]
            if t == 2:
                local_energy = element(g, u, True)[1]
            for c in range(3):
                top = adds[c].astype(bf16).astype(f32)
                hi[at_corner(c, g), :] = top
                lo[at_corner(c, g), :] = adds[c] - top
            return energy + local_energy if t > 0 else energy

        def summed(first, last, sums):
            parts = []
            for at in range(first * 3 * ROWS, last * 3 * ROWS):
                mask = name[at : at + 1, :] == names
                parts.append(
                    jnp.concatenate(
                        [
                            jnp.where(mask, hi[at : at + 1, :], 0.0),
                            jnp.where(mask, lo[at : at + 1, :], 0.0),
                        ],
                        axis=0,
                    ).astype(bf16)
                )
            product = lax.dot_general(
                jnp.concatenate(parts, axis=1),
                hot[first * 3 * ROWS * LANES : last * 3 * ROWS * LANES, :],
                (((1,), (0,)), ((), ())),
                preferred_element_type=f32,
            )
            return product if sums is None else sums + product

        bounds = [-(-groups * i // PARTS) for i in range(PARTS + 1)]
        energy = jnp.zeros((ROWS, LANES), f32)
        sums = jnp.zeros((2 * wide_rows, 2 * LANES), f32)
        if gathered is not None:
            for g in range(groups):
                energy = spread(g, energy, LAST[g % len(LAST)])
            gathered(energy)
        else:
            for g in range(bounds[0], bounds[1]):
                energy = spread(g, energy, FIRST)
            for part in range(1, PARTS):

                def some(_, carry, part=part):
                    sums, energy = carry
                    sums = summed(bounds[part - 1], bounds[part], sums)
                    for g in range(bounds[part], bounds[part + 1]):
                        energy = spread(g, energy, LATER[(g - bounds[part]) % len(LATER)])
                    return sums, energy

                sums, energy = lax.fori_loop(0, once, some, (sums, energy))
        first = bounds[PARTS - 1] if gathered is None else 0

        def finish(_, carry):
            sums, line = carry
            if t == 1:
                line = packed([table[t, 0:own] * table[t, 0:own], energy])
            return summed(first, groups, sums), line

        sums, line = lax.fori_loop(0, once, finish, (sums, jnp.zeros((1, LANES), f32)))
        sums = sums[:wide_rows] + sums[wide_rows:]
        return sums[:own, :LANES], sums[:halo, LANES:], line

    def element(g, u, with_energy):
        gx0, gy0, gx1, gy1 = [
            elem[pl.ds(pl.multiple_of((g * 4 + c) * ROWS, ROWS), ROWS), :] for c in range(4)
        ]
        here = pl.ds(pl.multiple_of(g * ROWS, ROWS), ROWS)
        size = area[here, :]
        scaled = depth[here, :] * size
        third = size / 3.0
        from0, from1 = u[0] - u[2], u[1] - u[2]
        raw_x = gx0 * from0 + gx1 * from1
        raw_y = gy0 * from0 + gy1 * from1
        slope_x = scaled * raw_x
        slope_y = scaled * raw_y
        flow0 = gx0 * slope_x + gy0 * slope_y
        flow1 = gx1 * slope_x + gy1 * slope_y
        adds = [
            flow0 + third * u[0],
            flow1 + third * u[1],
            third * u[2] - (flow0 + flow1),
        ]
        if not with_energy:
            return adds, None
        return adds, (
            slope_x * raw_x
            + slope_y * raw_y
            + third * (u[0] * u[0] + u[1] * u[1] + u[2] * u[2])
        )

    def exchange(e, own_part, halo_part):
        base[...] = own_part
        for distance in reversed(order):
            i = distances.index(distance)
            for j, (mine, theirs) in enumerate(pairs[distance]):
                if mine == 0:
                    o = shifts.index(theirs)
                    for s in range(slots):
                        at = jnp.minimum(send[0, o, s], own - 1)
                        mix_out[e, i, j, s : s + 1, :] = base[pl.ds(at, 1), :]
                else:
                    o = shifts.index(mine)
                    mix_out[e, i, j] = halo_part[o * slots : (o + 1) * slots]
            when_there(distance, lambda i=i: mix_copy(e, i).start())

    def collect(e, own_part, halo_part):
        own_total = own_part
        halo_total = [halo_part[o * slots : (o + 1) * slots] for o in range(offsets)]
        for distance in order:
            i = distances.index(distance)
            when_there(-distance, lambda i=i: mix_copy(e, i).wait_recv())
            for j, (theirs, mine) in enumerate(pairs[distance]):
                if mine == 0:
                    own_total = owned(own_total, shifts.index(theirs), mix_in.at[e, i, j])
                elif theirs == 0:
                    o = shifts.index(mine)
                    halo_total[o] = halo_total[o] + mix_in[e, i, j]
                else:
                    o, p = shifts.index(mine), shifts.index(theirs)
                    names = links_in[o, o * slots : (o + 1) * slots]
                    for s in range(slots):
                        at = p * slots + s
                        halo_total[o] = halo_total[o] + jnp.where(
                            names == links_in[o, at : at + 1, :], mix_in[e, i, j, s : s + 1, :], 0.0
                        )
        return own_total, halo_total

    def owned(total, o, part):
        for s in range(slots):
            total = total + jnp.where(own_names == send[0, o, s], part[s : s + 1, :], 0.0)
        return total

    def divide(own_total, halo_total):
        for side, total in enumerate([own_total, halo_total]):
            columns = slice(side * LANES, (side + 1) * LANES)
            top = total.astype(bf16)
            split[0:own, columns] = top
            split[own : 2 * own, columns] = (total - top.astype(f32)).astype(bf16)

    def fill(t, own_total, halo_total):
        halo_total = jnp.concatenate(halo_total, axis=0)
        table[t, 0:own] = own_total
        table[t, own:nodes] = halo_total
        divide(own_total, halo_total)

    def start_sum(k, line):
        sum_out[k] = line
        sum_in[k, me] = line

        def push(ahead):
            other = me + ahead
            pltpu.make_async_remote_copy(
                src_ref=sum_out.at[k],
                dst_ref=sum_in.at[k, me],
                send_sem=sum_send_sem.at[k],
                recv_sem=sum_recv_sem.at[k],
                device_id=(jnp.where(other >= n, other - n, other),),
                device_id_type=pl.DeviceIdType.MESH,
            ).start()

        def push_some(first, last):
            steps = (last - first) // PUSH

            def body(i, carry):
                for j in range(PUSH):
                    push(first + i * PUSH + j)
                return carry

            lax.fori_loop(0, steps, body, 0)
            for ahead in range(first + steps * PUSH, last):
                push(ahead)

        push_some(1, n)

    def sum_bytes(k):
        return sum_in.at[k, pl.ds(0, n - 1)]

    def finish_sum(k, count):
        pltpu.make_async_copy(sum_bytes(k), sum_bytes(k), sum_recv_sem.at[k]).wait()
        line = jnp.sum(sum_in[k], axis=0)
        return [
            jnp.sum(jnp.where(small == i, line, 0.0), axis=1, keepdims=True)
            for i in range(count)
        ]

    divide(table[0, 0:own], table[0, own:nodes])
    own_part, halo_part, _ = operate(0)
    own_part, halo_part = forcing[...] - own_part, -halo_part
    exchange(0, own_part, halo_part)
    next_round(2)
    for o in range(offsets):
        when_there(shifts[o], lambda o=o: link_copy(o).wait_recv())
    own_total, halo_total = collect(0, own_part, halo_part)
    fill(1, own_total, halo_total)
    next_round(3)

    own_part, halo_part, line = operate(1)
    exchange(1, own_part, halo_part)
    for i in range(4, len(rounds) + 1):
        next_round(i)
    start_sum(0, line)
    own_total, halo_total = collect(1, own_part, halo_part)
    fill(2, own_total, halo_total)

    norm, crossed = finish_sum(0, 2)
    step = norm / crossed

    def second_sums(energy):
        residual, image = table[1, 0:own], table[2, 0:own]
        later = residual - step * image
        start_sum(1, packed([later * later, energy, later * image]))

    own_part, halo_part, _ = operate(2, step, second_sums)
    for o in range(offsets):
        back_out[o] = halo_part[o * slots : (o + 1) * slots]
    for o in range(offsets):
        when_there(shifts[o], lambda o=o: back_copy(o).start())
    residual, image = table[1, 0:own], table[2, 0:own]
    later = residual - step * image

    for o in range(offsets):
        when_there(-shifts[o], lambda o=o: back_copy(o).wait_recv())
    for o in range(offsets):
        own_part = owned(own_part, o, back_in.at[o])
    applied = image - step * own_part
    for o in range(offsets):
        when_there(-shifts[o], lambda o=o: guess_copy(o).wait_send())
        when_there(-shifts[o], lambda o=o: link_copy(o).wait_send())
        when_there(shifts[o], lambda o=o: back_copy(o).wait_send())
    for e in range(2):
        for i, distance in enumerate(distances):
            when_there(distance, lambda e=e, i=i: mix_copy(e, i).wait_send())
    moved = guess[...] + step * residual
    per_norm = 1.0 / norm
    fresh, own_pair, mixed = finish_sum(1, 3)
    beta = fresh * per_norm
    next_step = fresh / (own_pair + beta * (2.0 * mixed + beta * crossed))
    both[0:own] = moved + next_step * (later + beta * residual)
    both[own : 2 * own] = later - next_step * (applied + beta * image)
    for k in range(2):
        pltpu.make_async_copy(sum_bytes(k), sum_bytes(k), sum_send_sem.at[k]).wait()


def local(
    n,
    forcing,
    first_guess,
    corners,
    gradients,
    element_area,
    element_depth,
    send_blocks,
    recv_blocks,
):
    own, columns = forcing.shape
    _, offsets, slots = send_blocks.shape
    count = element_area.shape[0]
    rows = count // LANES
    nodes = own + offsets * slots
    assert columns == LANES and nodes <= LANES and slots % ROWS == 0
    assert rows % ROWS == 0 and (3 * rows // ROWS) % HEAT == 0 and HEAT % 3 == 0
    assert own == offsets * slots and own % (2 * ROWS) == 0
    f32 = jnp.float32
    vmem = pl.BlockSpec(memory_space=pltpu.VMEM)
    dma = pltpu.SemaphoreType.DMA
    pairs = message_pairs(shift_list(offsets))
    most = max(len(listed) for listed in pairs.values())
    part = (offsets, slots, LANES)
    mix = (2, len(pairs), most, slots, LANES)
    both = pl.pallas_call(
        functools.partial(kernel, n),
        out_shape=pltpu.VMEM((2 * own, columns), f32),
        in_specs=[pl.BlockSpec(memory_space=pl.ANY)] * 8,
        out_specs=vmem,
        scratch_shapes=[
            pltpu.VMEM(forcing.shape, f32),
            pltpu.VMEM(first_guess.shape, f32),
            pltpu.VMEM(corners.shape, jnp.int32),
            pltpu.VMEM(gradients.shape, f32),
            pltpu.VMEM((rows, LANES), f32),
            pltpu.VMEM((rows, LANES), f32),
            pltpu.SMEM(send_blocks.shape, jnp.int32),
            pltpu.SMEM(recv_blocks.shape, jnp.int32),
            dma((8,)),
            pltpu.VMEM((3 * rows, LANES), jnp.int32),
            pltpu.VMEM((3 * rows, LANES), jnp.int32),
            pltpu.VMEM((3 * rows, LANES), jnp.int32),
            pltpu.VMEM((3 * count, 2 * LANES), jnp.float8_e4m3fn),
            pltpu.VMEM((2, 2 * LANES, count), jnp.float8_e4m3fn),
            pltpu.VMEM((2 * own, 2 * LANES), jnp.bfloat16),
            pltpu.VMEM((4 * rows, LANES), f32),
            pltpu.VMEM((3 * rows, LANES), f32),
            pltpu.VMEM((3 * rows, LANES), f32),
            pltpu.VMEM((3 * rows, LANES), f32),
            pltpu.VMEM((3, nodes, LANES), f32),
            pltpu.VMEM((own, LANES), f32),
            pltpu.VMEM((offsets * slots, LANES), jnp.int32),
            pltpu.VMEM((offsets, offsets * slots, LANES), jnp.int32),
            pltpu.VMEM(part, f32),
            pltpu.VMEM(mix, f32),
            pltpu.VMEM(mix, f32),
            pltpu.VMEM(part, f32),
            pltpu.VMEM(part, f32),
            pltpu.VMEM((2, 1, LANES), f32),
            pltpu.VMEM((2, n, 1, LANES), f32),
            dma((offsets,)),
            dma((offsets,)),
            dma((offsets,)),
            dma((offsets,)),
            dma((2, len(pairs))),
            dma((2, len(pairs))),
            dma((offsets,)),
            dma((offsets,)),
            dma((2,)),
            dma((2,)),
            pltpu.SemaphoreType.REGULAR((len(learning_rounds(n, max(shift_list(offsets)))) + 1, 2)),
        ],
        compiler_params=pltpu.CompilerParams(
            collective_id=0, has_side_effects=True
        ),
    )(
        forcing,
        first_guess,
        corners,
        gradients,
        element_area.reshape(rows, LANES),
        element_depth.reshape(rows, LANES),
        send_blocks,
        recv_blocks,
    )
    return both[:own], both[own:]


def solution(mesh):
    placed = (
        P("dom", None),
        P("dom", None),
        P(None, "dom"),
        P(None, "dom"),
        P("dom"),
        P("dom"),
        P("dom", None, None),
        P("dom", None, None),
    )
    return jax.shard_map(
        functools.partial(local, mesh.shape["dom"]),
        mesh=mesh,
        in_specs=placed,
        out_specs=(P("dom", None), P("dom", None)),
        check_vma=False,
    )
```

```python
import functools

import jax
import jax.numpy as jnp
from jax import lax
from jax.experimental import pallas as pl
from jax.experimental.pallas import tpu as pltpu
from jax.sharding import PartitionSpec as P

LANES = 128
ROWS = 8
HEAT = 6
PARTS = 2
FIRST = (1, 2)
LATER = ((1,), ())
LAST = ((1, 2), (1, 2), (1,))
PUSH = 8


def shift_list(offsets):
    half_count = offsets // 2
    return [
        shift_at - half_count if shift_at < half_count else shift_at - half_count + 1
        for shift_at in range(offsets)
    ]


def learning_rounds(n, reach):
    rounds = []
    while reach < n - 1:
        rounds.append(reach)
        reach *= 2
    return rounds


def message_pairs(shifts):
    roles = sorted([0, *shifts])
    reach = max(roles) - min(roles)
    return {
        distance: [(a, b) for a in roles for b in roles if a - b == distance]
        for distance in range(-reach, reach + 1)
        if distance != 0
    }


def kernel(
    n,
    forcing_in,
    guess_in,
    corners_in,
    gradients_in,
    area_in,
    depth_in,
    send_in,
    recv_in,
    both,
    forcing,
    guess,
    corners,
    gradients,
    area,
    depth,
    send,
    recv,
    load_sem,
    blk,
    name,
    lane,
    hot,
    wide_hot,
    split,
    elem,
    vals,
    hi,
    lo,
    table,
    base,
    links,
    links_in,
    guess_out,
    mix_out,
    mix_in,
    back_out,
    back_in,
    sum_out,
    sum_in,
    guess_send_sem,
    guess_recv_sem,
    link_send_sem,
    link_recv_sem,
    mix_send_sem,
    mix_recv_sem,
    back_send_sem,
    back_recv_sem,
    sum_send_sem,
    sum_recv_sem,
    known,
):
    own, _ = forcing.shape
    _, offsets, slots = send.shape
    halo = offsets * slots
    nodes = own + halo
    wide_rows = max(own, halo)
    rows = area.shape[0]
    groups = rows // ROWS
    shifts = shift_list(offsets)
    pairs = message_pairs(shifts)
    distances = list(pairs)
    order = sorted(distances, key=lambda distance: (-abs(distance), distance))
    me = lax.axis_index("dom")
    f32 = jnp.float32
    bf16 = jnp.bfloat16

    def there(distance):
        return jnp.logical_and(me + distance >= 0, me + distance < n)

    def when_there(distance, action):
        @pl.when(there(distance))
        def _():
            action()

    def remote(source, target, send_sem, recv_sem, distance):
        return pltpu.make_async_remote_copy(
            src_ref=source,
            dst_ref=target,
            send_sem=send_sem,
            recv_sem=recv_sem,
            device_id=(me + distance,),
            device_id_type=pl.DeviceIdType.MESH,
        )

    def guess_copy(o):
        return remote(
            guess_out.at[o],
            table.at[0, pl.ds(own + o * slots, slots)],
            guess_send_sem.at[o],
            guess_recv_sem.at[o],
            -shifts[o],
        )

    def link_copy(o):
        return remote(
            links, links_in.at[o], link_send_sem.at[o], link_recv_sem.at[o], -shifts[o]
        )

    def mix_copy(e, i):
        count = len(pairs[distances[i]])
        return remote(
            mix_out.at[e, i, pl.ds(0, count)],
            mix_in.at[e, i, pl.ds(0, count)],
            mix_send_sem.at[e, i],
            mix_recv_sem.at[e, i],
            distances[i],
        )

    def back_copy(o):
        return remote(
            back_out.at[o], back_in.at[o], back_send_sem.at[o], back_recv_sem.at[o], shifts[o]
        )

    loads = [
        pltpu.make_async_copy(source, target, load_sem.at[i])
        for i, (source, target) in enumerate(
            [
                (send_in, send),
                (guess_in, guess),
                (corners_in, corners),
                (recv_in, recv),
                (gradients_in, gradients),
                (area_in, area),
                (depth_in, depth),
                (forcing_in, forcing),
            ]
        )
    ]
    barrier = pltpu.get_barrier_semaphore()
    near = max(shifts)
    for distance in shifts:
        when_there(
            distance,
            lambda distance=distance: pl.semaphore_signal(
                barrier,
                inc=1,
                device_id=(me + distance,),
                device_id_type=pl.DeviceIdType.MESH,
            ),
        )

    for load in loads:
        load.start()
    rounds = learning_rounds(n, near)

    def tell(i):
        for side in range(2):
            far = rounds[i] * (2 * side - 1)
            when_there(
                far,
                lambda side=side, far=far: pl.semaphore_signal(
                    known.at[i, side],
                    inc=1,
                    device_id=(me + far,),
                    device_id_type=pl.DeviceIdType.MESH,
                ),
            )

    def learn(i):
        for side in range(2):
            far = rounds[i] * (1 - 2 * side)
            when_there(
                far, lambda side=side: pl.semaphore_wait(known.at[i, side], 1)
            )

    def next_round(i):
        if i > 0 and i <= len(rounds):
            learn(i - 1)
        if i < len(rounds):
            tell(i)

    for load in loads[:2]:
        load.wait()
    for o in range(offsets):
        for s in range(slots):
            at = jnp.minimum(send[0, o, s], own - 1)
            guess_out[o, s : s + 1, :] = guess[pl.ds(at, 1), :]
    for o in range(offsets):
        for s in range(slots):
            links[o * slots + s : o * slots + s + 1, :] = jnp.full(
                (1, LANES), send[0, o, s], jnp.int32
            )
    pl.semaphore_wait(
        barrier, jnp.minimum(me, near) + jnp.minimum(n - 1 - me, near)
    )
    for o in range(offsets):
        when_there(-shifts[o], lambda o=o: guess_copy(o).start())
    for o in range(offsets):
        when_there(-shifts[o], lambda o=o: link_copy(o).start())
    next_round(0)
    for o in range(offsets):

        @pl.when(jnp.logical_not(there(shifts[o])))
        def _():
            table[0, own + o * slots : own + (o + 1) * slots] = jnp.zeros((slots, LANES), f32)
            links_in[o] = jnp.full((halo, LANES), own, jnp.int32)

        @pl.when(jnp.logical_not(there(-shifts[o])))
        def _():
            back_in[o] = jnp.zeros((slots, LANES), f32)

    for i, distance in enumerate(distances):

        @pl.when(jnp.logical_not(there(-distance)))
        def _():
            for e in range(2):
                mix_in[e, i] = jnp.zeros(mix_in.shape[2:], f32)
    table[0, 0:own] = guess[...]
    for load in loads[2:5]:
        load.wait()

    def lay(r, carry):
        for j in range(ROWS):
            at = pl.multiple_of((r * ROWS + j) * LANES, LANES)
            for c in range(3):
                lane[pl.ds((r * 3 + c) * ROWS + j, 1), :] = corners[c : c + 1, pl.ds(at, LANES)]
            for c in range(4):
                elem[pl.ds((r * 4 + c) * ROWS + j, 1), :] = gradients[c : c + 1, pl.ds(at, LANES)]
        return carry

    lax.fori_loop(0, groups, lay, 0)

    wide = lax.broadcasted_iota(jnp.int32, (ROWS, LANES), 1)
    lookup = jnp.where(wide < own, wide, 2 * LANES)
    for o in range(offsets):
        for s in range(slots):
            lookup = jnp.where(wide == own + recv[0, o, s], own + o * slots + s, lookup)
    lookup = jnp.where(wide < nodes, lookup, 2 * LANES)

    for g in range(3 * groups):
        here = slice(g * ROWS, (g + 1) * ROWS)
        node = lane[here, :]
        block = jnp.take_along_axis(
            lookup, lax.shift_right_logical(node, 7), axis=1, mode="promise_in_bounds"
        )
        blk[here, :] = block
        name[here, :] = jnp.where(block < own, block, block - own)
        hi[here, :] = jnp.where(block < own, 1.0, -1.0)
        lane[here, :] = lax.bitwise_and(node, LANES - 1)

    tall = lax.broadcasted_iota(jnp.int32, (LANES, LANES), 0).astype(f32).astype(bf16)

    def heat(g, carry):
        for j in range(HEAT * ROWS):
            at = g * (HEAT * ROWS) + j

            def filled(ref):
                row = jnp.broadcast_to(ref[pl.ds(at, 1), :].astype(f32), (2 * ROWS, LANES))
                return jnp.concatenate([row.astype(bf16)] * (LANES // (2 * ROWS)), axis=0)

            code = jnp.where(filled(lane) == tall, filled(hi), jnp.zeros((LANES, LANES), bf16))
            block, row = divmod(j, ROWS)
            if block % 3 > 0:
                column = (g * (HEAT // 3) + block // 3) * ROWS + row
                columns = pl.ds(pl.multiple_of(column * LANES, LANES), LANES)
                side = block % 3 - 1
                wide_hot[side, 0:LANES, columns] = jnp.maximum(code, 0.0).astype(hot.dtype)
                wide_hot[side, LANES : 2 * LANES, columns] = jnp.maximum(-code, 0.0).astype(hot.dtype)
            code = code.T
            to = pl.ds(pl.multiple_of(at * LANES, LANES), LANES)
            hot[to, 0:LANES] = jnp.maximum(code, 0.0).astype(hot.dtype)
            hot[to, LANES : 2 * LANES] = jnp.maximum(-code, 0.0).astype(hot.dtype)
        return carry

    lax.fori_loop(0, 3 * groups // HEAT, heat, 0)
    for load in loads[5:]:
        load.wait()
    for o in range(offsets):
        when_there(shifts[o], lambda o=o: guess_copy(o).wait_recv())
    next_round(1)

    own_names = lax.broadcasted_iota(jnp.int32, (own, LANES), 0)
    names = lax.broadcasted_iota(jnp.int32, (wide_rows, LANES), 0)

    def at_corner(c, g):
        return pl.ds(pl.multiple_of((g * 3 + c) * ROWS, ROWS), ROWS)

    small = lax.broadcasted_iota(jnp.int32, (1, LANES), 1)

    def whole(a):
        return jnp.sum(jnp.sum(a, axis=0, keepdims=True), axis=1, keepdims=True)

    def packed(terms):
        line = jnp.zeros((1, LANES), f32)
        for i, term in enumerate(terms):
            line = jnp.where(small == i, whole(term), line)
        return line

    sublane = lax.broadcasted_iota(jnp.int32, (ROWS, LANES), 0)
    once = 1 + jnp.minimum(me, 0)

    def operate(t, length=None, gathered=None):
        def picked(c, g, count):
            index = lane[at_corner(c, g), :]
            block = blk[at_corner(c, g), :]
            value = jnp.zeros((ROWS, LANES), f32)
            for b in range(count):
                row = jnp.broadcast_to(table[t, b : b + 1, :], (ROWS, LANES))
                got = jnp.take_along_axis(row, index, axis=1, mode="promise_in_bounds")
                value = jnp.where(block == b, got, value)
            return value

        def multiplied(c, g):
            columns = pl.ds(pl.multiple_of(g * (ROWS * LANES), ROWS * LANES), ROWS * LANES)
            product = lax.dot_general(
                split[...],
                wide_hot[c - 1, :, columns],
                (((1,), (0,)), ((), ())),
                preferred_element_type=f32,
            )
            product = product[:wide_rows] + product[wide_rows:]
            at = pl.multiple_of((g * 3 + c) * ROWS, ROWS)
            rows_left = []
            for j in range(ROWS):
                kept = jnp.where(
                    name[pl.ds(at + j, 1), :] == names, product[:, j * LANES : (j + 1) * LANES], 0.0
                )
                kept = [kept[r : r + ROWS] for r in range(0, wide_rows, ROWS)]
                while len(kept) > 1:
                    kept = [a + b for a, b in zip(kept[::2], kept[1::2])]
                rows_left.append(kept[0])
            bit = 1
            while bit < ROWS:
                upper = jnp.bitwise_and(sublane, bit) != 0
                rows_left = [
                    jnp.where(upper, b, a) + pltpu.roll(jnp.where(upper, a, b), bit, axis=0)
                    for a, b in zip(rows_left[::2], rows_left[1::2])
                ]
                bit *= 2
            return rows_left[0]

        def spread(g, energy, products, step=None):
            u = [picked(0, g, own)] + [
                multiplied(c, g) if c in products else picked(c, g, nodes) for c in (1, 2)
            ]
            adds, local_energy = element(g, u, t == 1)
            if t == 1 or t == 2 and step is None:
                for c in range(3):
                    vals[t - 1, at_corner(c, g), :] = u[c]
            if step is not None:
                u = [vals[0, at_corner(c, g), :] - step * u[c] for c in range(3)]
                local_energy = element(g, u, True)[1]
            for c in range(3):
                top = adds[c].astype(bf16).astype(f32)
                hi[at_corner(c, g), :] = top
                lo[at_corner(c, g), :] = adds[c] - top
            return energy if local_energy is None else energy + local_energy

        def summed(first, last, sums):
            parts = []
            for at in range(first * 3 * ROWS, last * 3 * ROWS):
                mask = name[at : at + 1, :] == names
                parts.append(
                    jnp.concatenate(
                        [
                            jnp.where(mask, hi[at : at + 1, :], 0.0),
                            jnp.where(mask, lo[at : at + 1, :], 0.0),
                        ],
                        axis=0,
                    ).astype(bf16)
                )
            product = lax.dot_general(
                jnp.concatenate(parts, axis=1),
                hot[first * 3 * ROWS * LANES : last * 3 * ROWS * LANES, :],
                (((1,), (0,)), ((), ())),
                preferred_element_type=f32,
            )
            return product if sums is None else sums + product

        bounds = [-(-groups * i // PARTS) for i in range(PARTS + 1)]
        energy = jnp.zeros((ROWS, LANES), f32)
        sums = jnp.zeros((2 * wide_rows, 2 * LANES), f32)
        if gathered is not None:
            for g in range(groups // 2):
                energy = spread(g, energy, LAST[g % len(LAST)])
            step = length()
            for g in range(groups // 2):
                u = [
                    vals[0, at_corner(c, g), :] - step * vals[1, at_corner(c, g), :]
                    for c in range(3)
                ]
                energy = energy + element(g, u, True)[1]
            for g in range(groups // 2, groups):
                energy = spread(g, energy, LAST[g % len(LAST)], step)
            gathered(energy, step)
        else:
            for g in range(bounds[0], bounds[1]):
                energy = spread(g, energy, FIRST)
            for part in range(1, PARTS):

                def some(_, carry, part=part):
                    sums, energy = carry
                    sums = summed(bounds[part - 1], bounds[part], sums)
                    for g in range(bounds[part], bounds[part + 1]):
                        energy = spread(g, energy, LATER[(g - bounds[part]) % len(LATER)])
                    return sums, energy

                sums, energy = lax.fori_loop(0, once, some, (sums, energy))
        first = bounds[PARTS - 1] if gathered is None else 0

        def finish(_, carry):
            sums, line = carry
            if t == 1:
                line = packed([table[t, 0:own] * table[t, 0:own], energy])
            return summed(first, groups, sums), line

        sums, line = lax.fori_loop(0, once, finish, (sums, jnp.zeros((1, LANES), f32)))
        sums = sums[:wide_rows] + sums[wide_rows:]
        return sums[:own, :LANES], sums[:halo, LANES:], line

    def element(g, u, with_energy):
        gx0, gy0, gx1, gy1 = [
            elem[pl.ds(pl.multiple_of((g * 4 + c) * ROWS, ROWS), ROWS), :] for c in range(4)
        ]
        here = pl.ds(pl.multiple_of(g * ROWS, ROWS), ROWS)
        size = area[here, :]
        scaled = depth[here, :] * size
        third = size / 3.0
        from0, from1 = u[0] - u[2], u[1] - u[2]
        raw_x = gx0 * from0 + gx1 * from1
        raw_y = gy0 * from0 + gy1 * from1
        slope_x = scaled * raw_x
        slope_y = scaled * raw_y
        flow0 = gx0 * slope_x + gy0 * slope_y
        flow1 = gx1 * slope_x + gy1 * slope_y
        adds = [
            flow0 + third * u[0],
            flow1 + third * u[1],
            third * u[2] - (flow0 + flow1),
        ]
        if not with_energy:
            return adds, None
        return adds, (
            slope_x * raw_x
            + slope_y * raw_y
            + third * (u[0] * u[0] + u[1] * u[1] + u[2] * u[2])
        )

    def exchange(e, own_part, halo_part):
        base[...] = own_part
        for distance in reversed(order):
            i = distances.index(distance)
            for j, (mine, theirs) in enumerate(pairs[distance]):
                if mine == 0:
                    o = shifts.index(theirs)
                    for s in range(slots):
                        at = jnp.minimum(send[0, o, s], own - 1)
                        mix_out[e, i, j, s : s + 1, :] = base[pl.ds(at, 1), :]
                else:
                    o = shifts.index(mine)
                    mix_out[e, i, j] = halo_part[o * slots : (o + 1) * slots]
            when_there(distance, lambda i=i: mix_copy(e, i).start())

    def collect(e, own_part, halo_part):
        own_total = own_part
        halo_total = [halo_part[o * slots : (o + 1) * slots] for o in range(offsets)]
        for distance in order:
            i = distances.index(distance)
            when_there(-distance, lambda i=i: mix_copy(e, i).wait_recv())
            for j, (theirs, mine) in enumerate(pairs[distance]):
                if mine == 0:
                    own_total = owned(own_total, shifts.index(theirs), mix_in.at[e, i, j])
                elif theirs == 0:
                    o = shifts.index(mine)
                    halo_total[o] = halo_total[o] + mix_in[e, i, j]
                else:
                    o, p = shifts.index(mine), shifts.index(theirs)
                    names = links_in[o, o * slots : (o + 1) * slots]
                    for s in range(slots):
                        at = p * slots + s
                        halo_total[o] = halo_total[o] + jnp.where(
                            names == links_in[o, at : at + 1, :], mix_in[e, i, j, s : s + 1, :], 0.0
                        )
        return own_total, halo_total

    def owned(total, o, part):
        for s in range(slots):
            total = total + jnp.where(own_names == send[0, o, s], part[s : s + 1, :], 0.0)
        return total

    def divide(own_total, halo_total):
        for side, total in enumerate([own_total, halo_total]):
            columns = slice(side * LANES, (side + 1) * LANES)
            top = total.astype(bf16)
            split[0:own, columns] = top
            split[own : 2 * own, columns] = (total - top.astype(f32)).astype(bf16)

    def fill(t, own_total, halo_total):
        halo_total = jnp.concatenate(halo_total, axis=0)
        table[t, 0:own] = own_total
        table[t, own:nodes] = halo_total
        divide(own_total, halo_total)

    def start_sum(k, line):
        sum_out[k] = line
        sum_in[k, me] = line

        def push(ahead):
            other = me + ahead
            pltpu.make_async_remote_copy(
                src_ref=sum_out.at[k],
                dst_ref=sum_in.at[k, me],
                send_sem=sum_send_sem.at[k],
                recv_sem=sum_recv_sem.at[k],
                device_id=(jnp.where(other >= n, other - n, other),),
                device_id_type=pl.DeviceIdType.MESH,
            ).start()

        def push_some(first, last):
            steps = (last - first) // PUSH

            def body(i, carry):
                for j in range(PUSH):
                    push(first + i * PUSH + j)
                return carry

            lax.fori_loop(0, steps, body, 0)
            for ahead in range(first + steps * PUSH, last):
                push(ahead)

        push_some(1, n)

    def sum_bytes(k):
        return sum_in.at[k, pl.ds(0, n - 1)]

    def finish_sum(k, count):
        pltpu.make_async_copy(sum_bytes(k), sum_bytes(k), sum_recv_sem.at[k]).wait()
        line = jnp.sum(sum_in[k], axis=0)
        return [
            jnp.sum(jnp.where(small == i, line, 0.0), axis=1, keepdims=True)
            for i in range(count)
        ]

    divide(table[0, 0:own], table[0, own:nodes])
    own_part, halo_part, _ = operate(0)
    own_part, halo_part = forcing[...] - own_part, -halo_part
    exchange(0, own_part, halo_part)
    next_round(2)
    for o in range(offsets):
        when_there(shifts[o], lambda o=o: link_copy(o).wait_recv())
    own_total, halo_total = collect(0, own_part, halo_part)
    fill(1, own_total, halo_total)
    next_round(3)

    own_part, halo_part, line = operate(1)
    exchange(1, own_part, halo_part)
    for i in range(4, len(rounds) + 1):
        next_round(i)
    start_sum(0, line)
    own_total, halo_total = collect(1, own_part, halo_part)
    fill(2, own_total, halo_total)

    scalars = []

    def step_length():
        norm, crossed = finish_sum(0, 2)
        scalars.extend([norm, crossed, norm / crossed])
        return scalars[2]

    def second_sums(energy, step):
        residual, image = table[1, 0:own], table[2, 0:own]
        later = residual - step * image
        start_sum(1, packed([later * later, energy, later * image]))

    own_part, halo_part, _ = operate(2, step_length, second_sums)
    norm, crossed, step = scalars
    for o in range(offsets):
        back_out[o] = halo_part[o * slots : (o + 1) * slots]
    for o in range(offsets):
        when_there(shifts[o], lambda o=o: back_copy(o).start())
    residual, image = table[1, 0:own], table[2, 0:own]
    later = residual - step * image

    for o in range(offsets):
        when_there(-shifts[o], lambda o=o: back_copy(o).wait_recv())
    for o in range(offsets):
        own_part = owned(own_part, o, back_in.at[o])
    applied = image - step * own_part
    for o in range(offsets):
        when_there(-shifts[o], lambda o=o: guess_copy(o).wait_send())
        when_there(-shifts[o], lambda o=o: link_copy(o).wait_send())
        when_there(shifts[o], lambda o=o: back_copy(o).wait_send())
    for e in range(2):
        for i, distance in enumerate(distances):
            when_there(distance, lambda e=e, i=i: mix_copy(e, i).wait_send())
    moved = guess[...] + step * residual
    per_norm = 1.0 / norm
    fresh, own_pair, mixed = finish_sum(1, 3)
    beta = fresh * per_norm
    next_step = fresh / (own_pair + beta * (2.0 * mixed + beta * crossed))
    both[0:own] = moved + next_step * (later + beta * residual)
    both[own : 2 * own] = later - next_step * (applied + beta * image)
    for k in range(2):
        pltpu.make_async_copy(sum_bytes(k), sum_bytes(k), sum_send_sem.at[k]).wait()


def local(
    n,
    forcing,
    first_guess,
    corners,
    gradients,
    element_area,
    element_depth,
    send_blocks,
    recv_blocks,
):
    own, columns = forcing.shape
    _, offsets, slots = send_blocks.shape
    count = element_area.shape[0]
    rows = count // LANES
    nodes = own + offsets * slots
    assert columns == LANES and nodes <= LANES and slots % ROWS == 0
    assert rows % ROWS == 0 and (3 * rows // ROWS) % HEAT == 0 and HEAT % 3 == 0
    assert own == offsets * slots and own % (2 * ROWS) == 0
    f32 = jnp.float32
    vmem = pl.BlockSpec(memory_space=pltpu.VMEM)
    dma = pltpu.SemaphoreType.DMA
    pairs = message_pairs(shift_list(offsets))
    most = max(len(listed) for listed in pairs.values())
    part = (offsets, slots, LANES)
    mix = (2, len(pairs), most, slots, LANES)
    both = pl.pallas_call(
        functools.partial(kernel, n),
        out_shape=pltpu.VMEM((2 * own, columns), f32),
        in_specs=[pl.BlockSpec(memory_space=pl.ANY)] * 8,
        out_specs=vmem,
        scratch_shapes=[
            pltpu.VMEM(forcing.shape, f32),
            pltpu.VMEM(first_guess.shape, f32),
            pltpu.VMEM(corners.shape, jnp.int32),
            pltpu.VMEM(gradients.shape, f32),
            pltpu.VMEM((rows, LANES), f32),
            pltpu.VMEM((rows, LANES), f32),
            pltpu.SMEM(send_blocks.shape, jnp.int32),
            pltpu.SMEM(recv_blocks.shape, jnp.int32),
            dma((8,)),
            pltpu.VMEM((3 * rows, LANES), jnp.int32),
            pltpu.VMEM((3 * rows, LANES), jnp.int32),
            pltpu.VMEM((3 * rows, LANES), jnp.int32),
            pltpu.VMEM((3 * count, 2 * LANES), jnp.float8_e4m3fn),
            pltpu.VMEM((2, 2 * LANES, count), jnp.float8_e4m3fn),
            pltpu.VMEM((2 * own, 2 * LANES), jnp.bfloat16),
            pltpu.VMEM((4 * rows, LANES), f32),
            pltpu.VMEM((2, 3 * rows, LANES), f32),
            pltpu.VMEM((3 * rows, LANES), f32),
            pltpu.VMEM((3 * rows, LANES), f32),
            pltpu.VMEM((3, nodes, LANES), f32),
            pltpu.VMEM((own, LANES), f32),
            pltpu.VMEM((offsets * slots, LANES), jnp.int32),
            pltpu.VMEM((offsets, offsets * slots, LANES), jnp.int32),
            pltpu.VMEM(part, f32),
            pltpu.VMEM(mix, f32),
            pltpu.VMEM(mix, f32),
            pltpu.VMEM(part, f32),
            pltpu.VMEM(part, f32),
            pltpu.VMEM((2, 1, LANES), f32),
            pltpu.VMEM((2, n, 1, LANES), f32),
            dma((offsets,)),
            dma((offsets,)),
            dma((offsets,)),
            dma((offsets,)),
            dma((2, len(pairs))),
            dma((2, len(pairs))),
            dma((offsets,)),
            dma((offsets,)),
            dma((2,)),
            dma((2,)),
            pltpu.SemaphoreType.REGULAR((len(learning_rounds(n, max(shift_list(offsets)))) + 1, 2)),
        ],
        compiler_params=pltpu.CompilerParams(
            collective_id=0, has_side_effects=True
        ),
    )(
        forcing,
        first_guess,
        corners,
        gradients,
        element_area.reshape(rows, LANES),
        element_depth.reshape(rows, LANES),
        send_blocks,
        recv_blocks,
    )
    return both[:own], both[own:]


def solution(mesh):
    placed = (
        P("dom", None),
        P("dom", None),
        P(None, "dom"),
        P(None, "dom"),
        P("dom"),
        P("dom"),
        P("dom", None, None),
        P("dom", None, None),
    )
    return jax.shard_map(
        functools.partial(local, mesh.shape["dom"]),
        mesh=mesh,
        in_specs=placed,
        out_specs=(P("dom", None), P("dom", None)),
        check_vma=False,
    )
```
